32 devices in a mesh: dp: 4 (over z), row: 2 (over y), col: 4 (over x, core).
Axes of the slice: x: 2, y: 2, z: 4, core: 2. Of those that a mesh axis runs over, the one named last changes fastest.
Arguments:
- tokens: bfloat16 [4096, 2048], P(('dp', 'row'), 'col'), may hold values from -6 to 6
- w_query: bfloat16 [2048, 2048], P(('dp', 'row'), 'col'), may hold values from -0.125 to 0.125
- key_matrix: bfloat16 [2048, 1024], P(('dp', 'row'), 'col'), may hold values from -0.125 to 0.125
- value_matrix: bfloat16 [2048, 1024], P(('dp', 'row'), 'col'), may hold values from -0.125 to 0.125
- w_output: bfloat16 [2048, 2048], P('col', ('dp', 'row')), may hold values from -1 to 1
- w_gate: bfloat16 [2048, 8192], P(('dp', 'row'), 'col'), may hold values from -0.125 to 0.125
- w_up: bfloat16 [2048, 8192], P(('dp', 'row'), 'col'), may hold values from -0.125 to 0.125
- w_down: bfloat16 [8192, 2048], P('col', ('dp', 'row')), may hold values from -0.0625 to 0.0625
- gain_attn: bfloat16 [2048], P(('dp', 'row')), may hold values from 0.5 to 1.5
- gain_ffn: bfloat16 [2048], P(('dp', 'row')), may hold values from 0.5 to 1.5
- lengths: int32 [4], P('dp'), may hold values from 256 to 1024, as said below
- cotangent: bfloat16 [4096, 2048], P(('dp', 'row'), 'col'), may hold values from -6 to 6
Outputs:
- layer_out: bfloat16 [4096, 2048], P(('dp', 'row'), 'col')
- grad_tokens: bfloat16 [4096, 2048], P(('dp', 'row'), 'col')
- grad_gain_attn: float32 [2048], P(('dp', 'row'))
- grad_gain_ffn: float32 [2048], P(('dp', 'row'))
- grad_query: float32 [2048, 2048], P(('dp', 'row'), 'col')
- grad_key: float32 [2048, 1024], P(('dp', 'row'), 'col')
- grad_value: float32 [2048, 1024], P(('dp', 'row'), 'col')
- grad_output: float32 [2048, 2048], P('col', ('dp', 'row'))
- grad_gate: float32 [2048, 8192], P(('dp', 'row'), 'col')
- grad_up: float32 [2048, 8192], P(('dp', 'row'), 'col')
- grad_down: float32 [8192, 2048], P('col', ('dp', 'row'))
The draws below stay inside these ranges and needn't reach their ends.
Inputs may be any that keep to these rules, and one draw needn't show every extreme that they name: lengths[s] counts the valid leading positions of sequence s; in every draw some sequence fills all 1024 positions.
All inputs are finite; a program needn't handle non-finite values.
Results may differ from the reference program's by a relative error of at most 0.025.
Values may be sent and summed in bfloat16 or wider, within the bound.
A program may use at most 192 MiB of HBM per device.

```python
import math
import jax
import jax.numpy as jnp
from jax import lax

MODEL_WIDTH = 2048
QUERY_HEADS = 8
KEY_VALUE_HEADS = 4
HEAD_SIZE = 256
FF = 8192
SEQUENCE_COUNT = 4
SEQUENCE_SLOT = 1024
TOKEN_COUNT = 4096


def draw_lengths(key, part):
    first, second = jax.random.split(jax.random.fold_in(key, 7))
    values = jax.random.randint(first, (SEQUENCE_COUNT,), SEQUENCE_SLOT // 4, SEQUENCE_SLOT + 1)
    chosen = jax.random.randint(second, (), 0, SEQUENCE_COUNT)
    return jnp.where(jnp.arange(SEQUENCE_COUNT) == chosen, SEQUENCE_SLOT, values).astype(jnp.int32)


def shard_levels(rng, shape, cuts, smallest, largest):
    level, own = 1.0, jax.random.fold_in(rng, 6)
    for dim, parts in cuts:
        heights = jnp.exp(jax.random.uniform(jax.random.fold_in(own, dim), (parts,), jnp.float32, smallest / len(cuts), largest / len(cuts)))
        level = level * jnp.repeat(heights, shape[dim] // parts).reshape([-1 if axis == dim else 1 for axis in range(len(shape))])
    return level


def gaussian(rng, shape, width, bound, shards=(), kind=jnp.bfloat16):
    gain = shard_levels(rng, shape, shards, -0.22, 0.18) if shards else 1.0
    values = jax.random.normal(rng, shape, jnp.float32) * width * gain
    return jnp.minimum(jnp.maximum(values, -bound), bound).astype(kind)


def setup_inputs(seed: int = 0) -> dict:
    streams_of = jax.random.split(jax.random.key(seed), 13)
    return {
        "tokens": gaussian(streams_of[0], (TOKEN_COUNT, MODEL_WIDTH), 1.0, 6.0, ((0, 8), (1, 4))),
        "w_query": gaussian(streams_of[1], (MODEL_WIDTH, QUERY_HEADS * HEAD_SIZE), MODEL_WIDTH ** -0.5, 0.125, ((0, 8), (1, 4))),
        "key_matrix": gaussian(streams_of[2], (MODEL_WIDTH, KEY_VALUE_HEADS * HEAD_SIZE), MODEL_WIDTH ** -0.5, 0.125, ((0, 8), (1, 4))),
        "value_matrix": gaussian(streams_of[3], (MODEL_WIDTH, KEY_VALUE_HEADS * HEAD_SIZE), MODEL_WIDTH ** -0.5, 0.125, ((0, 8), (1, 4))),
        "w_output": gaussian(streams_of[4], (QUERY_HEADS * HEAD_SIZE, MODEL_WIDTH), (QUERY_HEADS * HEAD_SIZE // 64) ** -0.5, 1.0, ((0, 4), (1, 8))),
        "w_gate": gaussian(streams_of[5], (MODEL_WIDTH, FF), MODEL_WIDTH ** -0.5, 0.125, ((0, 8), (1, 4))),
        "w_up": gaussian(streams_of[6], (MODEL_WIDTH, FF), MODEL_WIDTH ** -0.5, 0.125, ((0, 8), (1, 4))),
        "w_down": gaussian(streams_of[7], (FF, MODEL_WIDTH), FF ** -0.5, 0.0625, ((0, 4), (1, 8))),
        "gain_attn": jnp.clip(1.0 + 0.1 * jax.random.normal(streams_of[8], (MODEL_WIDTH,), jnp.float32), 0.5, 1.5).astype(jnp.bfloat16),
        "gain_ffn": jnp.clip(1.0 + 0.1 * jax.random.normal(streams_of[9], (MODEL_WIDTH,), jnp.float32), 0.5, 1.5).astype(jnp.bfloat16),
        "lengths": draw_lengths(jax.random.fold_in(streams_of[12], 71), 0),
        "cotangent": gaussian(streams_of[11], (TOKEN_COUNT, MODEL_WIDTH), 1.0, 6.0, ((0, 8), (1, 4))),
    }


EPSILON = 1e-06
ROPE_BASE = 1000042.0

@jax.custom_vjp
def lower_precision(v):
    return lax.optimization_barrier(v.astype(jnp.bfloat16)).astype(jnp.float32)

@jax.custom_vjp
def low_back(v):
    return v

def low_keep(v):
    return (lower_precision(v), None)

def low_pass(kept, grad):
    return (grad,)

def back_keep(v):
    return (v, None)

def back_low(kept, grad):
    return (lower_precision(grad),)
lower_precision.defvjp(low_keep, low_pass)
low_back.defvjp(back_keep, back_low)

def wide_dot(left, right):
    return jnp.dot(left, right, precision=lax.Precision.HIGHEST)

def rope_tables(positions):
    half = HEAD_SIZE // 2
    freq = ROPE_BASE ** (-jnp.arange(half, dtype=jnp.float32) * 2.0 / HEAD_SIZE)
    angle = positions[:, None] * freq[None, :]
    return (jnp.cos(angle), jnp.sin(angle))

def rotary_apply(values, cosine_table, sine_table):
    half = values.shape[-1] // 2
    first = values[..., :half]
    second = values[..., half:]
    cos_part = cosine_table[:, None, :]
    sin_part = sine_table[:, None, :]
    return jnp.concatenate([first * cos_part - second * sin_part, second * cos_part + first * sin_part], axis=-1)

def attend_block(query_tile_block, start, keys, values):
    token_count = query_tile_block.shape[0]
    query_rows = query_tile_block.reshape(token_count, KEY_VALUE_HEADS, QUERY_HEADS // KEY_VALUE_HEADS, HEAD_SIZE)
    raw_scores = jnp.einsum('qhgd,khd->hgqk', query_rows, keys, precision=lax.Precision.HIGHEST)
    scores = low_back(raw_scores / math.sqrt(HEAD_SIZE))
    query_pos = start + jnp.arange(token_count, dtype=jnp.int32)
    key_pos = jnp.arange(keys.shape[0], dtype=jnp.int32)
    scores = jnp.where(key_pos[None, :] <= query_pos[:, None], scores, -1e+30)
    log_total = jax.nn.logsumexp(scores, axis=-1, keepdims=True)
    probs = lower_precision(jnp.exp(scores - log_total))
    mixed_heads = jnp.einsum('hgqk,khd->qhgd', probs, values, precision=lax.Precision.HIGHEST)
    return mixed_heads.reshape(token_count, QUERY_HEADS * HEAD_SIZE)

def attend_sequence(query_rows, keys, values):
    size = min(512, SEQUENCE_SLOT)
    blocks = query_rows.reshape(SEQUENCE_SLOT // size, size, QUERY_HEADS, HEAD_SIZE)
    starts = jnp.arange(SEQUENCE_SLOT // size, dtype=jnp.int32) * size
    checked = jax.checkpoint(attend_block)

    def one_block(item):
        return checked(item[0], item[1], keys, values)
    mixed_heads = lax.map(one_block, (blocks, starts))
    return mixed_heads.reshape(SEQUENCE_SLOT, QUERY_HEADS * HEAD_SIZE)

def reference(tokens, w_query, key_matrix, value_matrix, w_output, w_gate, w_up, w_down, gain_attn, gain_ffn, lengths, cotangent):
    position = jnp.tile(jnp.arange(SEQUENCE_SLOT, dtype=jnp.int32), SEQUENCE_COUNT)
    sequence = jnp.repeat(jnp.arange(SEQUENCE_COUNT, dtype=jnp.int32), SEQUENCE_SLOT)
    valid = (position < lengths[sequence]).astype(jnp.float32)[:, None]
    cosine_table, sine_table = rope_tables(position.astype(jnp.float32))

    def layer(x_in, weight_query, weight_key, weight_value, weight_output, weight_gate, weight_up, weight_down, gain_one, gain_two):
        scale_one = lax.rsqrt(lax.optimization_barrier(jnp.mean(x_in * x_in, axis=1, keepdims=True)) + EPSILON)
        normed = lower_precision(x_in * scale_one * gain_one)
        query_raw = low_back(wide_dot(normed, weight_query))
        unrotated_key = low_back(wide_dot(normed, weight_key))
        all_values_packed = lower_precision(low_back(wide_dot(normed, weight_value)))
        all_queries_packed = lower_precision(rotary_apply(query_raw.reshape(TOKEN_COUNT, QUERY_HEADS, HEAD_SIZE), cosine_table, sine_table))
        all_keys_packed = lower_precision(rotary_apply(unrotated_key.reshape(TOKEN_COUNT, KEY_VALUE_HEADS, HEAD_SIZE), cosine_table, sine_table))

        def sequence_wise(item):
            return attend_sequence(item[0], item[1], item[2])
        mixed_heads = lax.map(sequence_wise, (all_queries_packed.reshape(SEQUENCE_COUNT, SEQUENCE_SLOT, QUERY_HEADS, HEAD_SIZE), all_keys_packed.reshape(SEQUENCE_COUNT, SEQUENCE_SLOT, KEY_VALUE_HEADS, HEAD_SIZE), all_values_packed.reshape(SEQUENCE_COUNT, SEQUENCE_SLOT, KEY_VALUE_HEADS, HEAD_SIZE)))
        mixed_heads = low_back(lower_precision(mixed_heads.reshape(TOKEN_COUNT, QUERY_HEADS * HEAD_SIZE) * valid))
        residual = low_back(x_in + wide_dot(mixed_heads, weight_output))
        scale_two = lax.rsqrt(lax.optimization_barrier(jnp.mean(residual * residual, axis=1, keepdims=True)) + EPSILON)
        normed_two = lower_precision(residual * scale_two * gain_two)
        gate = low_back(wide_dot(normed_two, weight_gate))
        upward = low_back(wide_dot(normed_two, weight_up))
        hidden = lower_precision(jax.nn.silu(gate) * upward)
        return residual + wide_dot(hidden, weight_down)
    floats = tuple((item.astype(jnp.float32) for item in (tokens, w_query, key_matrix, value_matrix, w_output, w_gate, w_up, w_down, gain_attn, gain_ffn)))
    layer_out, pullback = jax.vjp(layer, *floats)
    grads = pullback(cotangent.astype(jnp.float32) * valid)
    return (layer_out.astype(jnp.bfloat16), grads[0].astype(jnp.bfloat16), grads[8], grads[9], grads[1], grads[2], grads[3], grads[4], grads[5], grads[6], grads[7])
```

```python
import math

import jax
import jax.numpy as jnp
from jax import lax
from jax.sharding import PartitionSpec as P

QUERY_HEADS = 8
KEY_VALUE_HEADS = 4
HEAD_SIZE = 256


EPSILON = 1e-06
ROPE_BASE = 1000042.0


def rope_tables(positions):
    half = HEAD_SIZE // 2
    freq = ROPE_BASE ** (-jnp.arange(half, dtype=jnp.float32) * 2.0 / HEAD_SIZE)
    angle = positions[:, None] * freq[None, :]
    return (jnp.cos(angle), jnp.sin(angle))


def rotary_apply(values, cosine_table, sine_table):
    half = values.shape[-1] // 2
    first = values[..., :half]
    second = values[..., half:]
    cos_part = cosine_table[:, None, :]
    sin_part = sine_table[:, None, :]
    return jnp.concatenate(
        [first * cos_part - second * sin_part, second * cos_part + first * sin_part], axis=-1
    )


def rotate_back(grads, cosine_table, sine_table):
    half = grads.shape[-1] // 2
    first = grads[..., :half]
    second = grads[..., half:]
    cos_part = cosine_table[:, None, :]
    sin_part = sine_table[:, None, :]
    return jnp.concatenate(
        [first * cos_part + second * sin_part, second * cos_part - first * sin_part], axis=-1
    )


def norm_rows(full, gain):
    factor = lax.rsqrt(jnp.mean(full * full, axis=1, keepdims=True) + EPSILON)
    return (factor, (full * factor * gain).astype(jnp.bfloat16))


def norm_back(full, factor, gain, grad):
    inner = jnp.mean(gain * grad * full, axis=1, keepdims=True)
    back = factor * gain * grad - full * factor * factor * factor * inner
    gain_grad = jnp.sum(grad * full * factor, axis=0)
    return (back, gain_grad)


def contract_rows(left, right):
    return lax.dot_general(
        left, right, (((0,), (0,)), ((), ())), preferred_element_type=jnp.float32
    )


def times_transposed(left, right):
    return lax.dot_general(
        left, right, (((1,), (1,)), ((), ())), preferred_element_type=jnp.float32
    )


def masked_scores(query_rows, key_part, query_pos, index, key_block, score_scale):
    scores = (
        jnp.einsum("hgqd,khd->hgqk", query_rows, key_part, preferred_element_type=jnp.float32)
        * score_scale
    )
    key_pos = index * key_block + jnp.arange(key_block, dtype=jnp.int32)
    return jnp.where(key_pos[None, :] <= query_pos[:, None], scores, -1e30)


def attend(query_rows, keys, values, query_pos, key_block, score_scale):
    heads, query_group, token_count, size = query_rows.shape
    blocks = keys.shape[0] // key_block
    key_parts = keys.reshape(blocks, key_block, heads, size)
    value_parts = values.reshape(blocks, key_block, heads, size)
    indices = jnp.arange(blocks, dtype=jnp.int32)

    def totals(carry, item):
        top, total = carry
        key_part, index = item
        scores = masked_scores(query_rows, key_part, query_pos, index, key_block, score_scale)
        new_top = jnp.maximum(top, jnp.max(scores, axis=-1))
        total = total * jnp.exp(top - new_top) + jnp.sum(
            jnp.exp(scores - new_top[..., None]), axis=-1
        )
        return ((new_top, total), None)

    start = (
        jnp.full((heads, query_group, token_count), -1e30, jnp.float32),
        jnp.zeros((heads, query_group, token_count), jnp.float32),
    )
    (top, total), unused = lax.scan(totals, start, (key_parts, indices))
    log_total = top + jnp.log(total)

    def mixing(accum, item):
        key_part, value_part, index = item
        scores = masked_scores(query_rows, key_part, query_pos, index, key_block, score_scale)
        probs = jnp.exp(scores - log_total[..., None]).astype(jnp.bfloat16)
        return (
            accum
            + jnp.einsum("hgqk,khd->hgqd", probs, value_part, preferred_element_type=jnp.float32),
            None,
        )

    accum, unused = lax.scan(
        mixing,
        jnp.zeros((heads, query_group, token_count, size), jnp.float32),
        (key_parts, value_parts, indices),
    )
    return (accum, log_total)


def attend_back(
    query_rows, keys, values, query_pos, key_block, score_scale, log_total, delta, grad_out
):
    heads, query_group, token_count, size = query_rows.shape
    blocks = keys.shape[0] // key_block
    key_parts = keys.reshape(blocks, key_block, heads, size)
    value_parts = values.reshape(blocks, key_block, heads, size)

    def step(grad_query, item):
        key_part, value_part, index = item
        scores = masked_scores(query_rows, key_part, query_pos, index, key_block, score_scale)
        probs = jnp.exp(scores - log_total[..., None])
        probs_low = probs.astype(jnp.bfloat16)
        grad_probs = jnp.einsum(
            "hgqd,khd->hgqk", grad_out, value_part, preferred_element_type=jnp.float32
        )
        grad_scores = (probs * (grad_probs - delta[..., None]) * score_scale).astype(jnp.bfloat16)
        grad_query = grad_query + jnp.einsum(
            "hgqk,khd->hgqd", grad_scores, key_part, preferred_element_type=jnp.float32
        )
        grad_key = jnp.einsum(
            "hgqk,hgqd->khd", grad_scores, query_rows, preferred_element_type=jnp.float32
        )
        grad_value = jnp.einsum(
            "hgqk,hgqd->khd", probs_low, grad_out, preferred_element_type=jnp.float32
        )
        return (grad_query, (grad_key, grad_value))

    grad_query, (grad_keys, grad_values) = lax.scan(
        step,
        jnp.zeros((heads, query_group, token_count, size), jnp.float32),
        (key_parts, value_parts, jnp.arange(blocks, dtype=jnp.int32)),
    )
    return (
        grad_query,
        grad_keys.reshape(blocks * key_block, heads * size),
        grad_values.reshape(blocks * key_block, heads * size),
    )


def swap(value, axis, bit):
    size = lax.axis_size(axis)
    return lax.ppermute(value, axis, [(i, i ^ bit) for i in range(size)])


def gather_col(value):
    width = value.shape[1]
    far = swap(value, "col", 2)
    near = swap(jnp.concatenate([value, far], axis=1), "col", 1)
    return jnp.concatenate([value, near[:, :width], far, near[:, width:]], axis=1)


def scatter_col(value):
    width = value.shape[1] // 4
    part = [value[:, p * width : (p + 1) * width].astype(jnp.float32) for p in range(4)]
    low = jnp.bfloat16
    got = swap(jnp.concatenate([part[1], part[3]], axis=1).astype(low), "col", 1)
    keep_own = part[0] + got[:, :width].astype(jnp.float32)
    keep_far = part[2] + got[:, width:].astype(jnp.float32)
    return keep_own + swap(keep_far.astype(low), "col", 2).astype(jnp.float32)


def col_sum(value):
    value = value + swap(value, "col", 1)
    return value + swap(value, "col", 2)


def gather_row(value, axis):
    if lax.axis_size("row") == 2:
        other = swap(value, "row", 1)
        first = lax.axis_index("row") == 0
        return jnp.concatenate(
            [jnp.where(first, value, other), jnp.where(first, other, value)], axis=axis
        )
    return lax.all_gather(value, "row", axis=axis, tiled=True)


def scatter_row(value, axis):
    if lax.axis_size("row") == 2:
        me = lax.axis_index("row")
        mine = lax.dynamic_index_in_dim(value, me, axis, keepdims=False)
        theirs = lax.dynamic_index_in_dim(value, 1 - me, axis, keepdims=False)
        got = swap(theirs.astype(jnp.bfloat16), "row", 1)
        return mine.astype(jnp.float32) + got.astype(jnp.float32)
    value = lax.psum_scatter(value.astype(jnp.bfloat16), "row", scatter_dimension=axis, tiled=True)
    return jnp.squeeze(value, axis).astype(jnp.float32)


def reorder(blocks, shift):
    out = []
    for p in range(4):
        pick = blocks[p]
        for s in range(1, 4):
            pick = jnp.where(shift == s, blocks[p ^ s], pick)
        out.append(pick)
    return out


def gather_weight(local, shift):
    got = [local] + [swap(local, "dp", j) for j in range(1, 4)]
    full = gather_row(jnp.stack(reorder(got, shift))[:, None], 1)
    return full.reshape(-1, local.shape[1])


def exchange_weight(local, shift):
    me = lax.axis_index("dp")
    quarter = local.shape[1] // 4

    def part(j):
        return lax.dynamic_slice_in_dim(local, (me ^ j) * quarter, quarter, 1)

    got = [part(0)] + [swap(part(j), "dp", j) for j in range(1, 4)]
    full = gather_row(jnp.stack(reorder(got, shift))[:, None], 1)
    return full.reshape(-1, quarter)


def return_weight(grad, shift):
    rows, quarter = grad.shape
    row_size = lax.axis_size("row")
    own = scatter_row(grad.reshape(4, row_size, rows // (4 * row_size), quarter), 1)
    own = own.astype(jnp.bfloat16)
    sends = reorder([own[p] for p in range(4)], shift)
    got = [sends[0]] + [swap(sends[j], "dp", j) for j in range(1, 4)]
    natural = reorder(got, lax.axis_index("dp"))
    return jnp.concatenate(natural, axis=1).astype(jnp.float32)


def sum_weight(grad, shift):
    rows, width = grad.shape
    row_size = lax.axis_size("row")
    own = scatter_row(grad.reshape(4, row_size, rows // (4 * row_size), width), 1)
    sends = reorder([own[p] for p in range(4)], shift)
    total = sends[0]
    for j in range(1, 4):
        total = total + swap(sends[j].astype(jnp.bfloat16), "dp", j).astype(jnp.float32)
    return total


def gather_tokens(value):
    full = gather_col(
        jnp.concatenate([value] + [swap(value, "dp", j) for j in range(1, 4)], axis=0)
    )
    return full


def scatter_tokens(value):
    own = scatter_col(value)
    rows = own.shape[0] // 4
    total = own[:rows]
    for j in range(1, 4):
        total = total + swap(
            own[j * rows : (j + 1) * rows].astype(jnp.bfloat16), "dp", j
        ).astype(jnp.float32)
    return total


def per_device(
    tokens,
    w_query,
    key_matrix,
    value_matrix,
    w_output,
    w_gate,
    w_up,
    w_down,
    gain_attn,
    gain_ffn,
    lengths,
    cotangent,
):
    low = jnp.bfloat16
    wide = jnp.float32
    row_count, col_width = tokens.shape
    model_width = col_width * 4
    slot_size = row_count * lax.axis_size("row")
    key_block = min(512, slot_size)
    query_group = QUERY_HEADS // KEY_VALUE_HEADS
    score_scale = 1.0 / math.sqrt(HEAD_SIZE)
    me_dp, me_row, me_col = (lax.axis_index(name) for name in ("dp", "row", "col"))
    shift = me_dp ^ me_col
    query_pos = me_row * row_count + jnp.arange(row_count, dtype=jnp.int32)
    valid = (query_pos < lengths[0]).astype(wide)[:, None]
    cosine_table, sine_table = rope_tables(query_pos.astype(wide))

    gains = lax.all_gather(jnp.stack([gain_attn, gain_ffn]), ("dp", "row"), axis=1, tiled=True)
    gains = gains.reshape(2, 4, col_width)
    gains = jnp.concatenate(reorder([gains[:, p] for p in range(4)], me_col), axis=1)
    gain_one, gain_two = gains[0].astype(wide), gains[1].astype(wide)

    x_full = gather_col(tokens)
    q_cols, k_cols = w_query.shape[1], key_matrix.shape[1]
    attn_weight = gather_weight(
        jnp.concatenate([w_query, key_matrix, value_matrix], axis=1), shift
    )
    out_weight = gather_weight(w_output.T, shift)
    down_weight = exchange_weight(w_down.T, shift)
    gate_weight = exchange_weight(w_gate, shift)
    up_weight = exchange_weight(w_up, shift)
    x_wide = x_full.astype(wide)
    factor_one, normed = norm_rows(x_wide, gain_one)
    qkv = jnp.dot(normed, attn_weight, preferred_element_type=wide)
    kv_heads = k_cols // HEAD_SIZE
    query_rot = rotary_apply(
        qkv[:, :q_cols].reshape(row_count, kv_heads * query_group, HEAD_SIZE),
        cosine_table,
        sine_table,
    ).astype(low)
    key_rot = rotary_apply(
        qkv[:, q_cols : q_cols + k_cols].reshape(row_count, kv_heads, HEAD_SIZE),
        cosine_table,
        sine_table,
    ).astype(low)
    kv_all = gather_row(
        jnp.concatenate(
            [key_rot.reshape(row_count, k_cols), qkv[:, q_cols + k_cols :].astype(low)], axis=1
        ),
        0,
    )
    keys_all = kv_all[:, :k_cols].reshape(slot_size, kv_heads, HEAD_SIZE)
    values_all = kv_all[:, k_cols:].reshape(slot_size, kv_heads, HEAD_SIZE)
    query_rows = query_rot.reshape(row_count, kv_heads, query_group, HEAD_SIZE).transpose(
        1, 2, 0, 3
    )
    attended, log_total = attend(
        query_rows, keys_all, values_all, query_pos, key_block, score_scale
    )
    mixed_heads = (
        attended.transpose(2, 0, 1, 3).reshape(row_count, q_cols) * valid
    ).astype(low)
    residual = tokens.astype(wide) + scatter_col(times_transposed(mixed_heads, out_weight))

    grad_out = (cotangent.astype(wide) * valid).astype(low)
    residual_full = gather_tokens(residual.astype(low)).astype(wide)
    grad_out_full = gather_tokens(grad_out)
    factor_two, normed_two = norm_rows(residual_full, gain_two)
    gate = jnp.dot(normed_two, gate_weight, preferred_element_type=wide)
    upward = jnp.dot(normed_two, up_weight, preferred_element_type=wide)
    sigmoid_gate = jax.nn.sigmoid(gate)
    silu_gate = gate * sigmoid_gate
    hidden = (silu_gate * upward).astype(low)
    layer_out = (residual + scatter_tokens(times_transposed(hidden, down_weight))).astype(low)
    grad_hidden = jnp.dot(grad_out_full, down_weight, preferred_element_type=wide)
    grad_gate_act = (
        grad_hidden * upward * sigmoid_gate * (1.0 + gate * (1.0 - sigmoid_gate))
    ).astype(low)
    grad_up_act = (grad_hidden * silu_gate).astype(low)
    grad_down_part = contract_rows(grad_out_full, hidden)
    grad_gate_part = contract_rows(normed_two, grad_gate_act)
    grad_up_part = contract_rows(normed_two, grad_up_act)
    grad_normed_two = scatter_tokens(
        times_transposed(grad_gate_act, gate_weight) + times_transposed(grad_up_act, up_weight)
    )
    own_gain_two = gain_two[:col_width]
    own_factor_two = factor_two[:row_count]
    own_residual = residual_full[:row_count, :col_width]
    scaled = own_gain_two * grad_normed_two
    inner = col_sum(jnp.sum(scaled * own_residual, axis=1)[:, None]) / model_width
    grad_residual = (
        grad_out.astype(wide)
        + own_factor_two * scaled
        - own_residual * own_factor_two * own_factor_two * own_factor_two * inner
    ).astype(low)
    gain_two_grad = jnp.sum(grad_normed_two * own_residual * own_factor_two, axis=0)

    grad_residual_full = gather_col(grad_residual)
    grad_output_part = contract_rows(grad_residual_full, mixed_heads)
    grad_mixed = (
        jnp.dot(grad_residual_full, out_weight, preferred_element_type=wide) * valid
    ).astype(low)
    grad_heads = grad_mixed.reshape(row_count, kv_heads, query_group, HEAD_SIZE).transpose(
        1, 2, 0, 3
    )
    delta = jnp.sum(grad_heads.astype(wide) * attended, axis=-1)
    grad_query_rot, grad_keys_all, grad_values_all = attend_back(
        query_rows,
        keys_all,
        values_all,
        query_pos,
        key_block,
        score_scale,
        log_total,
        delta,
        grad_heads,
    )
    grad_kv = scatter_row(
        jnp.concatenate([grad_keys_all, grad_values_all], axis=1).reshape(
            slot_size // row_count, row_count, 2 * k_cols
        ),
        0,
    )
    grad_query_raw = (
        rotate_back(
            grad_query_rot.transpose(2, 0, 1, 3).reshape(
                row_count, kv_heads * query_group, HEAD_SIZE
            ),
            cosine_table,
            sine_table,
        )
        .reshape(row_count, q_cols)
        .astype(low)
    )
    grad_key_raw = (
        rotate_back(
            grad_kv[:, :k_cols].reshape(row_count, kv_heads, HEAD_SIZE), cosine_table, sine_table
        )
        .reshape(row_count, k_cols)
        .astype(low)
    )
    grad_raw = jnp.concatenate([grad_query_raw, grad_key_raw, grad_kv[:, k_cols:].astype(low)], axis=1)
    grad_attn_part = contract_rows(normed, grad_raw)
    grad_normed = scatter_col(times_transposed(grad_raw, attn_weight))
    own_gain_one = gain_one[:col_width]
    own_tokens = tokens.astype(wide)
    scaled = own_gain_one * grad_normed
    inner = col_sum(jnp.sum(scaled * own_tokens, axis=1)[:, None]) / model_width
    grad_tokens = (
        grad_residual.astype(wide)
        + factor_one * scaled
        - own_tokens * factor_one * factor_one * factor_one * inner
    ).astype(low)
    gain_one_grad = jnp.sum(grad_normed * own_tokens * factor_one, axis=0)

    gain_grads = jnp.zeros((2, model_width), wide)
    gain_grads = lax.dynamic_update_slice(
        gain_grads, jnp.stack([gain_one_grad, gain_two_grad]), (0, me_col * col_width)
    )
    gain_grads = lax.psum(gain_grads, ("dp", "row", "col"))
    own = gain_attn.shape[0]
    gain_grads = lax.dynamic_slice_in_dim(
        gain_grads, (me_dp * lax.axis_size("row") + me_row) * own, own, 1
    )
    grad_attn = sum_weight(grad_attn_part, shift)
    return (
        layer_out,
        grad_tokens,
        gain_grads[0],
        gain_grads[1],
        grad_attn[:, :q_cols],
        grad_attn[:, q_cols : q_cols + k_cols],
        grad_attn[:, q_cols + k_cols :],
        sum_weight(grad_output_part, shift).T,
        return_weight(grad_gate_part, shift),
        return_weight(grad_up_part, shift),
        return_weight(grad_down_part, shift).T,
    )


def solution(mesh):
    in_specs = (
        P(("dp", "row"), "col"),
        P(("dp", "row"), "col"),
        P(("dp", "row"), "col"),
        P(("dp", "row"), "col"),
        P("col", ("dp", "row")),
        P(("dp", "row"), "col"),
        P(("dp", "row"), "col"),
        P("col", ("dp", "row")),
        P(("dp", "row")),
        P(("dp", "row")),
        P("dp"),
        P(("dp", "row"), "col"),
    )
    out_specs = (
        P(("dp", "row"), "col"),
        P(("dp", "row"), "col"),
        P(("dp", "row")),
        P(("dp", "row")),
        P(("dp", "row"), "col"),
        P(("dp", "row"), "col"),
        P(("dp", "row"), "col"),
        P("col", ("dp", "row")),
        P(("dp", "row"), "col"),
        P(("dp", "row"), "col"),
        P("col", ("dp", "row")),
    )
    return jax.shard_map(
        per_device, mesh=mesh, in_specs=in_specs, out_specs=out_specs, check_vma=False
    )
```

```python
import math

import jax
import jax.numpy as jnp
from jax import lax
from jax.experimental import pallas as pl
from jax.experimental.pallas import tpu as pltpu
from jax.sharding import PartitionSpec as P

QUERY_HEADS = 8
KEY_VALUE_HEADS = 4
HEAD_SIZE = 256


EPSILON = 1e-06
ROPE_BASE = 1000042.0


def rope_tables(positions):
    half = HEAD_SIZE // 2
    freq = ROPE_BASE ** (-jnp.arange(half, dtype=jnp.float32) * 2.0 / HEAD_SIZE)
    angle = positions[:, None] * freq[None, :]
    return (jnp.cos(angle), jnp.sin(angle))


def rotary_apply(values, cosine_table, sine_table):
    half = values.shape[-1] // 2
    first = values[..., :half]
    second = values[..., half:]
    cos_part = cosine_table[:, None, :]
    sin_part = sine_table[:, None, :]
    return jnp.concatenate(
        [first * cos_part - second * sin_part, second * cos_part + first * sin_part], axis=-1
    )


def rotate_back(grads, cosine_table, sine_table):
    half = grads.shape[-1] // 2
    first = grads[..., :half]
    second = grads[..., half:]
    cos_part = cosine_table[:, None, :]
    sin_part = sine_table[:, None, :]
    return jnp.concatenate(
        [first * cos_part + second * sin_part, second * cos_part - first * sin_part], axis=-1
    )


def norm_rows(full, gain):
    factor = lax.rsqrt(jnp.mean(full * full, axis=1, keepdims=True) + EPSILON)
    return (factor, (full * factor * gain).astype(jnp.bfloat16))


def norm_back(full, factor, gain, grad):
    inner = jnp.mean(gain * grad * full, axis=1, keepdims=True)
    back = factor * gain * grad - full * factor * factor * factor * inner
    gain_grad = jnp.sum(grad * full * factor, axis=0)
    return (back, gain_grad)


def contract_rows(left, right):
    return lax.dot_general(
        left, right, (((0,), (0,)), ((), ())), preferred_element_type=jnp.float32
    )


def times_transposed(left, right):
    return lax.dot_general(
        left, right, (((1,), (1,)), ((), ())), preferred_element_type=jnp.float32
    )


def masked_scores(query_rows, key_part, query_pos, index, key_block, score_scale):
    scores = (
        jnp.einsum("hgqd,khd->hgqk", query_rows, key_part, preferred_element_type=jnp.float32)
        * score_scale
    )
    key_pos = index * key_block + jnp.arange(key_block, dtype=jnp.int32)
    return jnp.where(key_pos[None, :] <= query_pos[:, None], scores, -1e30)


def attend(query_rows, keys, values, query_pos, key_block, score_scale):
    heads, query_group, token_count, size = query_rows.shape
    blocks = keys.shape[0] // key_block
    key_parts = keys.reshape(blocks, key_block, heads, size)
    value_parts = values.reshape(blocks, key_block, heads, size)
    indices = jnp.arange(blocks, dtype=jnp.int32)

    def totals(carry, item):
        top, total = carry
        key_part, index = item
        scores = masked_scores(query_rows, key_part, query_pos, index, key_block, score_scale)
        new_top = jnp.maximum(top, jnp.max(scores, axis=-1))
        total = total * jnp.exp(top - new_top) + jnp.sum(
            jnp.exp(scores - new_top[..., None]), axis=-1
        )
        return ((new_top, total), None)

    start = (
        jnp.full((heads, query_group, token_count), -1e30, jnp.float32),
        jnp.zeros((heads, query_group, token_count), jnp.float32),
    )
    (top, total), unused = lax.scan(totals, start, (key_parts, indices))
    log_total = top + jnp.log(total)

    def mixing(accum, item):
        key_part, value_part, index = item
        scores = masked_scores(query_rows, key_part, query_pos, index, key_block, score_scale)
        probs = jnp.exp(scores - log_total[..., None]).astype(jnp.bfloat16)
        return (
            accum
            + jnp.einsum("hgqk,khd->hgqd", probs, value_part, preferred_element_type=jnp.float32),
            None,
        )

    accum, unused = lax.scan(
        mixing,
        jnp.zeros((heads, query_group, token_count, size), jnp.float32),
        (key_parts, value_parts, indices),
    )
    return (accum, log_total)


def attend_back(
    query_rows, keys, values, query_pos, key_block, score_scale, log_total, delta, grad_out
):
    heads, query_group, token_count, size = query_rows.shape
    blocks = keys.shape[0] // key_block
    key_parts = keys.reshape(blocks, key_block, heads, size)
    value_parts = values.reshape(blocks, key_block, heads, size)

    def step(grad_query, item):
        key_part, value_part, index = item
        scores = masked_scores(query_rows, key_part, query_pos, index, key_block, score_scale)
        probs = jnp.exp(scores - log_total[..., None])
        probs_low = probs.astype(jnp.bfloat16)
        grad_probs = jnp.einsum(
            "hgqd,khd->hgqk", grad_out, value_part, preferred_element_type=jnp.float32
        )
        grad_scores = (probs * (grad_probs - delta[..., None]) * score_scale).astype(jnp.bfloat16)
        grad_query = grad_query + jnp.einsum(
            "hgqk,khd->hgqd", grad_scores, key_part, preferred_element_type=jnp.float32
        )
        grad_key = jnp.einsum(
            "hgqk,hgqd->khd", grad_scores, query_rows, preferred_element_type=jnp.float32
        )
        grad_value = jnp.einsum(
            "hgqk,hgqd->khd", probs_low, grad_out, preferred_element_type=jnp.float32
        )
        return (grad_query, (grad_key, grad_value))

    grad_query, (grad_keys, grad_values) = lax.scan(
        step,
        jnp.zeros((heads, query_group, token_count, size), jnp.float32),
        (key_parts, value_parts, jnp.arange(blocks, dtype=jnp.int32)),
    )
    return (
        grad_query,
        grad_keys.reshape(blocks * key_block, heads * size),
        grad_values.reshape(blocks * key_block, heads * size),
    )


def swap(value, axis, bit):
    size = lax.axis_size(axis)
    return lax.ppermute(value, axis, [(i, i ^ bit) for i in range(size)])


def gather_col(value):
    width = value.shape[1]
    far = swap(value, "col", 2)
    near = swap(jnp.concatenate([value, far], axis=1), "col", 1)
    return jnp.concatenate([value, near[:, :width], far, near[:, width:]], axis=1)


def scatter_col(value):
    width = value.shape[1] // 4
    part = [value[:, p * width : (p + 1) * width].astype(jnp.float32) for p in range(4)]
    low = jnp.bfloat16
    got = swap(jnp.concatenate([part[1], part[3]], axis=1).astype(low), "col", 1)
    keep_own = part[0] + got[:, :width].astype(jnp.float32)
    keep_far = part[2] + got[:, width:].astype(jnp.float32)
    return keep_own + swap(keep_far.astype(low), "col", 2).astype(jnp.float32)


def col_sum(value):
    value = value + swap(value, "col", 1)
    return value + swap(value, "col", 2)


def gather_row(value, axis):
    if lax.axis_size("row") == 2:
        other = swap(value, "row", 1)
        first = lax.axis_index("row") == 0
        return jnp.concatenate(
            [jnp.where(first, value, other), jnp.where(first, other, value)], axis=axis
        )
    return lax.all_gather(value, "row", axis=axis, tiled=True)


def scatter_row(value, axis):
    if lax.axis_size("row") == 2:
        me = lax.axis_index("row")
        mine = lax.dynamic_index_in_dim(value, me, axis, keepdims=False)
        theirs = lax.dynamic_index_in_dim(value, 1 - me, axis, keepdims=False)
        got = swap(theirs.astype(jnp.bfloat16), "row", 1)
        return mine.astype(jnp.float32) + got.astype(jnp.float32)
    value = lax.psum_scatter(value.astype(jnp.bfloat16), "row", scatter_dimension=axis, tiled=True)
    return jnp.squeeze(value, axis).astype(jnp.float32)


def reorder(blocks, shift):
    out = []
    for p in range(4):
        pick = blocks[p]
        for s in range(1, 4):
            pick = jnp.where(shift == s, blocks[p ^ s], pick)
        out.append(pick)
    return out


def gather_weight(local, shift):
    got = [local] + [swap(local, "dp", j) for j in range(1, 4)]
    full = gather_row(jnp.stack(reorder(got, shift))[:, None], 1)
    return full.reshape(-1, local.shape[1])


def exchange_weight(local, shift):
    me = lax.axis_index("dp")
    quarter = local.shape[1] // 4

    def part(j):
        return lax.dynamic_slice_in_dim(local, (me ^ j) * quarter, quarter, 1)

    got = [part(0)] + [swap(part(j), "dp", j) for j in range(1, 4)]
    full = gather_row(jnp.stack(reorder(got, shift))[:, None], 1)
    return full.reshape(-1, quarter)


def return_weight(grad, shift):
    rows, quarter = grad.shape
    row_size = lax.axis_size("row")
    own = scatter_row(grad.reshape(4, row_size, rows // (4 * row_size), quarter), 1)
    own = own.astype(jnp.bfloat16)
    sends = reorder([own[p] for p in range(4)], shift)
    got = [sends[0]] + [swap(sends[j], "dp", j) for j in range(1, 4)]
    natural = reorder(got, lax.axis_index("dp"))
    return jnp.concatenate(natural, axis=1).astype(jnp.float32)


def sum_weight(grad, shift):
    rows, width = grad.shape
    row_size = lax.axis_size("row")
    own = scatter_row(grad.reshape(4, row_size, rows // (4 * row_size), width), 1)
    sends = reorder([own[p] for p in range(4)], shift)
    total = sends[0]
    for j in range(1, 4):
        total = total + swap(sends[j].astype(jnp.bfloat16), "dp", j).astype(jnp.float32)
    return total


def gather_tokens(value):
    full = gather_col(
        jnp.concatenate([value] + [swap(value, "dp", j) for j in range(1, 4)], axis=0)
    )
    return full


def scatter_tokens(value):
    own = scatter_col(value)
    rows = own.shape[0] // 4
    total = own[:rows]
    for j in range(1, 4):
        total = total + swap(
            own[j * rows : (j + 1) * rows].astype(jnp.bfloat16), "dp", j
        ).astype(jnp.float32)
    return total


def dot_nn(left, right):
    return lax.dot_general(left, right, (((1,), (0,)), ((), ())), preferred_element_type=jnp.float32)


def tiles(count, size, body):
    def step(i, unused):
        body(pl.ds(pl.multiple_of(i * size, size), size))
        return unused

    lax.fori_loop(0, count // size, step, 0)


def remote(src, dst, send_sem, recv_sem, target):
    return pltpu.make_async_remote_copy(
        src_ref=src,
        dst_ref=dst,
        send_sem=send_sem,
        recv_sem=recv_sem,
        device_id=target,
        device_id_type=pl.DeviceIdType.MESH,
    )


def greet(targets):
    barrier = pltpu.get_barrier_semaphore()
    for target in targets:
        pl.semaphore_signal(
            barrier, inc=1, device_id=target, device_id_type=pl.DeviceIdType.MESH
        )
    pl.semaphore_wait(barrier, len(targets))


def ffn_kernel(
    h_ref,
    gain_ref,
    do_hbm,
    wg_hbm,
    wu_hbm,
    wd_hbm,
    dhn_ref,
    factor_ref,
    out_hbm,
    dwg_hbm,
    dwu_hbm,
    dwd_hbm,
    full,
    do,
    wg,
    wu,
    wd,
    hid,
    dg,
    du,
    gate,
    up,
    dhid,
    part,
    outp,
    core_in,
    x_out,
    x_in,
    z_out,
    z_in,
    stage,
    load_sem,
    z_send,
    f_send,
    z_recv,
    x_send,
    x_recv,
    c_send,
    c_recv,
    p_send,
    p_recv,
    rx_send,
    rx_recv,
    rz_send,
    rz_recv,
    o_sem,
    s_sem,
):
    rows, width = h_ref.shape
    model = width * 4
    hidden = wg.shape[1]
    low, wide = jnp.bfloat16, jnp.float32
    z, col = lax.axis_index("dp"), lax.axis_index("col")
    core, far = {"col": col ^ 1}, {"col": col ^ 2}
    mid = jnp.logical_and(z > 0, z < 3)

    def chunk(s):
        return jnp.where(jnp.logical_and(mid, s >= 2), 5 - s, s)

    def cols(p):
        return pl.ds(p * width, width)

    greet([{"dp": z ^ 1}, {"dp": z ^ 2}, {"dp": z ^ 3}, core, far])

    def z_own(target, index):
        slot = z ^ target
        return remote(
            h_ref, full.at[slot, :, cols(0)], z_send.at[index], z_recv.at[slot], {"dp": target}
        )

    @pl.when(z < 3)
    def _():
        z_own(z + 1, 0).start()

    @pl.when(z > 0)
    def _():
        z_own(z - 1, 1).start()

    def x_copy(j, src):
        return remote(src, full.at[j, :, cols(2)], x_send.at[j], x_recv.at[j], far)

    def c_copy(j, src, which):
        return remote(
            src, full.at[j, :, cols(1 + 2 * which)], c_send.at[which, j], c_recv.at[which, j], core
        )

    x_copy(0, h_ref).start()
    c_copy(0, h_ref, 0).start()
    loads = [
        pltpu.make_async_copy(wg_hbm, wg, load_sem.at[0]),
        pltpu.make_async_copy(wu_hbm, wu, load_sem.at[1]),
        pltpu.make_async_copy(wd_hbm, wd, load_sem.at[2]),
    ]
    for load in loads:
        load.start()

    def do_load(j):
        return pltpu.make_async_copy(do_hbm.at[j], do.at[j], load_sem.at[3 + j])

    for j in range(4):
        do_load(j).start()

    def copy_own(r):
        full[0, r, 0:width] = h_ref[r, :]

    tiles(rows, 64, copy_own)

    def forward(j, target):
        return remote(
            full.at[j, :, cols(0)],
            full.at[(z ^ j) ^ target, :, cols(0)],
            f_send.at[j],
            z_recv.at[(z ^ j) ^ target],
            {"dp": target},
        )

    def goes_up(j):
        return jnp.logical_and((z ^ j) < z, z < 3)

    def goes_down(j):
        return jnp.logical_and((z ^ j) > z, z > 0)

    def arrive(j):
        block = full.at[j, :, cols(0)]
        remote(block, block, f_send.at[j], z_recv.at[j], core).wait_recv()

        @pl.when(goes_up(j))
        def _():
            forward(j, z + 1).start()

        @pl.when(goes_down(j))
        def _():
            forward(j, z - 1).start()

        x_copy(j, block).start()
        c_copy(j, block, 0).start()

    def settle(j):
        block = full.at[j, :, cols(0)]
        x_copy(j, block).wait_recv()
        c_copy(j, full.at[j, :, cols(2)], 1).start()
        x_copy(j, block).wait_send()
        c_copy(j, block, 0).wait_send()

        @pl.when(jnp.logical_and(j > 0, jnp.logical_or(goes_up(j), goes_down(j))))
        def _():
            forward(j, z ^ j).wait_send()

        c_copy(j, block, 0).wait_recv()
        c_copy(j, block, 1).wait()

    def part_copy(s, slot):
        return remote(
            part.at[slot, :, pl.ds(2 * width, 2 * width)],
            core_in.at[s],
            p_send.at[s],
            p_recv.at[s],
            core,
        )

    def rx_copy(s):
        return remote(x_out.at[s], x_in.at[s], rx_send.at[s], rx_recv.at[s], far)

    def rz_copy(s, j):
        return remote(z_out.at[s], z_in.at[j], rz_send.at[s], rz_recv.at[j], {"dp": z ^ j})

    def reduce_core(s):
        slot = lax.rem(s, 2)
        part_copy(s, slot).wait()

        def add(r):
            x_out[s, r, :] = (
                part[slot, r, width : 2 * width].astype(wide)
                + core_in[s, r, width : 2 * width].astype(wide)
            ).astype(low)
            z_out[s, r, :] = (
                part[slot, r, 0:width].astype(wide) + core_in[s, r, 0:width].astype(wide)
            ).astype(low)

        tiles(rows, 64, add)
        rx_copy(s).start()

    def reduce_far(s):
        rx_copy(s).wait()

        def add(r):
            z_out[s, r, :] = (z_out[s, r, :].astype(wide) + x_in[s, r, :].astype(wide)).astype(low)

        tiles(rows, 64, add)

        @pl.when(s > 0)
        def _():
            rz_copy(s, chunk(s)).start()

    def out_copy(s):
        return pltpu.make_async_copy(
            outp.at[lax.rem(s, 2)], out_hbm.at[chunk(s)], o_sem.at[lax.rem(s, 2)]
        )

    def step(s, unused):
        j = chunk(s)
        base = s * rows

        @pl.when(jnp.logical_and(s < 3, jnp.logical_not(jnp.logical_and(s == 1, mid))))
        def _():
            arrive(chunk(s + 1))

        @pl.when(jnp.logical_and(s == 0, mid))
        def _():
            arrive(chunk(2))

        settle(j)

        def norm(r):
            x = full[j, r, :].astype(wide)
            factor = lax.rsqrt(jnp.sum(x * x, axis=1, keepdims=True) * (1.0 / model) + EPSILON)
            full[j, r, :] = (x * factor * gain_ref[...]).astype(low)

            @pl.when(s == 0)
            def _():
                factor_ref[r, :] = jnp.broadcast_to(factor, (factor.shape[0], 128))

        tiles(rows, 32, norm)

        @pl.when(s == 0)
        def _():
            for load in loads:
                load.wait()

        gate[...] = dot_nn(full[j], wg[...])
        up[...] = dot_nn(full[j], wu[...])

        @pl.when(s > 0)
        def _():
            reduce_core(s - 1)

        do_load(j).wait()
        dhid[...] = dot_nn(do[j], wd[...])

        def act(r):
            g = gate[r, :]
            u = up[r, :]
            d = dhid[r, :]
            sig = jax.nn.sigmoid(g)
            silu = g * sig
            at = pl.ds(pl.multiple_of(base + r.start, 64), 64)
            hid[at, :] = (silu * u).astype(low)
            dg[at, :] = (d * u * sig * (1.0 + g * (1.0 - sig))).astype(low)
            du[at, :] = (d * silu).astype(low)

        tiles(rows, 64, act)
        slot = lax.rem(s, 2)
        mine = pl.ds(pl.multiple_of(base, rows), rows)

        def dhn(q, p):
            w_rows = slice(p * width, (p + 1) * width)
            part[slot, :, q * width : (q + 1) * width] = (
                times_transposed(dg[mine, :], wg[w_rows, :])
                + times_transposed(du[mine, :], wu[w_rows, :])
            ).astype(low)

        dhn(2, 1)
        dhn(3, 3)
        dhn(0, 0)
        part_copy(s, slot).start()
        dhn(1, 2)

        @pl.when(s > 0)
        def _():
            reduce_far(s - 1)

        @pl.when(s >= 2)
        def _():
            out_copy(s - 2).wait()

        for p in range(4):
            outp[slot, :, p * width : (p + 1) * width] = times_transposed(
                hid[mine, :], wd[p * width : (p + 1) * width, :]
            ).astype(low)
        out_copy(s).start()
        return unused

    lax.fori_loop(0, 4, step, 0)

    reduce_core(3)
    count = model // width

    def stage_copy(target, i, slot):
        at = pl.ds(pl.multiple_of(i * width, width), width)
        return pltpu.make_async_copy(stage.at[slot], target.at[at, :], s_sem.at[slot])

    def weight_grad(target, right, left_of, first):
        def tile(i, unused):
            slot = lax.rem(i, 2)

            @pl.when(jnp.logical_or(i >= 2, not first))
            def _():
                stage_copy(target, 0, slot).wait()

            total = left_of(0, i, right)
            for s in range(1, 4):
                total = total + left_of(s, i, right)
            stage[slot] = total.astype(low)
            stage_copy(target, i, slot).start()
            return unused

        lax.fori_loop(0, count, tile, 0)

    def from_full(s, i, right):
        at = pl.ds(pl.multiple_of(i * width, width), width)
        return contract_rows(full[chunk(s), :, at], right[s * rows : (s + 1) * rows, :])

    def from_do(s, i, right):
        at = pl.ds(pl.multiple_of(i * width, width), width)
        return contract_rows(do[chunk(s), :, at], right[s * rows : (s + 1) * rows, :])

    weight_grad(dwg_hbm, dg, from_full, True)
    reduce_far(3)
    weight_grad(dwu_hbm, du, from_full, False)
    weight_grad(dwd_hbm, hid, from_do, False)
    stage_copy(dwd_hbm, 0, 0).wait()
    stage_copy(dwd_hbm, 0, 1).wait()
    out_copy(2).wait()
    out_copy(3).wait()
    for s in range(1, 4):
        rz_copy(s, chunk(s)).wait()

    def final(r):
        total = z_out[0, r, :].astype(wide)
        for j in range(1, 4):
            total = total + z_in[j, r, :].astype(wide)
        dhn_ref[r, :] = total

    tiles(rows, 64, final)

    @pl.when(z < 3)
    def _():
        z_own(z + 1, 0).wait_send()

    @pl.when(z > 0)
    def _():
        z_own(z - 1, 1).wait_send()


def ffn_call(h_low, gain, grad_full, wg, wu, wd):
    rows, width = h_low.shape
    model, hidden = wg.shape
    low, wide = jnp.bfloat16, jnp.float32
    vmem = pl.BlockSpec(memory_space=pltpu.VMEM)
    hbm = pl.BlockSpec(memory_space=pl.ANY)
    dma = pltpu.SemaphoreType.DMA
    tokens = 4 * rows
    return pl.pallas_call(
        ffn_kernel,
        out_shape=(
            jax.ShapeDtypeStruct((rows, width), wide),
            jax.ShapeDtypeStruct((rows, 128), wide),
            jax.ShapeDtypeStruct((4, rows, model), low),
            jax.ShapeDtypeStruct((model, hidden), low),
            jax.ShapeDtypeStruct((model, hidden), low),
            jax.ShapeDtypeStruct((model, hidden), low),
        ),
        in_specs=[vmem, vmem, hbm, hbm, hbm, hbm],
        out_specs=(vmem, vmem, hbm, hbm, hbm, hbm),
        scratch_shapes=[
            pltpu.VMEM((4, rows, model), low),
            pltpu.VMEM((4, rows, model), low),
            pltpu.VMEM((model, hidden), low),
            pltpu.VMEM((model, hidden), low),
            pltpu.VMEM((model, hidden), low),
            pltpu.VMEM((tokens, hidden), low),
            pltpu.VMEM((tokens, hidden), low),
            pltpu.VMEM((tokens, hidden), low),
            pltpu.VMEM((rows, hidden), wide),
            pltpu.VMEM((rows, hidden), wide),
            pltpu.VMEM((rows, hidden), wide),
            pltpu.VMEM((2, rows, model), low),
            pltpu.VMEM((2, rows, model), low),
            pltpu.VMEM((4, rows, 2 * width), low),
            pltpu.VMEM((4, rows, width), low),
            pltpu.VMEM((4, rows, width), low),
            pltpu.VMEM((4, rows, width), low),
            pltpu.VMEM((4, rows, width), low),
            pltpu.VMEM((2, width, hidden), low),
            dma((7,)),
            dma((2,)),
            dma((4,)),
            dma((4,)),
            dma((4,)),
            dma((4,)),
            dma((2, 4)),
            dma((2, 4)),
            dma((4,)),
            dma((4,)),
            dma((4,)),
            dma((4,)),
            dma((4,)),
            dma((4,)),
            dma((2,)),
            dma((2,)),
        ],
        compiler_params=pltpu.CompilerParams(
            collective_id=2, has_side_effects=True, vmem_limit_bytes=66_000_000
        ),
        cost_estimate=pl.CostEstimate(
            flops=18 * tokens * model * hidden,
            bytes_accessed=40_000_000,
            transcendentals=tokens * hidden,
        ),
    )(h_low, gain, grad_full, wg, wu, wd)


def per_device(
    tokens,
    w_query,
    key_matrix,
    value_matrix,
    w_output,
    w_gate,
    w_up,
    w_down,
    gain_attn,
    gain_ffn,
    lengths,
    cotangent,
):
    low = jnp.bfloat16
    wide = jnp.float32
    row_count, col_width = tokens.shape
    model_width = col_width * 4
    slot_size = row_count * lax.axis_size("row")
    key_block = min(512, slot_size)
    query_group = QUERY_HEADS // KEY_VALUE_HEADS
    score_scale = 1.0 / math.sqrt(HEAD_SIZE)
    me_dp, me_row, me_col = (lax.axis_index(name) for name in ("dp", "row", "col"))
    shift = me_dp ^ me_col
    query_pos = me_row * row_count + jnp.arange(row_count, dtype=jnp.int32)
    valid = (query_pos < lengths[0]).astype(wide)[:, None]
    cosine_table, sine_table = rope_tables(query_pos.astype(wide))

    gains = lax.all_gather(jnp.stack([gain_attn, gain_ffn]), ("dp", "row"), axis=1, tiled=True)
    gains = gains.reshape(2, 4, col_width)
    gains = jnp.concatenate(reorder([gains[:, p] for p in range(4)], me_col), axis=1)
    gain_one, gain_two = gains[0].astype(wide), gains[1].astype(wide)

    x_full = gather_col(tokens)
    q_cols, k_cols = w_query.shape[1], key_matrix.shape[1]
    attn_weight = gather_weight(
        jnp.concatenate([w_query, key_matrix, value_matrix], axis=1), shift
    )
    out_weight = gather_weight(w_output.T, shift)
    down_weight = exchange_weight(w_down.T, shift)
    gate_weight = exchange_weight(w_gate, shift)
    up_weight = exchange_weight(w_up, shift)
    x_wide = x_full.astype(wide)
    factor_one, normed = norm_rows(x_wide, gain_one)
    qkv = jnp.dot(normed, attn_weight, preferred_element_type=wide)
    kv_heads = k_cols // HEAD_SIZE
    query_rot = rotary_apply(
        qkv[:, :q_cols].reshape(row_count, kv_heads * query_group, HEAD_SIZE),
        cosine_table,
        sine_table,
    ).astype(low)
    key_rot = rotary_apply(
        qkv[:, q_cols : q_cols + k_cols].reshape(row_count, kv_heads, HEAD_SIZE),
        cosine_table,
        sine_table,
    ).astype(low)
    kv_all = gather_row(
        jnp.concatenate(
            [key_rot.reshape(row_count, k_cols), qkv[:, q_cols + k_cols :].astype(low)], axis=1
        ),
        0,
    )
    keys_all = kv_all[:, :k_cols].reshape(slot_size, kv_heads, HEAD_SIZE)
    values_all = kv_all[:, k_cols:].reshape(slot_size, kv_heads, HEAD_SIZE)
    query_rows = query_rot.reshape(row_count, kv_heads, query_group, HEAD_SIZE).transpose(
        1, 2, 0, 3
    )
    attended, log_total = attend(
        query_rows, keys_all, values_all, query_pos, key_block, score_scale
    )
    mixed_heads = (
        attended.transpose(2, 0, 1, 3).reshape(row_count, q_cols) * valid
    ).astype(low)
    residual = tokens.astype(wide) + scatter_col(times_transposed(mixed_heads, out_weight))

    grad_out = (cotangent.astype(wide) * valid).astype(low)
    grad_out_full = gather_tokens(grad_out).reshape(4, row_count, model_width)
    residual_low = residual.astype(low)
    grad_normed_two, factor_two, out_part, grad_gate_part, grad_up_part, grad_down_part = ffn_call(
        residual_low, gain_two[None], grad_out_full, gate_weight, up_weight, down_weight
    )
    layer_out = (residual + scatter_tokens(out_part.reshape(-1, model_width))).astype(low)
    own_gain_two = gain_two[:col_width]
    own_factor_two = factor_two[:, :1]
    own_residual = residual_low.astype(wide)
    scaled = own_gain_two * grad_normed_two
    inner = col_sum(jnp.sum(scaled * own_residual, axis=1)[:, None]) / model_width
    grad_residual = (
        grad_out.astype(wide)
        + own_factor_two * scaled
        - own_residual * own_factor_two * own_factor_two * own_factor_two * inner
    ).astype(low)
    gain_two_grad = jnp.sum(grad_normed_two * own_residual * own_factor_two, axis=0)

    grad_residual_full = gather_col(grad_residual)
    grad_output_part = contract_rows(grad_residual_full, mixed_heads)
    grad_mixed = (
        jnp.dot(grad_residual_full, out_weight, preferred_element_type=wide) * valid
    ).astype(low)
    grad_heads = grad_mixed.reshape(row_count, kv_heads, query_group, HEAD_SIZE).transpose(
        1, 2, 0, 3
    )
    delta = jnp.sum(grad_heads.astype(wide) * attended, axis=-1)
    grad_query_rot, grad_keys_all, grad_values_all = attend_back(
        query_rows,
        keys_all,
        values_all,
        query_pos,
        key_block,
        score_scale,
        log_total,
        delta,
        grad_heads,
    )
    grad_kv = scatter_row(
        jnp.concatenate([grad_keys_all, grad_values_all], axis=1).reshape(
            slot_size // row_count, row_count, 2 * k_cols
        ),
        0,
    )
    grad_query_raw = (
        rotate_back(
            grad_query_rot.transpose(2, 0, 1, 3).reshape(
                row_count, kv_heads * query_group, HEAD_SIZE
            ),
            cosine_table,
            sine_table,
        )
        .reshape(row_count, q_cols)
        .astype(low)
    )
    grad_key_raw = (
        rotate_back(
            grad_kv[:, :k_cols].reshape(row_count, kv_heads, HEAD_SIZE), cosine_table, sine_table
        )
        .reshape(row_count, k_cols)
        .astype(low)
    )
    grad_raw = jnp.concatenate([grad_query_raw, grad_key_raw, grad_kv[:, k_cols:].astype(low)], axis=1)
    grad_attn_part = contract_rows(normed, grad_raw)
    grad_normed = scatter_col(times_transposed(grad_raw, attn_weight))
    own_gain_one = gain_one[:col_width]
    own_tokens = tokens.astype(wide)
    scaled = own_gain_one * grad_normed
    inner = col_sum(jnp.sum(scaled * own_tokens, axis=1)[:, None]) / model_width
    grad_tokens = (
        grad_residual.astype(wide)
        + factor_one * scaled
        - own_tokens * factor_one * factor_one * factor_one * inner
    ).astype(low)
    gain_one_grad = jnp.sum(grad_normed * own_tokens * factor_one, axis=0)

    gain_grads = jnp.zeros((2, model_width), wide)
    gain_grads = lax.dynamic_update_slice(
        gain_grads, jnp.stack([gain_one_grad, gain_two_grad]), (0, me_col * col_width)
    )
    gain_grads = lax.psum(gain_grads, ("dp", "row", "col"))
    own = gain_attn.shape[0]
    gain_grads = lax.dynamic_slice_in_dim(
        gain_grads, (me_dp * lax.axis_size("row") + me_row) * own, own, 1
    )
    grad_attn = sum_weight(grad_attn_part, shift)
    return (
        layer_out,
        grad_tokens,
        gain_grads[0],
        gain_grads[1],
        grad_attn[:, :q_cols],
        grad_attn[:, q_cols : q_cols + k_cols],
        grad_attn[:, q_cols + k_cols :],
        sum_weight(grad_output_part, shift).T,
        return_weight(grad_gate_part, shift),
        return_weight(grad_up_part, shift),
        return_weight(grad_down_part, shift).T,
    )


def solution(mesh):
    in_specs = (
        P(("dp", "row"), "col"),
        P(("dp", "row"), "col"),
        P(("dp", "row"), "col"),
        P(("dp", "row"), "col"),
        P("col", ("dp", "row")),
        P(("dp", "row"), "col"),
        P(("dp", "row"), "col"),
        P("col", ("dp", "row")),
        P(("dp", "row")),
        P(("dp", "row")),
        P("dp"),
        P(("dp", "row"), "col"),
    )
    out_specs = (
        P(("dp", "row"), "col"),
        P(("dp", "row"), "col"),
        P(("dp", "row")),
        P(("dp", "row")),
        P(("dp", "row"), "col"),
        P(("dp", "row"), "col"),
        P(("dp", "row"), "col"),
        P("col", ("dp", "row")),
        P(("dp", "row"), "col"),
        P(("dp", "row"), "col"),
        P("col", ("dp", "row")),
    )
    return jax.shard_map(
        per_device, mesh=mesh, in_specs=in_specs, out_specs=out_specs, check_vma=False
    )
```

```python
import math

import jax
import jax.numpy as jnp
from jax import lax
from jax.experimental import pallas as pl
from jax.experimental.pallas import tpu as pltpu
from jax.sharding import PartitionSpec as P

QUERY_HEADS = 8
KEY_VALUE_HEADS = 4
HEAD_SIZE = 256


EPSILON = 1e-06
ROPE_BASE = 1000042.0


def rope_tables(positions):
    half = HEAD_SIZE // 2
    freq = ROPE_BASE ** (-jnp.arange(half, dtype=jnp.float32) * 2.0 / HEAD_SIZE)
    angle = positions[:, None] * freq[None, :]
    return (jnp.cos(angle), jnp.sin(angle))


def rotary_apply(values, cosine_table, sine_table):
    half = values.shape[-1] // 2
    first = values[..., :half]
    second = values[..., half:]
    cos_part = cosine_table[:, None, :]
    sin_part = sine_table[:, None, :]
    return jnp.concatenate(
        [first * cos_part - second * sin_part, second * cos_part + first * sin_part], axis=-1
    )


def rotate_back(grads, cosine_table, sine_table):
    half = grads.shape[-1] // 2
    first = grads[..., :half]
    second = grads[..., half:]
    cos_part = cosine_table[:, None, :]
    sin_part = sine_table[:, None, :]
    return jnp.concatenate(
        [first * cos_part + second * sin_part, second * cos_part - first * sin_part], axis=-1
    )


def norm_rows(full, gain):
    factor = lax.rsqrt(jnp.mean(full * full, axis=1, keepdims=True) + EPSILON)
    return (factor, (full * factor * gain).astype(jnp.bfloat16))


def norm_back(full, factor, gain, grad):
    inner = jnp.mean(gain * grad * full, axis=1, keepdims=True)
    back = factor * gain * grad - full * factor * factor * factor * inner
    gain_grad = jnp.sum(grad * full * factor, axis=0)
    return (back, gain_grad)


def contract_rows(left, right):
    return lax.dot_general(
        left, right, (((0,), (0,)), ((), ())), preferred_element_type=jnp.float32
    )


def times_transposed(left, right):
    return lax.dot_general(
        left, right, (((1,), (1,)), ((), ())), preferred_element_type=jnp.float32
    )


def masked_scores(query_rows, key_part, query_pos, index, key_block, score_scale):
    scores = (
        jnp.einsum("hgqd,khd->hgqk", query_rows, key_part, preferred_element_type=jnp.float32)
        * score_scale
    )
    key_pos = index * key_block + jnp.arange(key_block, dtype=jnp.int32)
    return jnp.where(key_pos[None, :] <= query_pos[:, None], scores, -1e30)


def attend(query_rows, keys, values, query_pos, key_block, score_scale):
    heads, query_group, token_count, size = query_rows.shape
    blocks = keys.shape[0] // key_block
    key_parts = keys.reshape(blocks, key_block, heads, size)
    value_parts = values.reshape(blocks, key_block, heads, size)
    indices = jnp.arange(blocks, dtype=jnp.int32)

    def totals(carry, item):
        top, total = carry
        key_part, index = item
        scores = masked_scores(query_rows, key_part, query_pos, index, key_block, score_scale)
        new_top = jnp.maximum(top, jnp.max(scores, axis=-1))
        total = total * jnp.exp(top - new_top) + jnp.sum(
            jnp.exp(scores - new_top[..., None]), axis=-1
        )
        return ((new_top, total), None)

    start = (
        jnp.full((heads, query_group, token_count), -1e30, jnp.float32),
        jnp.zeros((heads, query_group, token_count), jnp.float32),
    )
    (top, total), unused = lax.scan(totals, start, (key_parts, indices))
    log_total = top + jnp.log(total)

    def mixing(accum, item):
        key_part, value_part, index = item
        scores = masked_scores(query_rows, key_part, query_pos, index, key_block, score_scale)
        probs = jnp.exp(scores - log_total[..., None]).astype(jnp.bfloat16)
        return (
            accum
            + jnp.einsum("hgqk,khd->hgqd", probs, value_part, preferred_element_type=jnp.float32),
            None,
        )

    accum, unused = lax.scan(
        mixing,
        jnp.zeros((heads, query_group, token_count, size), jnp.float32),
        (key_parts, value_parts, indices),
    )
    return (accum, log_total)


def attend_back(
    query_rows, keys, values, query_pos, key_block, score_scale, log_total, delta, grad_out
):
    heads, query_group, token_count, size = query_rows.shape
    blocks = keys.shape[0] // key_block
    key_parts = keys.reshape(blocks, key_block, heads, size)
    value_parts = values.reshape(blocks, key_block, heads, size)

    def step(grad_query, item):
        key_part, value_part, index = item
        scores = masked_scores(query_rows, key_part, query_pos, index, key_block, score_scale)
        probs = jnp.exp(scores - log_total[..., None])
        probs_low = probs.astype(jnp.bfloat16)
        grad_probs = jnp.einsum(
            "hgqd,khd->hgqk", grad_out, value_part, preferred_element_type=jnp.float32
        )
        grad_scores = (probs * (grad_probs - delta[..., None]) * score_scale).astype(jnp.bfloat16)
        grad_query = grad_query + jnp.einsum(
            "hgqk,khd->hgqd", grad_scores, key_part, preferred_element_type=jnp.float32
        )
        grad_key = jnp.einsum(
            "hgqk,hgqd->khd", grad_scores, query_rows, preferred_element_type=jnp.float32
        )
        grad_value = jnp.einsum(
            "hgqk,hgqd->khd", probs_low, grad_out, preferred_element_type=jnp.float32
        )
        return (grad_query, (grad_key, grad_value))

    grad_query, (grad_keys, grad_values) = lax.scan(
        step,
        jnp.zeros((heads, query_group, token_count, size), jnp.float32),
        (key_parts, value_parts, jnp.arange(blocks, dtype=jnp.int32)),
    )
    return (
        grad_query,
        grad_keys.reshape(blocks * key_block, heads * size),
        grad_values.reshape(blocks * key_block, heads * size),
    )


def swap(value, axis, bit):
    size = lax.axis_size(axis)
    return lax.ppermute(value, axis, [(i, i ^ bit) for i in range(size)])


def gather_col(value):
    width = value.shape[1]
    far = swap(value, "col", 2)
    near = swap(jnp.concatenate([value, far], axis=1), "col", 1)
    return jnp.concatenate([value, near[:, :width], far, near[:, width:]], axis=1)


def scatter_col(value):
    width = value.shape[1] // 4
    part = [value[:, p * width : (p + 1) * width].astype(jnp.float32) for p in range(4)]
    low = jnp.bfloat16
    got = swap(jnp.concatenate([part[1], part[3]], axis=1).astype(low), "col", 1)
    keep_own = part[0] + got[:, :width].astype(jnp.float32)
    keep_far = part[2] + got[:, width:].astype(jnp.float32)
    return keep_own + swap(keep_far.astype(low), "col", 2).astype(jnp.float32)


def col_sum(value):
    value = value + swap(value, "col", 1)
    return value + swap(value, "col", 2)


def gather_row(value, axis):
    if lax.axis_size("row") == 2:
        other = swap(value, "row", 1)
        first = lax.axis_index("row") == 0
        return jnp.concatenate(
            [jnp.where(first, value, other), jnp.where(first, other, value)], axis=axis
        )
    return lax.all_gather(value, "row", axis=axis, tiled=True)


def scatter_row(value, axis):
    if lax.axis_size("row") == 2:
        me = lax.axis_index("row")
        mine = lax.dynamic_index_in_dim(value, me, axis, keepdims=False)
        theirs = lax.dynamic_index_in_dim(value, 1 - me, axis, keepdims=False)
        got = swap(theirs.astype(jnp.bfloat16), "row", 1)
        return mine.astype(jnp.float32) + got.astype(jnp.float32)
    value = lax.psum_scatter(value.astype(jnp.bfloat16), "row", scatter_dimension=axis, tiled=True)
    return jnp.squeeze(value, axis).astype(jnp.float32)


def reorder(blocks, shift):
    out = []
    for p in range(4):
        pick = blocks[p]
        for s in range(1, 4):
            pick = jnp.where(shift == s, blocks[p ^ s], pick)
        out.append(pick)
    return out


def gather_weight(local, shift):
    got = [local] + [swap(local, "dp", j) for j in range(1, 4)]
    full = gather_row(jnp.stack(reorder(got, shift))[:, None], 1)
    return full.reshape(-1, local.shape[1])


def exchange_weight(local, shift):
    me = lax.axis_index("dp")
    quarter = local.shape[1] // 4

    def part(j):
        return lax.dynamic_slice_in_dim(local, (me ^ j) * quarter, quarter, 1)

    got = [part(0)] + [swap(part(j), "dp", j) for j in range(1, 4)]
    full = gather_row(jnp.stack(reorder(got, shift))[:, None], 1)
    return full.reshape(-1, quarter)


def return_weight(grad, shift):
    rows, quarter = grad.shape
    row_size = lax.axis_size("row")
    own = scatter_row(grad.reshape(4, row_size, rows // (4 * row_size), quarter), 1)
    own = own.astype(jnp.bfloat16)
    sends = reorder([own[p] for p in range(4)], shift)
    got = [sends[0]] + [swap(sends[j], "dp", j) for j in range(1, 4)]
    natural = reorder(got, lax.axis_index("dp"))
    return jnp.concatenate(natural, axis=1).astype(jnp.float32)


def sum_weight(grad, shift):
    rows, width = grad.shape
    row_size = lax.axis_size("row")
    own = scatter_row(grad.reshape(4, row_size, rows // (4 * row_size), width), 1)
    sends = reorder([own[p] for p in range(4)], shift)
    total = sends[0]
    for j in range(1, 4):
        total = total + swap(sends[j].astype(jnp.bfloat16), "dp", j).astype(jnp.float32)
    return total


def gather_tokens(value):
    full = gather_col(
        jnp.concatenate([value] + [swap(value, "dp", j) for j in range(1, 4)], axis=0)
    )
    return full


def scatter_tokens(value):
    own = scatter_col(value)
    rows = own.shape[0] // 4
    total = own[:rows]
    for j in range(1, 4):
        total = total + swap(
            own[j * rows : (j + 1) * rows].astype(jnp.bfloat16), "dp", j
        ).astype(jnp.float32)
    return total


def dot_nn(left, right):
    return lax.dot_general(left, right, (((1,), (0,)), ((), ())), preferred_element_type=jnp.float32)


def tiles(count, size, body):
    def step(i, unused):
        body(pl.ds(pl.multiple_of(i * size, size), size))
        return unused

    lax.fori_loop(0, count // size, step, 0)


def remote(src, dst, send_sem, recv_sem, target):
    return pltpu.make_async_remote_copy(
        src_ref=src,
        dst_ref=dst,
        send_sem=send_sem,
        recv_sem=recv_sem,
        device_id=target,
        device_id_type=pl.DeviceIdType.MESH,
    )


def greet(targets):
    barrier = pltpu.get_barrier_semaphore()
    for target in targets:
        pl.semaphore_signal(
            barrier, inc=1, device_id=target, device_id_type=pl.DeviceIdType.MESH
        )
    pl.semaphore_wait(barrier, len(targets))


def ffn_kernel(
    h_ref,
    gain_ref,
    do_hbm,
    wg_hbm,
    wu_hbm,
    wd_hbm,
    dhn_ref,
    factor_ref,
    out_hbm,
    dwg_hbm,
    dwu_hbm,
    dwd_hbm,
    full,
    do,
    wg,
    wu,
    wd,
    hid,
    dg,
    du,
    gate,
    up,
    dhid,
    part,
    outp,
    core_in,
    x_out,
    x_in,
    z_out,
    z_in,
    stage,
    load_sem,
    z_send,
    f_send,
    z_recv,
    x_send,
    x_recv,
    c_send,
    c_recv,
    p_send,
    p_recv,
    rx_send,
    rx_recv,
    rz_send,
    rz_recv,
    o_sem,
    s_sem,
):
    rows, width = h_ref.shape
    model = width * 4
    hidden = wg.shape[1]
    low, wide = jnp.bfloat16, jnp.float32
    z, col = lax.axis_index("dp"), lax.axis_index("col")
    core, far = {"col": col ^ 1}, {"col": col ^ 2}
    mid = jnp.logical_and(z > 0, z < 3)

    def chunk(s):
        return jnp.where(jnp.logical_and(mid, s >= 2), 5 - s, s)

    def cols(p):
        return pl.ds(p * width, width)

    greet([{"dp": z ^ 1}, {"dp": z ^ 2}, {"dp": z ^ 3}, core, far])

    def z_own(target, index):
        slot = z ^ target
        return remote(
            h_ref, full.at[slot, :, cols(0)], z_send.at[index], z_recv.at[slot], {"dp": target}
        )

    @pl.when(z < 3)
    def _():
        z_own(z + 1, 0).start()

    @pl.when(z > 0)
    def _():
        z_own(z - 1, 1).start()

    def x_copy(j, src):
        return remote(src, full.at[j, :, cols(2)], x_send.at[j], x_recv.at[j], far)

    def c_copy(j, src, which):
        return remote(
            src, full.at[j, :, cols(1 + 2 * which)], c_send.at[which, j], c_recv.at[which, j], core
        )

    x_copy(0, h_ref).start()
    c_copy(0, h_ref, 0).start()
    loads = [
        pltpu.make_async_copy(wg_hbm, wg, load_sem.at[0]),
        pltpu.make_async_copy(wu_hbm, wu, load_sem.at[1]),
        pltpu.make_async_copy(wd_hbm, wd, load_sem.at[2]),
    ]
    for load in loads:
        load.start()

    def do_load(j):
        return pltpu.make_async_copy(do_hbm.at[j], do.at[j], load_sem.at[3 + j])

    for j in range(4):
        do_load(j).start()

    def copy_own(r):
        full[0, r, 0:width] = h_ref[r, :]

    tiles(rows, 64, copy_own)

    def forward(j, target):
        return remote(
            full.at[j, :, cols(0)],
            full.at[(z ^ j) ^ target, :, cols(0)],
            f_send.at[j],
            z_recv.at[(z ^ j) ^ target],
            {"dp": target},
        )

    def goes_up(j):
        return jnp.logical_and((z ^ j) < z, z < 3)

    def goes_down(j):
        return jnp.logical_and((z ^ j) > z, z > 0)

    def arrive(j):
        block = full.at[j, :, cols(0)]
        remote(block, block, f_send.at[j], z_recv.at[j], core).wait_recv()

        @pl.when(goes_up(j))
        def _():
            forward(j, z + 1).start()

        @pl.when(goes_down(j))
        def _():
            forward(j, z - 1).start()

        x_copy(j, block).start()
        c_copy(j, block, 0).start()

    def settle(j):
        block = full.at[j, :, cols(0)]
        x_copy(j, block).wait_recv()
        c_copy(j, full.at[j, :, cols(2)], 1).start()
        x_copy(j, block).wait_send()
        c_copy(j, block, 0).wait_send()

        @pl.when(jnp.logical_and(j > 0, jnp.logical_or(goes_up(j), goes_down(j))))
        def _():
            forward(j, z ^ j).wait_send()

        c_copy(j, block, 0).wait_recv()
        c_copy(j, block, 1).wait()

    def part_copy(s, slot):
        return remote(
            part.at[slot, :, pl.ds(2 * width, 2 * width)],
            core_in.at[s],
            p_send.at[s],
            p_recv.at[s],
            core,
        )

    def rx_copy(s):
        return remote(x_out.at[s], x_in.at[s], rx_send.at[s], rx_recv.at[s], far)

    def rz_copy(s, j):
        return remote(z_out.at[s], z_in.at[j], rz_send.at[s], rz_recv.at[j], {"dp": z ^ j})

    def reduce_core(s):
        slot = lax.rem(s, 2)
        part_copy(s, slot).wait()

        def add(r):
            x_out[s, r, :] = (
                part[slot, r, width : 2 * width].astype(wide)
                + core_in[s, r, width : 2 * width].astype(wide)
            ).astype(low)
            z_out[s, r, :] = (
                part[slot, r, 0:width].astype(wide) + core_in[s, r, 0:width].astype(wide)
            ).astype(low)

        tiles(rows, 64, add)
        rx_copy(s).start()

    def reduce_far(s):
        rx_copy(s).wait()

        def add(r):
            z_out[s, r, :] = (z_out[s, r, :].astype(wide) + x_in[s, r, :].astype(wide)).astype(low)

        tiles(rows, 64, add)

        @pl.when(s > 0)
        def _():
            rz_copy(s, chunk(s)).start()

    def out_copy(s):
        return pltpu.make_async_copy(
            outp.at[lax.rem(s, 2)], out_hbm.at[chunk(s)], o_sem.at[lax.rem(s, 2)]
        )

    def step(s, unused):
        j = chunk(s)
        base = s * rows

        @pl.when(jnp.logical_and(s < 3, jnp.logical_not(jnp.logical_and(s == 1, mid))))
        def _():
            arrive(chunk(s + 1))

        @pl.when(jnp.logical_and(s == 0, mid))
        def _():
            arrive(chunk(2))

        settle(j)

        def norm(r):
            x = full[j, r, :].astype(wide)
            factor = lax.rsqrt(jnp.sum(x * x, axis=1, keepdims=True) * (1.0 / model) + EPSILON)
            full[j, r, :] = (x * factor * gain_ref[...]).astype(low)

            @pl.when(s == 0)
            def _():
                factor_ref[r, :] = jnp.broadcast_to(factor, (factor.shape[0], 128))

        tiles(rows, 32, norm)

        @pl.when(s == 0)
        def _():
            for load in loads:
                load.wait()

        gate[...] = dot_nn(full[j], wg[...])
        up[...] = dot_nn(full[j], wu[...])

        @pl.when(s > 0)
        def _():
            reduce_core(s - 1)

        do_load(j).wait()
        dhid[...] = dot_nn(do[j], wd[...])

        def act(r):
            g = gate[r, :]
            u = up[r, :]
            d = dhid[r, :]
            sig = jax.nn.sigmoid(g)
            silu = g * sig
            at = pl.ds(pl.multiple_of(base + r.start, 64), 64)
            hid[at, :] = (silu * u).astype(low)
            dg[at, :] = (d * u * sig * (1.0 + g * (1.0 - sig))).astype(low)
            du[at, :] = (d * silu).astype(low)

        tiles(rows, 64, act)
        slot = lax.rem(s, 2)
        mine = pl.ds(pl.multiple_of(base, rows), rows)

        def dhn(q, p):
            w_rows = slice(p * width, (p + 1) * width)
            part[slot, :, q * width : (q + 1) * width] = (
                times_transposed(dg[mine, :], wg[w_rows, :])
                + times_transposed(du[mine, :], wu[w_rows, :])
            ).astype(low)

        dhn(2, 1)
        dhn(3, 3)
        dhn(0, 0)
        part_copy(s, slot).start()
        dhn(1, 2)

        @pl.when(s > 0)
        def _():
            reduce_far(s - 1)

        @pl.when(s >= 2)
        def _():
            out_copy(s - 2).wait()

        for p in range(4):
            outp[slot, :, p * width : (p + 1) * width] = times_transposed(
                hid[mine, :], wd[p * width : (p + 1) * width, :]
            ).astype(low)
        out_copy(s).start()
        return unused

    lax.fori_loop(0, 4, step, 0)

    reduce_core(3)
    count = model // width

    def stage_copy(target, i, slot):
        at = pl.ds(pl.multiple_of(i * width, width), width)
        return pltpu.make_async_copy(stage.at[slot], target.at[at, :], s_sem.at[slot])

    def weight_grad(target, right, left_of, first):
        def tile(i, unused):
            slot = lax.rem(i, 2)

            @pl.when(jnp.logical_or(i >= 2, not first))
            def _():
                stage_copy(target, 0, slot).wait()

            total = left_of(0, i, right)
            for s in range(1, 4):
                total = total + left_of(s, i, right)
            stage[slot] = total.astype(low)
            stage_copy(target, i, slot).start()
            return unused

        lax.fori_loop(0, count, tile, 0)

    def from_full(s, i, right):
        at = pl.ds(pl.multiple_of(i * width, width), width)
        return contract_rows(full[chunk(s), :, at], right[s * rows : (s + 1) * rows, :])

    def from_do(s, i, right):
        at = pl.ds(pl.multiple_of(i * width, width), width)
        return contract_rows(do[chunk(s), :, at], right[s * rows : (s + 1) * rows, :])

    weight_grad(dwg_hbm, dg, from_full, True)
    reduce_far(3)
    weight_grad(dwu_hbm, du, from_full, False)
    weight_grad(dwd_hbm, hid, from_do, False)
    stage_copy(dwd_hbm, 0, 0).wait()
    stage_copy(dwd_hbm, 0, 1).wait()
    out_copy(2).wait()
    out_copy(3).wait()
    for s in range(1, 4):
        rz_copy(s, chunk(s)).wait()

    def final(r):
        total = z_out[0, r, :].astype(wide)
        for j in range(1, 4):
            total = total + z_in[j, r, :].astype(wide)
        dhn_ref[r, :] = total

    tiles(rows, 64, final)

    @pl.when(z < 3)
    def _():
        z_own(z + 1, 0).wait_send()

    @pl.when(z > 0)
    def _():
        z_own(z - 1, 1).wait_send()


def ffn_call(h_low, gain, grad_full, wg, wu, wd):
    rows, width = h_low.shape
    model, hidden = wg.shape
    low, wide = jnp.bfloat16, jnp.float32
    vmem = pl.BlockSpec(memory_space=pltpu.VMEM)
    hbm = pl.BlockSpec(memory_space=pl.ANY)
    dma = pltpu.SemaphoreType.DMA
    tokens = 4 * rows
    return pl.pallas_call(
        ffn_kernel,
        out_shape=(
            jax.ShapeDtypeStruct((rows, width), wide),
            jax.ShapeDtypeStruct((rows, 128), wide),
            jax.ShapeDtypeStruct((4, rows, model), low),
            jax.ShapeDtypeStruct((model, hidden), low),
            jax.ShapeDtypeStruct((model, hidden), low),
            jax.ShapeDtypeStruct((model, hidden), low),
        ),
        in_specs=[vmem, vmem, hbm, hbm, hbm, hbm],
        out_specs=(vmem, vmem, hbm, hbm, hbm, hbm),
        scratch_shapes=[
            pltpu.VMEM((4, rows, model), low),
            pltpu.VMEM((4, rows, model), low),
            pltpu.VMEM((model, hidden), low),
            pltpu.VMEM((model, hidden), low),
            pltpu.VMEM((model, hidden), low),
            pltpu.VMEM((tokens, hidden), low),
            pltpu.VMEM((tokens, hidden), low),
            pltpu.VMEM((tokens, hidden), low),
            pltpu.VMEM((rows, hidden), wide),
            pltpu.VMEM((rows, hidden), wide),
            pltpu.VMEM((rows, hidden), wide),
            pltpu.VMEM((2, rows, model), low),
            pltpu.VMEM((2, rows, model), low),
            pltpu.VMEM((4, rows, 2 * width), low),
            pltpu.VMEM((4, rows, width), low),
            pltpu.VMEM((4, rows, width), low),
            pltpu.VMEM((4, rows, width), low),
            pltpu.VMEM((4, rows, width), low),
            pltpu.VMEM((2, width, hidden), low),
            dma((7,)),
            dma((2,)),
            dma((4,)),
            dma((4,)),
            dma((4,)),
            dma((4,)),
            dma((2, 4)),
            dma((2, 4)),
            dma((4,)),
            dma((4,)),
            dma((4,)),
            dma((4,)),
            dma((4,)),
            dma((4,)),
            dma((2,)),
            dma((2,)),
        ],
        compiler_params=pltpu.CompilerParams(
            collective_id=2, has_side_effects=True, vmem_limit_bytes=66_000_000
        ),
        cost_estimate=pl.CostEstimate(
            flops=18 * tokens * model * hidden,
            bytes_accessed=40_000_000,
            transcendentals=tokens * hidden,
        ),
    )(h_low, gain, grad_full, wg, wu, wd)


class Relay:
    def __init__(self, z, place, own_send, forward_send, recv):
        self.z, self.place = z, place
        self.own_send, self.forward_send, self.recv = own_send, forward_send, recv

    def own_copy(self, src, target, index):
        return remote(
            src,
            self.place(self.z, target),
            self.own_send.at[index],
            self.recv.at[self.z],
            {"dp": target},
        )

    def own(self, src, wait=False):
        @pl.when(self.z < 3)
        def _():
            copy = self.own_copy(src, self.z + 1, 0)
            copy.wait_send() if wait else copy.start()

        @pl.when(self.z > 0)
        def _():
            copy = self.own_copy(src, self.z - 1, 1)
            copy.wait_send() if wait else copy.start()

    def forward_copy(self, o, target):
        return remote(
            self.place(o, self.z),
            self.place(o, target),
            self.forward_send.at[o],
            self.recv.at[o],
            {"dp": target},
        )

    def forward(self, o, wait=False):
        @pl.when(jnp.logical_and(o < self.z, self.z < 3))
        def _():
            copy = self.forward_copy(o, self.z + 1)
            copy.wait_send() if wait else copy.start()

        @pl.when(jnp.logical_and(o > self.z, self.z > 0))
        def _():
            copy = self.forward_copy(o, self.z - 1)
            copy.wait_send() if wait else copy.start()

    def arrive(self, o):
        self.forward_copy(o, self.z ^ 1).wait_recv()
        self.forward(o)


def attn_fwd_kernel(
    tok_ref,
    cot_ref,
    gains_ref,
    cos_ref,
    sin_ref,
    valid_ref,
    wq_hbm,
    wk_hbm,
    wv_hbm,
    wo_hbm,
    wg_hbm,
    wu_hbm,
    wd_hbm,
    xn_ref,
    factor_ref,
    q_ref,
    kv_ref,
    lse_ref,
    mix_ref,
    h_ref,
    aw_ref,
    wo_ref,
    gain_ref,
    fg_hbm,
    fu_hbm,
    fd_hbm,
    do_hbm,
    full,
    qkv,
    gain_in,
    own_piece,
    part,
    core_in,
    x_out,
    x_in,
    load_sem,
    piece_sem,
    do_sem,
    g_send,
    g_recv,
    x_send,
    x_recv,
    t_send,
    t_recv,
    a_own,
    a_fwd,
    a_recv,
    ay_send,
    ay_recv,
    o_own,
    o_fwd,
    o_recv,
    oy_send,
    oy_recv,
    f_send,
    f_recv,
    fy_send,
    fy_recv,
    d_own,
    d_fwd,
    d_recv,
    dx_send,
    dx_recv,
    dc_send,
    dc_recv,
    kv_send,
    kv_recv,
    p_send,
    p_recv,
    r_send,
    r_recv,
):
    rows, width = tok_ref.shape
    model = 4 * width
    low, wide = jnp.bfloat16, jnp.float32
    row_size = lax.axis_size("row")
    local = wq_hbm.shape[0]
    q_cols, k_cols = wq_hbm.shape[1], wk_hbm.shape[1]
    hidden = fg_hbm.shape[1]
    half = HEAD_SIZE // 2
    z, y, col = (lax.axis_index(name) for name in ("dp", "row", "col"))
    core, far = {"col": col ^ 1}, {"col": col ^ 2}
    mid = jnp.logical_and(z > 0, z < 3)
    others = range(1, row_size)

    def chunk(s):
        return jnp.where(mid, 5 - s, s) if s >= 2 else s

    def cols(p):
        return pl.ds(p * width, width)

    def slot(o, r):
        return pl.ds(pl.multiple_of(((o ^ col) * row_size + r) * local, local), local)

    greet(
        [{"dp": z ^ j, "row": y ^ k} for j in range(4) for k in range(row_size) if j + k > 0]
        + [core, far]
    )

    loads = [
        pltpu.make_async_copy(src, aw_ref.at[slot(z, y), pl.ds(at, src.shape[1])], load_sem.at[i])
        for i, (src, at) in enumerate(
            ((wq_hbm, 0), (wk_hbm, q_cols), (wv_hbm, q_cols + k_cols))
        )
    ]
    load_out = pltpu.make_async_copy(wo_hbm, wo_ref.at[slot(z, y)], load_sem.at[3])
    for load in loads:
        load.start()
    load_out.start()

    def t_copy(which):
        src = full.at[:, cols(2)] if which == 2 else tok_ref
        target = far if which == 1 else core
        dst = full.at[:, cols((1, 2, 3)[which])]
        return remote(src, dst, t_send.at[which], t_recv.at[which], target)

    t_copy(1).start()
    t_copy(0).start()

    def g_copy(j, k):
        at = (z ^ col) * row_size + y
        return remote(
            gains_ref,
            gain_in.at[at],
            g_send.at[j, k],
            g_recv.at[j, k],
            {"dp": z ^ j, "row": y ^ k},
        )

    pairs = [(j, k) for j in range(4) for k in range(row_size) if j + k > 0]
    for j, k in pairs:
        g_copy(j, k).start()
    gain_in[(z ^ col) * row_size + y] = gains_ref[...]

    attn = Relay(z, lambda o, t: aw_ref.at[slot(o, y)], a_own, a_fwd, a_recv)
    outw = Relay(z, lambda o, t: wo_ref.at[slot(o, y)], o_own, o_fwd, o_recv)
    douts = Relay(z, lambda o, t: do_hbm.at[o ^ t, :, cols(0)], d_own, d_fwd, d_recv)

    def row_copy(ref, o, k, send, recv):
        block = ref.at[slot(o, y)]
        return remote(block, block, send.at[k, o], recv.at[k, o], {"row": y ^ k})

    def row_wait(ref, o, k, send, recv):
        block = ref.at[slot(o, y ^ k)]
        remote(block, block, send.at[k, o], recv.at[k, o], {"row": y ^ k}).wait_recv()

    for load in loads:
        load.wait()
    attn.own(aw_ref.at[slot(z, y)])
    for k in others:
        row_copy(aw_ref, z, k, ay_send, ay_recv).start()

    weights = ((wg_hbm, fg_hbm), (wu_hbm, fu_hbm), (wd_hbm, fd_hbm))

    def quarter(j):
        return pl.ds(pl.multiple_of((z ^ j) * hidden, hidden), hidden)

    pieces = [
        pltpu.make_async_copy(weights[a][0].at[:, quarter(0)], own_piece.at[a], piece_sem.at[a])
        for a in range(3)
    ]
    for piece in pieces:
        piece.start()

    full[:, 0:width] = tok_ref[...]
    t_copy(1).wait_recv()
    t_copy(2).start()
    attn.arrive(z ^ 1)
    for k in others:
        row_copy(aw_ref, z ^ 1, k, ay_send, ay_recv).start()
    load_out.wait()

    def attn_arrive(j):
        attn.arrive(z ^ j)
        for k in others:
            row_copy(aw_ref, z ^ j, k, ay_send, ay_recv).start()

    @pl.when(mid)
    def _():
        attn_arrive(3)

    outw.own(wo_ref.at[slot(z, y)])

    for j, k in pairs:
        g_copy(j, k).wait_recv()
    for i in range(4 * row_size):
        gain_ref[:, i * local : (i + 1) * local] = gain_in[i]
    t_copy(0).wait_recv()
    t_copy(2).wait_recv()

    def norm(r):
        x = full[r, :].astype(wide)
        factor = lax.rsqrt(jnp.sum(x * x, axis=1, keepdims=True) * (1.0 / model) + EPSILON)
        xn_ref[r, :] = (x * factor * gain_ref[0:1, :]).astype(low)
        factor_ref[r, :] = jnp.broadcast_to(factor, (factor.shape[0], 128))

    tiles(rows, 32, norm)

    @pl.when(jnp.logical_not(mid))
    def _():
        attn_arrive(2)

    attn_arrive_last = jnp.where(mid, 2, 3)
    attn.arrive(z ^ attn_arrive_last)
    for k in others:
        row_copy(aw_ref, z ^ attn_arrive_last, k, ay_send, ay_recv).start()
    for s in range(1, 4):
        outw.arrive(z ^ chunk(s))

    def f_copy(a, j):
        src, dst = weights[a]
        return remote(
            src.at[:, quarter(j)],
            dst.at[slot(z, y)],
            f_send.at[a, j],
            f_recv.at[a, j],
            {"dp": z ^ j},
        )

    for a in range(3):
        for j in (3, 2, 1):
            f_copy(a, j).start()

    def fy_copy(a, j, k):
        src = own_piece.at[a] if j == 0 else weights[a][1].at[slot(z ^ j, y)]
        return remote(
            src,
            weights[a][1].at[slot(z ^ j, y)],
            fy_send.at[a, k, j],
            fy_recv.at[a, k, j],
            {"row": y ^ k},
        )

    for o in range(4):
        for k in others:
            row_wait(aw_ref, o, k, ay_send, ay_recv)
    for n in range(0, q_cols + 2 * k_cols, 512):
        qkv[:, n : n + 512] = dot_nn(xn_ref[...], aw_ref[:, n : n + 512])

    def rope(r, at):
        c, s = cos_ref[r, :], sin_ref[r, :]
        first, second = qkv[r, at : at + half], qkv[r, at + half : at + 2 * half]
        return first * c - second * s, second * c + first * s

    def keys(r):
        first, second = rope(r, q_cols)
        kv_ref[y, r, 0:half] = first.astype(low)
        kv_ref[y, r, half : 2 * half] = second.astype(low)
        kv_ref[y, r, k_cols : 2 * k_cols] = qkv[r, q_cols + k_cols : q_cols + 2 * k_cols].astype(low)

    tiles(rows, 64, keys)
    heads = q_cols // HEAD_SIZE

    def queries(r):
        for h in range(heads):
            first, second = rope(r, h * HEAD_SIZE)
            q_ref[h, r, 0:half] = first.astype(low)
            q_ref[h, r, half : 2 * half] = second.astype(low)

    tiles(rows, 64, queries)

    def kv_copy(k, source):
        block = kv_ref.at[source]
        return remote(block, block, kv_send.at[k], kv_recv.at[k], {"row": y ^ k})

    for k in others:

        @pl.when((y ^ k) > y)
        def _():
            kv_copy(k, y).start()

    for o in range(4):
        for k in others:
            row_copy(wo_ref, o, k, oy_send, oy_recv).start()

    douts.own(cot_ref)

    def dx_copy(j):
        src = cot_ref if j == 0 else do_hbm.at[j, :, cols(0)]
        return remote(src, do_hbm.at[j, :, cols(2)], dx_send.at[j], dx_recv.at[j], far)

    def dc_copy(j, which):
        if which:
            src = do_hbm.at[j, :, cols(2)]
        else:
            src = cot_ref if j == 0 else do_hbm.at[j, :, cols(0)]
        return remote(
            src, do_hbm.at[j, :, cols(1 + 2 * which)], dc_send.at[which, j], dc_recv.at[which, j], core
        )

    dx_copy(0).start()
    dc_copy(0, 0).start()
    do_own = pltpu.make_async_copy(cot_ref, do_hbm.at[0, :, cols(0)], do_sem)
    do_own.start()
    for piece in pieces:
        piece.wait()
    stores = [
        pltpu.make_async_copy(own_piece.at[a], weights[a][1].at[slot(z, y)], piece_sem.at[a])
        for a in range(3)
    ]
    for a in range(3):
        stores[a].start()
        for k in others:
            fy_copy(a, 0, k).start()
    for k in others:

        @pl.when((y ^ k) < y)
        def _():
            kv_copy(k, y ^ k).wait_recv()

    q_tile = 256
    score_scale = 1.0 / math.sqrt(HEAD_SIZE)

    def attend_tile(i, unused):
        at = pl.ds(pl.multiple_of(i * q_tile, q_tile), q_tile)
        query_pos = y * rows + i * q_tile + lax.broadcasted_iota(jnp.int32, (q_tile, rows), 0)
        for h in range(heads):
            query = q_ref[h, at, :]

            def block(b, carry):
                top, total, accum = carry
                scores = times_transposed(query, kv_ref[b, :, 0:k_cols]) * score_scale
                key_pos = b * rows + lax.broadcasted_iota(jnp.int32, (q_tile, rows), 1)
                scores = jnp.where(key_pos <= query_pos, scores, -1e30)
                new_top = jnp.maximum(top, jnp.max(scores, axis=1, keepdims=True))
                probs = jnp.exp(scores - new_top)
                keep = jnp.exp(top - new_top)
                total = total * keep + jnp.sum(probs, axis=1, keepdims=True)
                accum = accum * keep + dot_nn(probs.astype(low), kv_ref[b, :, k_cols : 2 * k_cols])
                return new_top, total, accum

            top, total, accum = lax.fori_loop(
                0,
                y + 1,
                block,
                (
                    jnp.full((q_tile, 1), -1e30, wide),
                    jnp.zeros((q_tile, 1), wide),
                    jnp.zeros((q_tile, HEAD_SIZE), wide),
                ),
            )
            lse_ref[h, at, :] = jnp.broadcast_to(top + jnp.log(total), (q_tile, 128))
            mix_ref[at, h * HEAD_SIZE : (h + 1) * HEAD_SIZE] = (
                accum / total * valid_ref[at, :]
            ).astype(low)
        return unused

    lax.fori_loop(0, rows // q_tile, attend_tile, 0)

    for o in range(4):
        for k in others:
            row_wait(wo_ref, o, k, oy_send, oy_recv)
    part_copy = remote(part.at[:, pl.ds(2 * width, 2 * width)], core_in, p_send, p_recv, core)
    for at, p in ((2, 1), (3, 3), (0, 0)):
        part[:, at * width : (at + 1) * width] = times_transposed(
            mix_ref[...], wo_ref[p * width : (p + 1) * width, :]
        ).astype(low)
    part_copy.start()
    part[:, width : 2 * width] = times_transposed(
        mix_ref[...], wo_ref[2 * width : 3 * width, :]
    ).astype(low)
    part_copy.wait()

    def add_core(r):
        x_out[r, :] = (
            part[r, width : 2 * width].astype(wide) + core_in[r, width : 2 * width].astype(wide)
        ).astype(low)
        h_ref[r, :] = (
            tok_ref[r, :].astype(wide)
            + part[r, 0:width].astype(wide)
            + core_in[r, 0:width].astype(wide)
        )

    tiles(rows, 64, add_core)
    r_copy = remote(x_out, x_in, r_send, r_recv, far)
    r_copy.start()

    def f_arrive(a, j):
        f_copy(a, j).wait_recv()
        for k in others:
            fy_copy(a, j, k).start()

    for j in (1, 2, 3):
        f_arrive(0, j)
    r_copy.wait()

    def add_far(r):
        h_ref[r, :] = h_ref[r, :] + x_in[r, :].astype(wide)

    tiles(rows, 64, add_far)
    for a in (1, 2):
        for j in (1, 2, 3):
            f_arrive(a, j)

    def d_arrive(j):
        douts.arrive(z ^ j)
        dx_copy(j).start()
        dc_copy(j, 0).start()

    def d_settle(j):
        dx_copy(j).wait_recv()
        dc_copy(j, 1).start()

    d_settle(0)
    for s in range(1, 4):
        for j in sorted({s, 5 - s} if s >= 2 else {s}):
            if s < 2:
                d_arrive(j)
            else:

                @pl.when(chunk(s) == j)
                def _():
                    d_arrive(j)

    for j in (1, 2, 3):
        d_settle(j)

    for a in range(3):
        stores[a].wait()
        for j in range(4):
            for k in others:
                fy_copy(a, j, k).wait_send()
                block = weights[a][1].at[slot(z ^ j, y ^ k)]
                remote(
                    block, block, fy_send.at[a, k, j], fy_recv.at[a, k, j], {"row": y ^ k}
                ).wait_recv()
            if j:
                f_copy(a, j).wait_send()
    do_own.wait()
    for j in range(4):
        dx_copy(j).wait_send()
        dc_copy(j, 0).wait()
        dc_copy(j, 1).wait()
    for relay, src in ((attn, aw_ref.at[slot(z, y)]), (outw, wo_ref.at[slot(z, y)]), (douts, cot_ref)):
        relay.own(src, wait=True)
        for j in (1, 2, 3):
            relay.forward(z ^ j, wait=True)
    for o in range(4):
        for k in others:
            row_copy(aw_ref, o, k, ay_send, ay_recv).wait_send()
            row_copy(wo_ref, o, k, oy_send, oy_recv).wait_send()
    for k in others:

        @pl.when((y ^ k) > y)
        def _():
            kv_copy(k, y).wait_send()

    for j, k in pairs:
        g_copy(j, k).wait_send()
    for which in range(3):
        t_copy(which).wait_send()


def attn_fwd_call(tokens, cot, gains, cos, sin, valid, wq, wk, wv, wo, wg, wu, wd):
    rows, width = tokens.shape
    model = 4 * width
    low, wide = jnp.bfloat16, jnp.float32
    row_size = lax.axis_size("row")
    local, q_cols = wq.shape
    k_cols = wk.shape[1]
    hidden = wg.shape[1] // 4
    heads = q_cols // HEAD_SIZE
    vmem = pl.BlockSpec(memory_space=pltpu.VMEM)
    hbm = pl.BlockSpec(memory_space=pl.ANY)
    dma = pltpu.SemaphoreType.DMA
    relay = [dma((2,)), dma((4,)), dma((4,))]
    over_row = [dma((row_size, 4)), dma((row_size, 4))]
    shape = jax.ShapeDtypeStruct
    return pl.pallas_call(
        attn_fwd_kernel,
        out_shape=(
            shape((rows, model), low),
            shape((rows, 128), wide),
            shape((heads, rows, HEAD_SIZE), low),
            shape((row_size, rows, 2 * k_cols), low),
            shape((heads, rows, 128), wide),
            shape((rows, q_cols), low),
            shape((rows, width), wide),
            shape((model, q_cols + 2 * k_cols), low),
            shape((model, q_cols), low),
            shape((8, model), wide),
            shape((model, hidden), low),
            shape((model, hidden), low),
            shape((model, hidden), low),
            shape((4, rows, model), low),
        ),
        in_specs=[vmem] * 6 + [hbm] * 7,
        out_specs=(vmem,) * 10 + (hbm,) * 4,
        scratch_shapes=[
            pltpu.VMEM((rows, model), low),
            pltpu.VMEM((rows, q_cols + 2 * k_cols), wide),
            pltpu.VMEM((4 * row_size, 8, local), wide),
            pltpu.VMEM((3, local, hidden), low),
            pltpu.VMEM((rows, model), low),
            pltpu.VMEM((rows, 2 * width), low),
            pltpu.VMEM((rows, width), low),
            pltpu.VMEM((rows, width), low),
            dma((4,)),
            dma((3,)),
            dma(()),
            dma((4, row_size)),
            dma((4, row_size)),
            dma((1,)),
            dma((1,)),
            dma((3,)),
            dma((3,)),
            *relay,
            *over_row,
            *relay,
            *over_row,
            dma((3, 4)),
            dma((3, 4)),
            dma((3, row_size, 4)),
            dma((3, row_size, 4)),
            *relay,
            dma((4,)),
            dma((4,)),
            dma((2, 4)),
            dma((2, 4)),
            dma((row_size,)),
            dma((row_size,)),
            dma(()),
            dma(()),
            dma(()),
            dma(()),
        ],
        compiler_params=pltpu.CompilerParams(
            collective_id=1, has_side_effects=True, vmem_limit_bytes=60_000_000
        ),
        cost_estimate=pl.CostEstimate(
            flops=10_000_000_000, bytes_accessed=40_000_000, transcendentals=2_000_000
        ),
    )(tokens, cot, gains, cos, sin, valid, wq, wk, wv, wo, wg, wu, wd)


def per_device(
    tokens,
    w_query,
    key_matrix,
    value_matrix,
    w_output,
    w_gate,
    w_up,
    w_down,
    gain_attn,
    gain_ffn,
    lengths,
    cotangent,
):
    low = jnp.bfloat16
    wide = jnp.float32
    row_count, col_width = tokens.shape
    model_width = col_width * 4
    slot_size = row_count * lax.axis_size("row")
    key_block = min(512, slot_size)
    query_group = QUERY_HEADS // KEY_VALUE_HEADS
    score_scale = 1.0 / math.sqrt(HEAD_SIZE)
    me_dp, me_row, me_col = (lax.axis_index(name) for name in ("dp", "row", "col"))
    shift = me_dp ^ me_col
    query_pos = me_row * row_count + jnp.arange(row_count, dtype=jnp.int32)
    valid = (query_pos < lengths[0]).astype(wide)[:, None]
    cosine_table, sine_table = rope_tables(query_pos.astype(wide))

    gains = jnp.zeros((8, gain_attn.shape[0]), wide)
    gains = gains.at[0].set(gain_attn.astype(wide)).at[1].set(gain_ffn.astype(wide))
    q_cols, k_cols = w_query.shape[1], key_matrix.shape[1]
    kv_heads = k_cols // HEAD_SIZE
    grad_out = (cotangent.astype(wide) * valid).astype(low)
    (
        normed,
        factor_one,
        query_rows,
        kv_all,
        log_total,
        mixed_heads,
        residual,
        attn_weight,
        out_weight,
        gains,
        gate_weight,
        up_weight,
        down_weight,
        grad_out_full,
    ) = attn_fwd_call(
        tokens,
        grad_out,
        gains,
        cosine_table,
        sine_table,
        valid,
        w_query,
        key_matrix,
        value_matrix,
        w_output.T,
        w_gate,
        w_up,
        w_down.T,
    )
    factor_one = factor_one[:, :1]
    gain_one, gain_two = gains[0], gains[1]
    query_rows = query_rows.reshape(kv_heads, query_group, row_count, HEAD_SIZE)
    log_total = log_total[:, :, 0].reshape(kv_heads, query_group, row_count)
    attended = (
        mixed_heads.astype(wide)
        .reshape(row_count, kv_heads, query_group, HEAD_SIZE)
        .transpose(1, 2, 0, 3)
    )
    keys_all = kv_all[:, :, :k_cols].reshape(slot_size, kv_heads, HEAD_SIZE)
    values_all = kv_all[:, :, k_cols:].reshape(slot_size, kv_heads, HEAD_SIZE)
    seen = (jnp.arange(slot_size) < (me_row + 1) * row_count)[:, None, None]
    keys_all = jnp.where(seen, keys_all, 0)
    values_all = jnp.where(seen, values_all, 0)

    residual_low = residual.astype(low)
    grad_normed_two, factor_two, out_part, grad_gate_part, grad_up_part, grad_down_part = ffn_call(
        residual_low, gains[1:2], grad_out_full, gate_weight, up_weight, down_weight
    )
    layer_out = (residual + scatter_tokens(out_part.reshape(-1, model_width))).astype(low)
    own_gain_two = gain_two[:col_width]
    own_factor_two = factor_two[:, :1]
    own_residual = residual_low.astype(wide)
    scaled = own_gain_two * grad_normed_two
    inner = col_sum(jnp.sum(scaled * own_residual, axis=1)[:, None]) / model_width
    grad_residual = (
        grad_out.astype(wide)
        + own_factor_two * scaled
        - own_residual * own_factor_two * own_factor_two * own_factor_two * inner
    ).astype(low)
    gain_two_grad = jnp.sum(grad_normed_two * own_residual * own_factor_two, axis=0)

    grad_residual_full = gather_col(grad_residual)
    grad_output_part = contract_rows(grad_residual_full, mixed_heads)
    grad_mixed = (
        jnp.dot(grad_residual_full, out_weight, preferred_element_type=wide) * valid
    ).astype(low)
    grad_heads = grad_mixed.reshape(row_count, kv_heads, query_group, HEAD_SIZE).transpose(
        1, 2, 0, 3
    )
    delta = jnp.sum(grad_heads.astype(wide) * attended, axis=-1)
    grad_query_rot, grad_keys_all, grad_values_all = attend_back(
        query_rows,
        keys_all,
        values_all,
        query_pos,
        key_block,
        score_scale,
        log_total,
        delta,
        grad_heads,
    )
    grad_kv = scatter_row(
        jnp.concatenate([grad_keys_all, grad_values_all], axis=1).reshape(
            slot_size // row_count, row_count, 2 * k_cols
        ),
        0,
    )
    grad_query_raw = (
        rotate_back(
            grad_query_rot.transpose(2, 0, 1, 3).reshape(
                row_count, kv_heads * query_group, HEAD_SIZE
            ),
            cosine_table,
            sine_table,
        )
        .reshape(row_count, q_cols)
        .astype(low)
    )
    grad_key_raw = (
        rotate_back(
            grad_kv[:, :k_cols].reshape(row_count, kv_heads, HEAD_SIZE), cosine_table, sine_table
        )
        .reshape(row_count, k_cols)
        .astype(low)
    )
    grad_raw = jnp.concatenate([grad_query_raw, grad_key_raw, grad_kv[:, k_cols:].astype(low)], axis=1)
    grad_attn_part = contract_rows(normed, grad_raw)
    grad_normed = scatter_col(times_transposed(grad_raw, attn_weight))
    own_gain_one = gain_one[:col_width]
    own_tokens = tokens.astype(wide)
    scaled = own_gain_one * grad_normed
    inner = col_sum(jnp.sum(scaled * own_tokens, axis=1)[:, None]) / model_width
    grad_tokens = (
        grad_residual.astype(wide)
        + factor_one * scaled
        - own_tokens * factor_one * factor_one * factor_one * inner
    ).astype(low)
    gain_one_grad = jnp.sum(grad_normed * own_tokens * factor_one, axis=0)

    gain_grads = jnp.zeros((2, model_width), wide)
    gain_grads = lax.dynamic_update_slice(
        gain_grads, jnp.stack([gain_one_grad, gain_two_grad]), (0, me_col * col_width)
    )
    gain_grads = lax.psum(gain_grads, ("dp", "row", "col"))
    own = gain_attn.shape[0]
    gain_grads = lax.dynamic_slice_in_dim(
        gain_grads, (me_dp * lax.axis_size("row") + me_row) * own, own, 1
    )
    grad_attn = sum_weight(grad_attn_part, shift)
    return (
        layer_out,
        grad_tokens,
        gain_grads[0],
        gain_grads[1],
        grad_attn[:, :q_cols],
        grad_attn[:, q_cols : q_cols + k_cols],
        grad_attn[:, q_cols + k_cols :],
        sum_weight(grad_output_part, shift).T,
        return_weight(grad_gate_part, shift),
        return_weight(grad_up_part, shift),
        return_weight(grad_down_part, shift).T,
    )


def solution(mesh):
    in_specs = (
        P(("dp", "row"), "col"),
        P(("dp", "row"), "col"),
        P(("dp", "row"), "col"),
        P(("dp", "row"), "col"),
        P("col", ("dp", "row")),
        P(("dp", "row"), "col"),
        P(("dp", "row"), "col"),
        P("col", ("dp", "row")),
        P(("dp", "row")),
        P(("dp", "row")),
        P("dp"),
        P(("dp", "row"), "col"),
    )
    out_specs = (
        P(("dp", "row"), "col"),
        P(("dp", "row"), "col"),
        P(("dp", "row")),
        P(("dp", "row")),
        P(("dp", "row"), "col"),
        P(("dp", "row"), "col"),
        P(("dp", "row"), "col"),
        P("col", ("dp", "row")),
        P(("dp", "row"), "col"),
        P(("dp", "row"), "col"),
        P("col", ("dp", "row")),
    )
    return jax.shard_map(
        per_device, mesh=mesh, in_specs=in_specs, out_specs=out_specs, check_vma=False
    )
```

```python
import math

import jax
import jax.numpy as jnp
from jax import lax
from jax.experimental import pallas as pl
from jax.experimental.pallas import tpu as pltpu
from jax.sharding import PartitionSpec as P

HEAD_SIZE = 256
EPSILON = 1e-06
ROPE_BASE = 1000042.0


def rope_tables(positions):
    half = HEAD_SIZE // 2
    freq = ROPE_BASE ** (-jnp.arange(half, dtype=jnp.float32) * 2.0 / HEAD_SIZE)
    angle = positions[:, None] * freq[None, :]
    return (jnp.cos(angle), jnp.sin(angle))


def contract_rows(left, right):
    return lax.dot_general(
        left, right, (((0,), (0,)), ((), ())), preferred_element_type=jnp.float32
    )


def times_transposed(left, right):
    return lax.dot_general(
        left, right, (((1,), (1,)), ((), ())), preferred_element_type=jnp.float32
    )


def dot_nn(left, right):
    return lax.dot_general(left, right, (((1,), (0,)), ((), ())), preferred_element_type=jnp.float32)


def tiles(count, size, body):
    def step(i, unused):
        body(pl.ds(pl.multiple_of(i * size, size), size))
        return unused

    lax.fori_loop(0, count // size, step, 0)


def remote(src, dst, send_sem, recv_sem, target):
    return pltpu.make_async_remote_copy(
        src_ref=src,
        dst_ref=dst,
        send_sem=send_sem,
        recv_sem=recv_sem,
        device_id=target,
        device_id_type=pl.DeviceIdType.MESH,
    )


def greet(targets):
    barrier = pltpu.get_barrier_semaphore()
    for target in targets:
        pl.semaphore_signal(
            barrier, inc=1, device_id=target, device_id_type=pl.DeviceIdType.MESH
        )
    pl.semaphore_wait(barrier, len(targets))


def ffn_kernel(
    h_ref,
    gain_ref,
    do_hbm,
    wg_hbm,
    wu_hbm,
    wd_hbm,
    dhn_ref,
    factor_ref,
    out_hbm,
    dwg_hbm,
    dwu_hbm,
    dwd_hbm,
    full,
    do,
    wg,
    wu,
    wd,
    hid,
    dg,
    du,
    gate,
    up,
    dhid,
    part,
    outp,
    core_in,
    x_out,
    x_in,
    z_out,
    z_in,
    stage,
    load_sem,
    z_send,
    f_send,
    z_recv,
    x_send,
    x_recv,
    c_send,
    c_recv,
    p_send,
    p_recv,
    rx_send,
    rx_recv,
    rz_send,
    rz_recv,
    o_sem,
    s_sem,
):
    rows, width = h_ref.shape
    model = width * 4
    hidden = wg.shape[1]
    low, wide = jnp.bfloat16, jnp.float32
    z, col = lax.axis_index("dp"), lax.axis_index("col")
    core, far = {"col": col ^ 1}, {"col": col ^ 2}
    mid = jnp.logical_and(z > 0, z < 3)

    def chunk(s):
        return jnp.where(jnp.logical_and(mid, s >= 2), 5 - s, s)

    def cols(p):
        return pl.ds(p * width, width)

    greet([{"dp": z ^ 1}, {"dp": z ^ 2}, {"dp": z ^ 3}, core, far])

    def z_own(target, index):
        slot = z ^ target
        return remote(
            h_ref, full.at[slot, :, cols(0)], z_send.at[index], z_recv.at[slot], {"dp": target}
        )

    @pl.when(z < 3)
    def _():
        z_own(z + 1, 0).start()

    @pl.when(z > 0)
    def _():
        z_own(z - 1, 1).start()

    def x_copy(j, src):
        return remote(src, full.at[j, :, cols(2)], x_send.at[j], x_recv.at[j], far)

    def c_copy(j, src, which):
        return remote(
            src, full.at[j, :, cols(1 + 2 * which)], c_send.at[which, j], c_recv.at[which, j], core
        )

    x_copy(0, h_ref).start()
    c_copy(0, h_ref, 0).start()
    loads = [
        pltpu.make_async_copy(wg_hbm, wg, load_sem.at[0]),
        pltpu.make_async_copy(wu_hbm, wu, load_sem.at[1]),
        pltpu.make_async_copy(wd_hbm, wd, load_sem.at[2]),
    ]
    for load in loads:
        load.start()

    def do_load(j):
        return pltpu.make_async_copy(do_hbm.at[j], do.at[j], load_sem.at[3 + j])

    for j in range(4):
        do_load(j).start()

    def copy_own(r):
        full[0, r, 0:width] = h_ref[r, :]

    tiles(rows, 64, copy_own)

    def forward(j, target):
        return remote(
            full.at[j, :, cols(0)],
            full.at[(z ^ j) ^ target, :, cols(0)],
            f_send.at[j],
            z_recv.at[(z ^ j) ^ target],
            {"dp": target},
        )

    def goes_up(j):
        return jnp.logical_and((z ^ j) < z, z < 3)

    def goes_down(j):
        return jnp.logical_and((z ^ j) > z, z > 0)

    def arrive(j):
        block = full.at[j, :, cols(0)]
        remote(block, block, f_send.at[j], z_recv.at[j], core).wait_recv()

        @pl.when(goes_up(j))
        def _():
            forward(j, z + 1).start()

        @pl.when(goes_down(j))
        def _():
            forward(j, z - 1).start()

        x_copy(j, block).start()
        c_copy(j, block, 0).start()

    def settle(j):
        block = full.at[j, :, cols(0)]
        x_copy(j, block).wait_recv()
        c_copy(j, full.at[j, :, cols(2)], 1).start()
        x_copy(j, block).wait_send()
        c_copy(j, block, 0).wait_send()

        @pl.when(jnp.logical_and(j > 0, jnp.logical_or(goes_up(j), goes_down(j))))
        def _():
            forward(j, z ^ j).wait_send()

        c_copy(j, block, 0).wait_recv()
        c_copy(j, block, 1).wait()

    def part_copy(s, slot):
        return remote(
            part.at[slot, :, pl.ds(2 * width, 2 * width)],
            core_in.at[s],
            p_send.at[s],
            p_recv.at[s],
            core,
        )

    def rx_copy(s):
        return remote(x_out.at[s], x_in.at[s], rx_send.at[s], rx_recv.at[s], far)

    def rz_copy(s, j):
        return remote(z_out.at[s], z_in.at[j], rz_send.at[s], rz_recv.at[j], {"dp": z ^ j})

    def reduce_core(s):
        slot = lax.rem(s, 2)
        part_copy(s, slot).wait()

        def add(r):
            x_out[s, r, :] = (
                part[slot, r, width : 2 * width].astype(wide)
                + core_in[s, r, width : 2 * width].astype(wide)
            ).astype(low)
            z_out[s, r, :] = (
                part[slot, r, 0:width].astype(wide) + core_in[s, r, 0:width].astype(wide)
            ).astype(low)

        tiles(rows, 64, add)
        rx_copy(s).start()

    def reduce_far(s):
        rx_copy(s).wait()

        def add(r):
            z_out[s, r, :] = (z_out[s, r, :].astype(wide) + x_in[s, r, :].astype(wide)).astype(low)

        tiles(rows, 64, add)

        @pl.when(s > 0)
        def _():
            rz_copy(s, chunk(s)).start()

    def out_copy(s):
        return pltpu.make_async_copy(
            outp.at[lax.rem(s, 2)], out_hbm.at[chunk(s)], o_sem.at[lax.rem(s, 2)]
        )

    def step(s, unused):
        j = chunk(s)
        base = s * rows

        @pl.when(jnp.logical_and(s < 3, jnp.logical_not(jnp.logical_and(s == 1, mid))))
        def _():
            arrive(chunk(s + 1))

        @pl.when(jnp.logical_and(s == 0, mid))
        def _():
            arrive(chunk(2))

        settle(j)

        def norm(r):
            x = full[j, r, :].astype(wide)
            factor = lax.rsqrt(jnp.sum(x * x, axis=1, keepdims=True) * (1.0 / model) + EPSILON)
            full[j, r, :] = (x * factor * gain_ref[...]).astype(low)

            @pl.when(s == 0)
            def _():
                factor_ref[r, :] = jnp.broadcast_to(factor, (factor.shape[0], 128))

        tiles(rows, 32, norm)

        @pl.when(s == 0)
        def _():
            for load in loads:
                load.wait()

        gate[...] = dot_nn(full[j], wg[...])
        up[...] = dot_nn(full[j], wu[...])

        @pl.when(s > 0)
        def _():
            reduce_core(s - 1)

        do_load(j).wait()
        dhid[...] = dot_nn(do[j], wd[...])

        def act(r):
            g = gate[r, :]
            u = up[r, :]
            d = dhid[r, :]
            sig = jax.nn.sigmoid(g)
            silu = g * sig
            at = pl.ds(pl.multiple_of(base + r.start, 64), 64)
            hid[at, :] = (silu * u).astype(low)
            dg[at, :] = (d * u * sig * (1.0 + g * (1.0 - sig))).astype(low)
            du[at, :] = (d * silu).astype(low)

        tiles(rows, 64, act)
        slot = lax.rem(s, 2)
        mine = pl.ds(pl.multiple_of(base, rows), rows)

        def dhn(q, p):
            w_rows = slice(p * width, (p + 1) * width)
            part[slot, :, q * width : (q + 1) * width] = (
                times_transposed(dg[mine, :], wg[w_rows, :])
                + times_transposed(du[mine, :], wu[w_rows, :])
            ).astype(low)

        dhn(2, 1)
        dhn(3, 3)
        dhn(0, 0)
        part_copy(s, slot).start()
        dhn(1, 2)

        @pl.when(s > 0)
        def _():
            reduce_far(s - 1)

        @pl.when(s >= 2)
        def _():
            out_copy(s - 2).wait()

        for p in range(4):
            outp[slot, :, p * width : (p + 1) * width] = times_transposed(
                hid[mine, :], wd[p * width : (p + 1) * width, :]
            ).astype(low)
        out_copy(s).start()
        return unused

    lax.fori_loop(0, 4, step, 0)

    reduce_core(3)
    count = model // width

    def stage_copy(target, i, slot):
        at = pl.ds(pl.multiple_of(i * width, width), width)
        return pltpu.make_async_copy(stage.at[slot], target.at[at, :], s_sem.at[slot])

    def weight_grad(target, right, left_of, first):
        def tile(i, unused):
            slot = lax.rem(i, 2)

            @pl.when(jnp.logical_or(i >= 2, not first))
            def _():
                stage_copy(target, 0, slot).wait()

            total = left_of(0, i, right)
            for s in range(1, 4):
                total = total + left_of(s, i, right)
            stage[slot] = total.astype(low)
            stage_copy(target, i, slot).start()
            return unused

        lax.fori_loop(0, count, tile, 0)

    def from_full(s, i, right):
        at = pl.ds(pl.multiple_of(i * width, width), width)
        return contract_rows(full[chunk(s), :, at], right[s * rows : (s + 1) * rows, :])

    def from_do(s, i, right):
        at = pl.ds(pl.multiple_of(i * width, width), width)
        return contract_rows(do[chunk(s), :, at], right[s * rows : (s + 1) * rows, :])

    weight_grad(dwg_hbm, dg, from_full, True)
    reduce_far(3)
    weight_grad(dwu_hbm, du, from_full, False)
    weight_grad(dwd_hbm, hid, from_do, False)
    stage_copy(dwd_hbm, 0, 0).wait()
    stage_copy(dwd_hbm, 0, 1).wait()
    out_copy(2).wait()
    out_copy(3).wait()
    for s in range(1, 4):
        rz_copy(s, chunk(s)).wait()

    def final(r):
        total = z_out[0, r, :].astype(wide)
        for j in range(1, 4):
            total = total + z_in[j, r, :].astype(wide)
        dhn_ref[r, :] = total

    tiles(rows, 64, final)

    @pl.when(z < 3)
    def _():
        z_own(z + 1, 0).wait_send()

    @pl.when(z > 0)
    def _():
        z_own(z - 1, 1).wait_send()


def ffn_call(h_low, gain, grad_full, wg, wu, wd):
    rows, width = h_low.shape
    model, hidden = wg.shape
    low, wide = jnp.bfloat16, jnp.float32
    vmem = pl.BlockSpec(memory_space=pltpu.VMEM)
    hbm = pl.BlockSpec(memory_space=pl.ANY)
    dma = pltpu.SemaphoreType.DMA
    tokens = 4 * rows
    return pl.pallas_call(
        ffn_kernel,
        out_shape=(
            jax.ShapeDtypeStruct((rows, width), wide),
            jax.ShapeDtypeStruct((rows, 128), wide),
            jax.ShapeDtypeStruct((4, rows, model), low),
            jax.ShapeDtypeStruct((model, hidden), low),
            jax.ShapeDtypeStruct((model, hidden), low),
            jax.ShapeDtypeStruct((model, hidden), low),
        ),
        in_specs=[vmem, vmem, hbm, hbm, hbm, hbm],
        out_specs=(vmem, vmem, hbm, hbm, hbm, hbm),
        scratch_shapes=[
            pltpu.VMEM((4, rows, model), low),
            pltpu.VMEM((4, rows, model), low),
            pltpu.VMEM((model, hidden), low),
            pltpu.VMEM((model, hidden), low),
            pltpu.VMEM((model, hidden), low),
            pltpu.VMEM((tokens, hidden), low),
            pltpu.VMEM((tokens, hidden), low),
            pltpu.VMEM((tokens, hidden), low),
            pltpu.VMEM((rows, hidden), wide),
            pltpu.VMEM((rows, hidden), wide),
            pltpu.VMEM((rows, hidden), wide),
            pltpu.VMEM((2, rows, model), low),
            pltpu.VMEM((2, rows, model), low),
            pltpu.VMEM((4, rows, 2 * width), low),
            pltpu.VMEM((4, rows, width), low),
            pltpu.VMEM((4, rows, width), low),
            pltpu.VMEM((4, rows, width), low),
            pltpu.VMEM((4, rows, width), low),
            pltpu.VMEM((2, width, hidden), low),
            dma((7,)),
            dma((2,)),
            dma((4,)),
            dma((4,)),
            dma((4,)),
            dma((4,)),
            dma((2, 4)),
            dma((2, 4)),
            dma((4,)),
            dma((4,)),
            dma((4,)),
            dma((4,)),
            dma((4,)),
            dma((4,)),
            dma((2,)),
            dma((2,)),
        ],
        compiler_params=pltpu.CompilerParams(
            collective_id=2, has_side_effects=True, vmem_limit_bytes=66_000_000
        ),
        cost_estimate=pl.CostEstimate(
            flops=18 * tokens * model * hidden,
            bytes_accessed=40_000_000,
            transcendentals=tokens * hidden,
        ),
    )(h_low, gain, grad_full, wg, wu, wd)


class Relay:
    def __init__(self, z, place, own_send, forward_send, recv):
        self.z, self.place = z, place
        self.own_send, self.forward_send, self.recv = own_send, forward_send, recv

    def own_copy(self, src, target, index):
        return remote(
            src,
            self.place(self.z, target),
            self.own_send.at[index],
            self.recv.at[self.z],
            {"dp": target},
        )

    def own(self, src, wait=False):
        @pl.when(self.z < 3)
        def _():
            copy = self.own_copy(src, self.z + 1, 0)
            copy.wait_send() if wait else copy.start()

        @pl.when(self.z > 0)
        def _():
            copy = self.own_copy(src, self.z - 1, 1)
            copy.wait_send() if wait else copy.start()

    def forward_copy(self, o, target):
        return remote(
            self.place(o, self.z),
            self.place(o, target),
            self.forward_send.at[o],
            self.recv.at[o],
            {"dp": target},
        )

    def forward(self, o, wait=False):
        @pl.when(jnp.logical_and(o < self.z, self.z < 3))
        def _():
            copy = self.forward_copy(o, self.z + 1)
            copy.wait_send() if wait else copy.start()

        @pl.when(jnp.logical_and(o > self.z, self.z > 0))
        def _():
            copy = self.forward_copy(o, self.z - 1)
            copy.wait_send() if wait else copy.start()

    def arrive(self, o):
        self.forward_copy(o, self.z ^ 1).wait_recv()
        self.forward(o)


def attn_fwd_kernel(
    tok_ref,
    cot_ref,
    gains_ref,
    cos_ref,
    sin_ref,
    valid_ref,
    wq_hbm,
    wk_hbm,
    wv_hbm,
    wo_hbm,
    wg_hbm,
    wu_hbm,
    wd_hbm,
    xn_ref,
    factor_ref,
    q_ref,
    kv_ref,
    lse_ref,
    mix_ref,
    h_ref,
    aw_ref,
    wo_ref,
    gain_ref,
    fg_hbm,
    fu_hbm,
    fd_hbm,
    do_hbm,
    full,
    qkv,
    gain_in,
    own_piece,
    part,
    core_in,
    x_out,
    x_in,
    load_sem,
    piece_sem,
    do_sem,
    g_send,
    g_recv,
    x_send,
    x_recv,
    t_send,
    t_recv,
    a_own,
    a_fwd,
    a_recv,
    ay_send,
    ay_recv,
    o_own,
    o_fwd,
    o_recv,
    oy_send,
    oy_recv,
    f_send,
    f_recv,
    fy_send,
    fy_recv,
    d_own,
    d_fwd,
    d_recv,
    dx_send,
    dx_recv,
    dc_send,
    dc_recv,
    kv_send,
    kv_recv,
    p_send,
    p_recv,
    r_send,
    r_recv,
):
    rows, width = tok_ref.shape
    model = 4 * width
    low, wide = jnp.bfloat16, jnp.float32
    row_size = lax.axis_size("row")
    local = wq_hbm.shape[0]
    q_cols, k_cols = wq_hbm.shape[1], wk_hbm.shape[1]
    hidden = fg_hbm.shape[1]
    half = HEAD_SIZE // 2
    z, y, col = (lax.axis_index(name) for name in ("dp", "row", "col"))
    core, far = {"col": col ^ 1}, {"col": col ^ 2}
    mid = jnp.logical_and(z > 0, z < 3)
    others = range(1, row_size)

    def chunk(s):
        return jnp.where(mid, 5 - s, s) if s >= 2 else s

    def cols(p):
        return pl.ds(p * width, width)

    def slot(o, r):
        return pl.ds(pl.multiple_of(((o ^ col) * row_size + r) * local, local), local)

    greet(
        [{"dp": z ^ j, "row": y ^ k} for j in range(4) for k in range(row_size) if j + k > 0]
        + [core, far]
    )

    loads = [
        pltpu.make_async_copy(src, aw_ref.at[slot(z, y), pl.ds(at, src.shape[1])], load_sem.at[i])
        for i, (src, at) in enumerate(
            ((wq_hbm, 0), (wk_hbm, q_cols), (wv_hbm, q_cols + k_cols))
        )
    ]
    load_out = pltpu.make_async_copy(wo_hbm, wo_ref.at[slot(z, y)], load_sem.at[3])
    for load in loads:
        load.start()
    load_out.start()

    def t_copy(which):
        src = full.at[:, cols(2)] if which == 2 else tok_ref
        target = far if which == 1 else core
        dst = full.at[:, cols((1, 2, 3)[which])]
        return remote(src, dst, t_send.at[which], t_recv.at[which], target)

    t_copy(1).start()
    t_copy(0).start()

    def g_copy(j, k):
        at = (z ^ col) * row_size + y
        return remote(
            gains_ref,
            gain_in.at[at],
            g_send.at[j, k],
            g_recv.at[j, k],
            {"dp": z ^ j, "row": y ^ k},
        )

    pairs = [(j, k) for j in range(4) for k in range(row_size) if j + k > 0]
    for j, k in pairs:
        g_copy(j, k).start()
    gain_in[(z ^ col) * row_size + y] = gains_ref[...]

    attn = Relay(z, lambda o, t: aw_ref.at[slot(o, y)], a_own, a_fwd, a_recv)
    outw = Relay(z, lambda o, t: wo_ref.at[slot(o, y)], o_own, o_fwd, o_recv)
    douts = Relay(z, lambda o, t: do_hbm.at[o ^ t, :, cols(0)], d_own, d_fwd, d_recv)

    def row_copy(ref, o, k, send, recv):
        block = ref.at[slot(o, y)]
        return remote(block, block, send.at[k, o], recv.at[k, o], {"row": y ^ k})

    def row_wait(ref, o, k, send, recv):
        block = ref.at[slot(o, y ^ k)]
        remote(block, block, send.at[k, o], recv.at[k, o], {"row": y ^ k}).wait_recv()

    for load in loads:
        load.wait()
    attn.own(aw_ref.at[slot(z, y)])
    for k in others:
        row_copy(aw_ref, z, k, ay_send, ay_recv).start()

    weights = ((wg_hbm, fg_hbm), (wu_hbm, fu_hbm), (wd_hbm, fd_hbm))

    def quarter(j):
        return pl.ds(pl.multiple_of((z ^ j) * hidden, hidden), hidden)

    pieces = [
        pltpu.make_async_copy(weights[a][0].at[:, quarter(0)], own_piece.at[a], piece_sem.at[a])
        for a in range(3)
    ]
    for piece in pieces:
        piece.start()

    full[:, 0:width] = tok_ref[...]
    t_copy(1).wait_recv()
    t_copy(2).start()
    attn.arrive(z ^ 1)
    for k in others:
        row_copy(aw_ref, z ^ 1, k, ay_send, ay_recv).start()
    load_out.wait()

    def attn_arrive(j):
        attn.arrive(z ^ j)
        for k in others:
            row_copy(aw_ref, z ^ j, k, ay_send, ay_recv).start()

    @pl.when(mid)
    def _():
        attn_arrive(3)

    outw.own(wo_ref.at[slot(z, y)])

    for j, k in pairs:
        g_copy(j, k).wait_recv()
    for i in range(4 * row_size):
        gain_ref[:, i * local : (i + 1) * local] = gain_in[i]
    t_copy(0).wait_recv()
    t_copy(2).wait_recv()

    def norm(r):
        x = full[r, :].astype(wide)
        factor = lax.rsqrt(jnp.sum(x * x, axis=1, keepdims=True) * (1.0 / model) + EPSILON)
        xn_ref[r, :] = (x * factor * gain_ref[0:1, :]).astype(low)
        factor_ref[r, :] = jnp.broadcast_to(factor, (factor.shape[0], 128))

    tiles(rows, 32, norm)

    @pl.when(jnp.logical_not(mid))
    def _():
        attn_arrive(2)

    attn_arrive_last = jnp.where(mid, 2, 3)
    attn.arrive(z ^ attn_arrive_last)
    for k in others:
        row_copy(aw_ref, z ^ attn_arrive_last, k, ay_send, ay_recv).start()
    for s in range(1, 4):
        outw.arrive(z ^ chunk(s))

    def f_copy(a, j):
        src, dst = weights[a]
        return remote(
            src.at[:, quarter(j)],
            dst.at[slot(z, y)],
            f_send.at[a, j],
            f_recv.at[a, j],
            {"dp": z ^ j},
        )

    for a in range(3):
        for j in (3, 2, 1):
            f_copy(a, j).start()

    def fy_copy(a, j, k):
        src = own_piece.at[a] if j == 0 else weights[a][1].at[slot(z ^ j, y)]
        return remote(
            src,
            weights[a][1].at[slot(z ^ j, y)],
            fy_send.at[a, k, j],
            fy_recv.at[a, k, j],
            {"row": y ^ k},
        )

    for o in range(4):
        for k in others:
            row_wait(aw_ref, o, k, ay_send, ay_recv)
    for n in range(0, q_cols + 2 * k_cols, 512):
        qkv[:, n : n + 512] = dot_nn(xn_ref[...], aw_ref[:, n : n + 512])

    def rope(r, at):
        c, s = cos_ref[r, :], sin_ref[r, :]
        first, second = qkv[r, at : at + half], qkv[r, at + half : at + 2 * half]
        return first * c - second * s, second * c + first * s

    def keys(r):
        first, second = rope(r, q_cols)
        kv_ref[y, r, 0:half] = first.astype(low)
        kv_ref[y, r, half : 2 * half] = second.astype(low)
        kv_ref[y, r, k_cols : 2 * k_cols] = qkv[r, q_cols + k_cols : q_cols + 2 * k_cols].astype(low)

    tiles(rows, 64, keys)
    heads = q_cols // HEAD_SIZE

    def queries(r):
        for h in range(heads):
            first, second = rope(r, h * HEAD_SIZE)
            q_ref[h, r, 0:half] = first.astype(low)
            q_ref[h, r, half : 2 * half] = second.astype(low)

    tiles(rows, 64, queries)

    def kv_copy(k, source):
        block = kv_ref.at[source]
        return remote(block, block, kv_send.at[k], kv_recv.at[k], {"row": y ^ k})

    for k in others:

        @pl.when((y ^ k) > y)
        def _():
            kv_copy(k, y).start()

    for o in range(4):
        for k in others:
            row_copy(wo_ref, o, k, oy_send, oy_recv).start()

    douts.own(cot_ref)

    def dx_copy(j):
        src = cot_ref if j == 0 else do_hbm.at[j, :, cols(0)]
        return remote(src, do_hbm.at[j, :, cols(2)], dx_send.at[j], dx_recv.at[j], far)

    def dc_copy(j, which):
        if which:
            src = do_hbm.at[j, :, cols(2)]
        else:
            src = cot_ref if j == 0 else do_hbm.at[j, :, cols(0)]
        return remote(
            src, do_hbm.at[j, :, cols(1 + 2 * which)], dc_send.at[which, j], dc_recv.at[which, j], core
        )

    dx_copy(0).start()
    dc_copy(0, 0).start()
    do_own = pltpu.make_async_copy(cot_ref, do_hbm.at[0, :, cols(0)], do_sem)
    do_own.start()
    for piece in pieces:
        piece.wait()
    stores = [
        pltpu.make_async_copy(own_piece.at[a], weights[a][1].at[slot(z, y)], piece_sem.at[a])
        for a in range(3)
    ]
    for a in range(3):
        stores[a].start()
        for k in others:
            fy_copy(a, 0, k).start()
    for k in others:

        @pl.when((y ^ k) < y)
        def _():
            kv_copy(k, y ^ k).wait_recv()

    q_tile = 256
    score_scale = 1.0 / math.sqrt(HEAD_SIZE)

    def attend_tile(i, unused):
        at = pl.ds(pl.multiple_of(i * q_tile, q_tile), q_tile)
        query_pos = y * rows + i * q_tile + lax.broadcasted_iota(jnp.int32, (q_tile, rows), 0)
        for h in range(heads):
            query = q_ref[h, at, :]

            def block(b, carry):
                top, total, accum = carry
                scores = times_transposed(query, kv_ref[b, :, 0:k_cols]) * score_scale
                key_pos = b * rows + lax.broadcasted_iota(jnp.int32, (q_tile, rows), 1)
                scores = jnp.where(key_pos <= query_pos, scores, -1e30)
                new_top = jnp.maximum(top, jnp.max(scores, axis=1, keepdims=True))
                probs = jnp.exp(scores - new_top)
                keep = jnp.exp(top - new_top)
                total = total * keep + jnp.sum(probs, axis=1, keepdims=True)
                accum = accum * keep + dot_nn(probs.astype(low), kv_ref[b, :, k_cols : 2 * k_cols])
                return new_top, total, accum

            top, total, accum = lax.fori_loop(
                0,
                y + 1,
                block,
                (
                    jnp.full((q_tile, 1), -1e30, wide),
                    jnp.zeros((q_tile, 1), wide),
                    jnp.zeros((q_tile, HEAD_SIZE), wide),
                ),
            )
            lse_ref[h, at, :] = jnp.broadcast_to(top + jnp.log(total), (q_tile, 128))
            mix_ref[at, h * HEAD_SIZE : (h + 1) * HEAD_SIZE] = (
                accum / total * valid_ref[at, :]
            ).astype(low)
        return unused

    lax.fori_loop(0, rows // q_tile, attend_tile, 0)

    for o in range(4):
        for k in others:
            row_wait(wo_ref, o, k, oy_send, oy_recv)
    part_copy = remote(part.at[:, pl.ds(2 * width, 2 * width)], core_in, p_send, p_recv, core)
    for at, p in ((2, 1), (3, 3), (0, 0)):
        part[:, at * width : (at + 1) * width] = times_transposed(
            mix_ref[...], wo_ref[p * width : (p + 1) * width, :]
        ).astype(low)
    part_copy.start()
    part[:, width : 2 * width] = times_transposed(
        mix_ref[...], wo_ref[2 * width : 3 * width, :]
    ).astype(low)
    part_copy.wait()

    def add_core(r):
        x_out[r, :] = (
            part[r, width : 2 * width].astype(wide) + core_in[r, width : 2 * width].astype(wide)
        ).astype(low)
        h_ref[r, :] = (
            tok_ref[r, :].astype(wide)
            + part[r, 0:width].astype(wide)
            + core_in[r, 0:width].astype(wide)
        )

    tiles(rows, 64, add_core)
    r_copy = remote(x_out, x_in, r_send, r_recv, far)
    r_copy.start()

    def f_arrive(a, j):
        f_copy(a, j).wait_recv()
        for k in others:
            fy_copy(a, j, k).start()

    for j in (1, 2, 3):
        f_arrive(0, j)
    r_copy.wait()

    def add_far(r):
        h_ref[r, :] = h_ref[r, :] + x_in[r, :].astype(wide)

    tiles(rows, 64, add_far)
    for a in (1, 2):
        for j in (1, 2, 3):
            f_arrive(a, j)

    def d_arrive(j):
        douts.arrive(z ^ j)
        dx_copy(j).start()
        dc_copy(j, 0).start()

    def d_settle(j):
        dx_copy(j).wait_recv()
        dc_copy(j, 1).start()

    d_settle(0)
    for s in range(1, 4):
        for j in sorted({s, 5 - s} if s >= 2 else {s}):
            if s < 2:
                d_arrive(j)
            else:

                @pl.when(chunk(s) == j)
                def _():
                    d_arrive(j)

    for j in (1, 2, 3):
        d_settle(j)

    for a in range(3):
        stores[a].wait()
        for j in range(4):
            for k in others:
                fy_copy(a, j, k).wait_send()
                block = weights[a][1].at[slot(z ^ j, y ^ k)]
                remote(
                    block, block, fy_send.at[a, k, j], fy_recv.at[a, k, j], {"row": y ^ k}
                ).wait_recv()
            if j:
                f_copy(a, j).wait_send()
    do_own.wait()
    for j in range(4):
        dx_copy(j).wait_send()
        dc_copy(j, 0).wait()
        dc_copy(j, 1).wait()
    for relay, src in ((attn, aw_ref.at[slot(z, y)]), (outw, wo_ref.at[slot(z, y)]), (douts, cot_ref)):
        relay.own(src, wait=True)
        for j in (1, 2, 3):
            relay.forward(z ^ j, wait=True)
    for o in range(4):
        for k in others:
            row_copy(aw_ref, o, k, ay_send, ay_recv).wait_send()
            row_copy(wo_ref, o, k, oy_send, oy_recv).wait_send()
    for k in others:

        @pl.when((y ^ k) > y)
        def _():
            kv_copy(k, y).wait_send()

    for j, k in pairs:
        g_copy(j, k).wait_send()
    for which in range(3):
        t_copy(which).wait_send()


def attn_fwd_call(tokens, cot, gains, cos, sin, valid, wq, wk, wv, wo, wg, wu, wd):
    rows, width = tokens.shape
    model = 4 * width
    low, wide = jnp.bfloat16, jnp.float32
    row_size = lax.axis_size("row")
    local, q_cols = wq.shape
    k_cols = wk.shape[1]
    hidden = wg.shape[1] // 4
    heads = q_cols // HEAD_SIZE
    vmem = pl.BlockSpec(memory_space=pltpu.VMEM)
    hbm = pl.BlockSpec(memory_space=pl.ANY)
    dma = pltpu.SemaphoreType.DMA
    relay = [dma((2,)), dma((4,)), dma((4,))]
    over_row = [dma((row_size, 4)), dma((row_size, 4))]
    shape = jax.ShapeDtypeStruct
    return pl.pallas_call(
        attn_fwd_kernel,
        out_shape=(
            shape((rows, model), low),
            shape((rows, 128), wide),
            shape((heads, rows, HEAD_SIZE), low),
            shape((row_size, rows, 2 * k_cols), low),
            shape((heads, rows, 128), wide),
            shape((rows, q_cols), low),
            shape((rows, width), wide),
            shape((model, q_cols + 2 * k_cols), low),
            shape((model, q_cols), low),
            shape((8, model), wide),
            shape((model, hidden), low),
            shape((model, hidden), low),
            shape((model, hidden), low),
            shape((4, rows, model), low),
        ),
        in_specs=[vmem] * 6 + [hbm] * 7,
        out_specs=(vmem,) * 10 + (hbm,) * 4,
        scratch_shapes=[
            pltpu.VMEM((rows, model), low),
            pltpu.VMEM((rows, q_cols + 2 * k_cols), wide),
            pltpu.VMEM((4 * row_size, 8, local), wide),
            pltpu.VMEM((3, local, hidden), low),
            pltpu.VMEM((rows, model), low),
            pltpu.VMEM((rows, 2 * width), low),
            pltpu.VMEM((rows, width), low),
            pltpu.VMEM((rows, width), low),
            dma((4,)),
            dma((3,)),
            dma(()),
            dma((4, row_size)),
            dma((4, row_size)),
            dma((1,)),
            dma((1,)),
            dma((3,)),
            dma((3,)),
            *relay,
            *over_row,
            *relay,
            *over_row,
            dma((3, 4)),
            dma((3, 4)),
            dma((3, row_size, 4)),
            dma((3, row_size, 4)),
            *relay,
            dma((4,)),
            dma((4,)),
            dma((2, 4)),
            dma((2, 4)),
            dma((row_size,)),
            dma((row_size,)),
            dma(()),
            dma(()),
            dma(()),
            dma(()),
        ],
        compiler_params=pltpu.CompilerParams(
            collective_id=1, has_side_effects=True, vmem_limit_bytes=60_000_000
        ),
        cost_estimate=pl.CostEstimate(
            flops=10_000_000_000, bytes_accessed=40_000_000, transcendentals=2_000_000
        ),
    )(tokens, cot, gains, cos, sin, valid, wq, wk, wv, wo, wg, wu, wd)


def lane_sums(value):
    total = value[:, 0:128]
    for at in range(128, value.shape[1], 128):
        total = total + value[:, at : at + 128]
    return total


def attn_bwd_kernel(
    dhn_ref,
    factor_two_ref,
    h_ref,
    dout_ref,
    gain_ref,
    tok_ref,
    factor_one_ref,
    cos_ref,
    sin_ref,
    valid_ref,
    q_ref,
    lse_ref,
    mix_ref,
    xn_hbm,
    kv_hbm,
    aw_hbm,
    wo_hbm,
    out_hbm,
    dwg_hbm,
    dwu_hbm,
    dwd_hbm,
    layer_ref,
    dtok_ref,
    gains_ref,
    dattn_ref,
    dwo_ref,
    gg_ref,
    gu_ref,
    gd_ref,
    full,
    xn,
    kv,
    aw,
    wo,
    lanes,
    lanes_in,
    do,
    delta,
    dq,
    dkv,
    dkv_out,
    dkv_in,
    graw,
    dw_attn,
    dw_out,
    own_f,
    row_f,
    row_a,
    row_o,
    z_a,
    z_o,
    in_a,
    in_o,
    out_own,
    core_in,
    x_in,
    z_in,
    pcore_in,
    px_out,
    px_in,
    gvec,
    g_in,
    load_sem,
    l_send,
    l_recv,
    t_send,
    t_recv,
    fy_send,
    fy_recv,
    fz_send,
    fz_recv,
    own_sem,
    oc_send,
    oc_recv,
    oo_sem,
    ox_send,
    ox_recv,
    oz_send,
    oz_recv,
    kv_send,
    kv_recv,
    ay_send,
    ay_recv,
    az_send,
    az_recv,
    wy_send,
    wy_recv,
    wz_send,
    wz_recv,
    p_send,
    p_recv,
    r_send,
    r_recv,
    g_send,
    g_recv,
    gc_send,
    gc_recv,
):
    rows, width = tok_ref.shape
    model = 4 * width
    low, wide = jnp.bfloat16, jnp.float32
    row_size = lax.axis_size("row")
    local = model // (4 * row_size)
    heads = q_ref.shape[0]
    q_cols = heads * HEAD_SIZE
    all_cols = graw.shape[1]
    k_cols = (all_cols - q_cols) // 2
    hidden = own_f.shape[3]
    half = HEAD_SIZE // 2
    score_scale = 1.0 / math.sqrt(HEAD_SIZE)
    z, y, col = (lax.axis_index(name) for name in ("dp", "row", "col"))
    core, far = {"col": col ^ 1}, {"col": col ^ 2}
    others = range(1, row_size)
    partials = (dwg_hbm, dwu_hbm, dwd_hbm)
    results = (gg_ref, gu_ref, gd_ref)

    def cols(p):
        return pl.ds(p * width, width)

    greet(
        [{"dp": z ^ j, "row": y ^ k} for j in range(4) for k in range(row_size) if j + k > 0]
        + [{"col": col ^ m} for m in (1, 2, 3)]
    )

    def fy_copy(a, j, k):
        at = z ^ j ^ col
        return remote(
            partials[a].at[at, y ^ k],
            row_f.at[a, k - 1, j],
            fy_send.at[a, k, j],
            fy_recv.at[a, k, j],
            {"row": y ^ k},
        )

    far_first = (3, 2, 1, 0)
    for a in (0, 1):
        for j in far_first:
            for k in others:
                fy_copy(a, j, k).start()

    def own_load(a, j):
        return pltpu.make_async_copy(
            partials[a].at[z ^ j ^ col, y], own_f.at[a, j], own_sem.at[a, j]
        )

    def oc_copy(j, which):
        return remote(
            out_hbm.at[j, :, cols(1 + 2 * which)],
            core_in.at[j, :, cols(which)],
            oc_send.at[which, j],
            oc_recv.at[which, j],
            core,
        )

    def oo_copy(j, which):
        return pltpu.make_async_copy(
            out_hbm.at[j, :, cols(2 * which)], out_own.at[j, :, cols(which)], oo_sem.at[which, j]
        )

    loads = [
        pltpu.make_async_copy(src, dst, load_sem.at[i])
        for i, (src, dst) in enumerate(((wo_hbm, wo), (xn_hbm, xn), (aw_hbm, aw)))
    ]

    gain_two = gain_ref[1:2, 0:width]
    gain_one = gain_ref[0:1, 0:width]

    def residual(r):
        return h_ref[r, :].astype(low).astype(wide)

    def inner_two(r):
        lanes[0, r, :] = lane_sums(gain_two * dhn_ref[r, :] * residual(r)).astype(low)

    tiles(rows, 64, inner_two)
    for j in far_first:
        for which in (0, 1):
            oc_copy(j, which).start()
            oo_copy(j, which).start()

    def l_copy(n, m):
        return remote(
            lanes.at[n], lanes_in.at[n, m - 1], l_send.at[n, m - 1], l_recv.at[n, m - 1], {"col": col ^ m}
        )

    for m in (2, 3, 1):
        l_copy(0, m).start()
    for load in loads:
        load.start()
    for a in range(3):
        for j in far_first:
            own_load(a, j).start()

    def inner(n, r):
        total = lanes[n, r, :].astype(wide)
        for m in range(3):
            total = total + lanes_in[n, m, r, :].astype(wide)
        return jnp.sum(total, axis=1, keepdims=True) * (1.0 / model)

    def gain_two_sum(i, total):
        r = pl.ds(pl.multiple_of(i * 64, 64), 64)
        return total + jnp.sum(
            dhn_ref[r, :] * residual(r) * factor_two_ref[r, 0:1], axis=0, keepdims=True
        )

    gain_two_grad = lax.fori_loop(0, rows // 64, gain_two_sum, jnp.zeros((1, width), wide))
    for m in (1, 2, 3):
        l_copy(0, m).wait_recv()

    def grad_residual(r):
        factor = factor_two_ref[r, 0:1]
        grad = (
            dout_ref[r, :].astype(wide)
            + factor * gain_two * dhn_ref[r, :]
            - residual(r) * factor * factor * factor * inner(0, r)
        ).astype(low)
        full[r, 0:width] = grad
        dtok_ref[r, :] = grad

    tiles(rows, 64, grad_residual)

    def t_copy(which):
        src = full.at[:, cols(2)] if which == 2 else full.at[:, cols(0)]
        dst = full.at[:, cols((1, 2, 3)[which])]
        return remote(
            src, dst, t_send.at[which], t_recv.at[which], far if which == 1 else core
        )

    def ox_copy(j):
        return remote(out_own.at[j, :, cols(1)], x_in.at[j], ox_send.at[j], ox_recv.at[j], far)

    def out_core(j):
        for which in (0, 1):
            oo_copy(j, which).wait()
            oc_copy(j, which).wait_recv()

        def add(r):
            out_own[j, r, width : 2 * width] = (
                out_own[j, r, width : 2 * width].astype(wide)
                + core_in[j, r, width : 2 * width].astype(wide)
            ).astype(low)
            out_own[j, r, 0:width] = (
                out_own[j, r, 0:width].astype(wide) + core_in[j, r, 0:width].astype(wide)
            ).astype(low)

        tiles(rows, 64, add)

    out_core(3)
    t_copy(1).start()
    t_copy(0).start()
    ox_copy(3).start()

    def oz_copy(j):
        return remote(
            out_own.at[j, :, cols(0)], z_in.at[j - 1], oz_send.at[j], oz_recv.at[j], {"dp": z ^ j}
        )

    def out_far(j):
        ox_copy(j).wait_recv()

        def add(r):
            out_own[j, r, 0:width] = (
                out_own[j, r, 0:width].astype(wide) + x_in[j, r, :].astype(wide)
            ).astype(low)

        tiles(rows, 64, add)

    def fz_copy(a, j):
        at = pl.ds(pl.multiple_of(z * hidden, hidden), hidden)
        return remote(
            own_f.at[a, j], results[a].at[:, at], fz_send.at[a, j], fz_recv.at[a, j], {"dp": z ^ j}
        )

    def f_own(a):
        at = pl.ds(pl.multiple_of(z * hidden, hidden), hidden)
        return pltpu.make_async_copy(own_f.at[a, 0], results[a].at[:, at], own_sem.at[a, 0])

    def f_row(a, j):
        own_load(a, j).wait()
        for k in others:
            fy_copy(a, j, k).wait_recv()
        total = own_f[a, j].astype(wide)
        for k in others:
            total = total + row_f[a, k - 1, j].astype(wide)
        own_f[a, j] = total.astype(low)

    out_core(2)
    f_row(0, 3)
    ox_copy(2).start()
    out_core(1)
    fz_copy(0, 3).start()
    ox_copy(1).start()
    t_copy(1).wait_recv()
    t_copy(2).start()
    out_core(0)
    t_copy(0).wait_recv()
    f_row(0, 2)
    ox_copy(0).start()
    loads[0].wait()
    t_copy(2).wait_recv()

    do[...] = (dot_nn(full[...], wo[...]) * valid_ref[...]).astype(low)
    fz_copy(0, 2).start()
    for p in range(4):
        at = slice(p * width, (p + 1) * width)
        dw_out[at, :] = contract_rows(full[:, at], mix_ref[...]).astype(low)

    def deltas(r):
        for h in range(heads):
            at = slice(h * HEAD_SIZE, (h + 1) * HEAD_SIZE)
            total = jnp.sum(do[r, at].astype(wide) * mix_ref[r, at].astype(wide), axis=1, keepdims=True)
            delta[h, r, :] = jnp.broadcast_to(total, (total.shape[0], 128))

    tiles(rows, 64, deltas)
    dq[...] = jnp.zeros_like(dq)
    q_tile = 256

    def attend_block(b, slot):
        dkv[...] = jnp.zeros_like(dkv)

        def tile(i, unused):
            at = pl.ds(pl.multiple_of(i * q_tile, q_tile), q_tile)
            query_pos = y * rows + i * q_tile + lax.broadcasted_iota(jnp.int32, (q_tile, rows), 0)
            key_pos = b * rows + lax.broadcasted_iota(jnp.int32, (q_tile, rows), 1)
            for h in range(heads):
                head = slice(h * HEAD_SIZE, (h + 1) * HEAD_SIZE)
                query, grad = q_ref[h, at, :], do[at, head]
                keys, values = kv[slot, :, 0:k_cols], kv[slot, :, k_cols : 2 * k_cols]
                scores = times_transposed(query, keys) * score_scale
                probs = jnp.where(
                    key_pos <= query_pos, jnp.exp(scores - lse_ref[h, at, 0:1]), 0.0
                )
                grad_probs = times_transposed(grad, values)
                grad_scores = (probs * (grad_probs - delta[h, at, 0:1]) * score_scale).astype(low)
                dq[at, head] += dot_nn(grad_scores, keys)
                dkv[:, 0:k_cols] += contract_rows(grad_scores, query)
                dkv[:, k_cols : 2 * k_cols] += contract_rows(probs.astype(low), grad)
            return unused

        lax.fori_loop(0, rows // q_tile, tile, 0)

    def kv_copy(k):
        return remote(
            dkv_out, dkv_in.at[k - 1], kv_send.at[k], kv_recv.at[k], {"row": y ^ k}
        )

    blocks = [*others, 0]

    def when_block(k, body):
        if k:
            pl.when((y ^ k) < y)(body)
        else:
            body()

    def kv_load(i):
        return pltpu.make_async_copy(
            kv_hbm.at[y ^ blocks[i]], kv.at[i % 2], load_sem.at[3 + i % 2]
        )

    when_block(blocks[0], lambda: kv_load(0).start())
    for i, k in enumerate(others):
        when_block(k, lambda i=i: kv_load(i).wait())
        when_block(blocks[i + 1], lambda i=i: kv_load(i + 1).start())
        when_block(k, lambda i=i, k=k: attend_block(y ^ k, i % 2))
        if i:
            when_block(k - 1, lambda k=k: kv_copy(k - 1).wait_send())

        def keep(r):
            dkv_out[r, :] = dkv[r, :].astype(low)

        when_block(k, lambda: tiles(rows, 64, keep))
        if i == 0:
            f_row(0, 1)
            f_row(0, 0)
        when_block(k, lambda k=k: kv_copy(k).start())

    fz_copy(0, 1).start()
    f_own(0).start()
    out_far(3)
    f_row(1, 3)
    oz_copy(3).start()
    fz_copy(1, 3).start()

    def wy_copy(j, k):
        at = pl.ds(pl.multiple_of(((z ^ j ^ col) * row_size + (y ^ k)) * local, local), local)
        return remote(
            dw_out.at[at], row_o.at[k - 1, j], wy_send.at[k, j], wy_recv.at[k, j], {"row": y ^ k}
        )

    for j in far_first:
        for k in others:
            wy_copy(j, k).start()
    for j in far_first:
        for k in others:
            fy_copy(2, j, k).start()
    kv_load(len(others)).wait()
    attend_block(y, len(others) % 2)

    def back(r, first, second, at):
        c, s = cos_ref[r, :], sin_ref[r, :]
        graw[r, at : at + half] = (first * c + second * s).astype(low)
        graw[r, at + half : at + 2 * half] = (second * c - first * s).astype(low)

    def queries(r):
        for h in range(heads):
            at = h * HEAD_SIZE
            back(r, dq[r, at : at + half], dq[r, at + half : at + 2 * half], at)

    tiles(rows, 64, queries)
    for k in others:

        @pl.when((y ^ k) > y)
        def _():
            kv_copy(k).wait_recv()

            def add(r):
                dkv[r, :] = dkv[r, :] + dkv_in[k - 1, r, :].astype(wide)

            tiles(rows, 64, add)

    def keys_back(r):
        back(r, dkv[r, 0:half], dkv[r, half : 2 * half], q_cols)
        graw[r, q_cols + k_cols : all_cols] = dkv[r, k_cols : 2 * k_cols].astype(low)

    tiles(rows, 64, keys_back)
    loads[1].wait()
    loads[2].wait()
    f_row(1, 2)

    def ay_copy(j, k):
        at = pl.ds(pl.multiple_of(((z ^ j ^ col) * row_size + (y ^ k)) * local, local), local)
        return remote(
            dw_attn.at[at], row_a.at[k - 1, j], ay_send.at[k, j], ay_recv.at[k, j], {"row": y ^ k}
        )

    for p in range(4):
        at = slice(p * width, (p + 1) * width)
        for n in range(0, all_cols, 512):
            dw_attn[at, n : n + 512] = contract_rows(xn[:, at], graw[:, n : n + 512]).astype(low)
    fz_copy(1, 2).start()
    for which in range(3):
        t_copy(which).wait_send()
    part = full
    part_copy = remote(part.at[:, pl.ds(2 * width, 2 * width)], pcore_in, p_send, p_recv, core)
    for q, p in ((2, 1), (3, 3)):
        part[:, q * width : (q + 1) * width] = times_transposed(
            graw[...], aw[p * width : (p + 1) * width, :]
        ).astype(low)
    for j in far_first:
        for k in others:
            ay_copy(j, k).start()
    for q, p in ((0, 0), (1, 2)):
        part[:, q * width : (q + 1) * width] = times_transposed(
            graw[...], aw[p * width : (p + 1) * width, :]
        ).astype(low)
    part_copy.start()
    f_row(1, 1)
    f_row(1, 0)
    part_copy.wait()
    fz_copy(1, 1).start()
    f_own(1).start()

    def add_core(r):
        px_out[r, :] = (
            part[r, width : 2 * width].astype(wide) + pcore_in[r, width : 2 * width].astype(wide)
        ).astype(low)

    tiles(rows, 64, add_core)
    out_far(2)
    r_copy = remote(px_out, px_in, r_send, r_recv, far)
    r_copy.start()
    oz_copy(2).start()
    out_far(1)

    def wz_copy(j):
        return remote(z_o.at[j - 1], in_o.at[j - 1], wz_send.at[j], wz_recv.at[j], {"dp": z ^ j})

    def o_row(j):
        for k in others:
            wy_copy(j, k).wait_recv()
        at = pl.ds(pl.multiple_of(((z ^ j ^ col) * row_size + y) * local, local), local)
        total = dw_out[at, :].astype(wide)
        for k in others:
            total = total + row_o[k - 1, j].astype(wide)
        if j:
            z_o[j - 1] = total.astype(low)
        else:
            dwo_ref[...] = total

    o_row(3)
    oz_copy(1).start()
    out_far(0)
    o_row(2)
    wz_copy(3).start()
    o_row(1)
    wz_copy(2).start()
    o_row(0)
    wz_copy(1).start()
    r_copy.wait()

    def dxn(r):
        return (
            part[r, 0:width].astype(wide) + pcore_in[r, 0:width].astype(wide) + px_in[r, :].astype(wide)
        )

    def inner_one(i, total):
        r = pl.ds(pl.multiple_of(i * 64, 64), 64)
        grad, tokens = dxn(r), tok_ref[r, :].astype(wide)
        lanes[1, r, :] = lane_sums(gain_one * grad * tokens).astype(low)
        return total + jnp.sum(grad * tokens * factor_one_ref[r, 0:1], axis=0, keepdims=True)

    gain_one_grad = lax.fori_loop(0, rows // 64, inner_one, jnp.zeros((1, width), wide))
    for i in range(row_size):
        at = slice(i * local, (i + 1) * local)
        gvec[i, 0:1, :] = gain_one_grad[:, at]
        gvec[i, 1:2, :] = gain_two_grad[:, at]
        gvec[i, 2:8, :] = jnp.zeros((6, local), wide)
    f_row(2, 3)
    for m in (2, 3, 1):
        l_copy(1, m).start()
    mine = z == col

    def g_copy(k):
        return remote(
            gvec.at[y ^ k],
            g_in.at[z * row_size + y],
            g_send.at[k],
            g_recv.at[z, k],
            {"dp": col, "row": y ^ k},
        )

    for k in range(row_size):
        if k:
            g_copy(k).start()
        else:

            @pl.when(jnp.logical_not(mine))
            def _():
                g_copy(0).start()

            @pl.when(mine)
            def _():
                g_in[z * row_size + y] = gvec[y]

    fz_copy(2, 3).start()
    f_row(2, 2)
    f_row(2, 1)
    fz_copy(2, 2).start()
    f_row(2, 0)
    fz_copy(2, 1).start()
    f_own(2).start()
    for m in (1, 2, 3):
        l_copy(1, m).wait_recv()

    def grad_tokens(r):
        factor = factor_one_ref[r, 0:1]
        dtok_ref[r, :] = (
            dtok_ref[r, :].astype(wide)
            + factor * gain_one * dxn(r)
            - tok_ref[r, :].astype(wide) * factor * factor * factor * inner(1, r)
        ).astype(low)

    tiles(rows, 64, grad_tokens)

    def az_copy(j):
        return remote(z_a.at[j - 1], in_a.at[j - 1], az_send.at[j], az_recv.at[j], {"dp": z ^ j})

    def a_row(j):
        for k in others:
            ay_copy(j, k).wait_recv()
        at = pl.ds(pl.multiple_of(((z ^ j ^ col) * row_size + y) * local, local), local)
        total = dw_attn[at, :].astype(wide)
        for k in others:
            total = total + row_a[k - 1, j].astype(wide)
        if j:
            z_a[j - 1] = total.astype(low)
        else:
            dattn_ref[...] = total

    a_row(3)
    a_row(2)
    az_copy(3).start()
    a_row(1)
    az_copy(2).start()
    a_row(0)
    az_copy(1).start()

    def gc_copy(m):
        return remote(
            gains_ref, gains_ref, gc_send.at[m - 1], gc_recv, {"col": col ^ m}
        )

    @pl.when(mine)
    def _():
        for j in range(4):
            for k in range(row_size):
                if j + k:
                    block = g_in.at[(z ^ j) * row_size + (y ^ k)]
                    remote(
                        block, block, g_send.at[k], g_recv.at[z ^ j, k], {"dp": z ^ j, "row": y ^ k}
                    ).wait_recv()
        total = g_in[0]
        for i in range(1, 4 * row_size):
            total = total + g_in[i]
        gains_ref[...] = total

    for j in (1, 2, 3):
        oz_copy(j).wait_recv()

    @pl.when(mine)
    def _():
        for m in (1, 2, 3):
            gc_copy(m).start()

    def layer_out(r):
        total = h_ref[r, :] + out_own[0, r, 0:width].astype(wide)
        for j in (1, 2, 3):
            total = total + z_in[j - 1, r, :].astype(wide)
        layer_ref[r, :] = total.astype(low)

    tiles(rows, 64, layer_out)
    for j in (1, 2, 3):
        wz_copy(j).wait_recv()
        dwo_ref[...] = dwo_ref[...] + in_o[j - 1].astype(wide)
    for a in range(3):
        f_own(a).wait()
        for j in (1, 2, 3):
            at = pl.ds(pl.multiple_of((z ^ j) * hidden, hidden), hidden)
            block = results[a].at[:, at]
            remote(block, block, fz_send.at[a, j], fz_recv.at[a, j], {"dp": z ^ j}).wait_recv()
    for j in (1, 2, 3):
        az_copy(j).wait_recv()
        dattn_ref[...] = dattn_ref[...] + in_a[j - 1].astype(wide)

    @pl.when(jnp.logical_not(mine))
    def _():
        gc_copy(1).wait_recv()

    @pl.when(mine)
    def _():
        for m in (1, 2, 3):
            gc_copy(m).wait_send()

    for k in range(row_size):
        if k:
            g_copy(k).wait_send()
        else:

            @pl.when(jnp.logical_not(mine))
            def _():
                g_copy(0).wait_send()

    for n in (0, 1):
        for m in (1, 2, 3):
            l_copy(n, m).wait_send()
    for j in range(4):
        ox_copy(j).wait_send()
        for which in (0, 1):
            oc_copy(j, which).wait_send()
        if j:
            oz_copy(j).wait_send()
            wz_copy(j).wait_send()
            az_copy(j).wait_send()
            for a in range(3):
                fz_copy(a, j).wait_send()
        for k in others:
            wy_copy(j, k).wait_send()
            ay_copy(j, k).wait_send()
            for a in range(3):
                fy_copy(a, j, k).wait_send()
    when_block(row_size - 1, lambda: kv_copy(row_size - 1).wait_send())


def attn_bwd_call(
    dhn,
    factor_two,
    h,
    dout,
    gains,
    tokens,
    factor_one,
    cos,
    sin,
    valid,
    q,
    lse,
    mix,
    xn,
    kv,
    aw,
    wo,
    out_part,
    dwg,
    dwu,
    dwd,
):
    rows, width = tokens.shape
    model, hidden = dwg.shape
    low, wide = jnp.bfloat16, jnp.float32
    row_size = lax.axis_size("row")
    local = model // (4 * row_size)
    all_cols, q_cols = aw.shape[1], wo.shape[1]
    heads = q_cols // HEAD_SIZE
    kv_cols = kv.shape[2]
    vmem = pl.BlockSpec(memory_space=pltpu.VMEM)
    hbm = pl.BlockSpec(memory_space=pl.ANY)
    dma = pltpu.SemaphoreType.DMA
    shape = jax.ShapeDtypeStruct
    blocks = [part.reshape(4, row_size, local, hidden) for part in (dwg, dwu, dwd)]
    return pl.pallas_call(
        attn_bwd_kernel,
        out_shape=(
            shape((rows, width), low),
            shape((rows, width), low),
            shape((8, local), wide),
            shape((local, all_cols), wide),
            shape((local, q_cols), wide),
            shape((local, 4 * hidden), low),
            shape((local, 4 * hidden), low),
            shape((local, 4 * hidden), low),
        ),
        in_specs=[vmem] * 13 + [hbm] * 8,
        out_specs=(vmem,) * 5 + (hbm,) * 3,
        scratch_shapes=[
            pltpu.VMEM((rows, model), low),
            pltpu.VMEM((rows, model), low),
            pltpu.VMEM((2, rows, kv_cols), low),
            pltpu.VMEM((model, all_cols), low),
            pltpu.VMEM((model, q_cols), low),
            pltpu.VMEM((2, rows, 128), low),
            pltpu.VMEM((2, 3, rows, 128), low),
            pltpu.VMEM((rows, q_cols), low),
            pltpu.VMEM((heads, rows, 128), wide),
            pltpu.VMEM((rows, q_cols), wide),
            pltpu.VMEM((rows, kv_cols), wide),
            pltpu.VMEM((rows, kv_cols), low),
            pltpu.VMEM((row_size - 1, rows, kv_cols), low),
            pltpu.VMEM((rows, all_cols), low),
            pltpu.VMEM((model, all_cols), low),
            pltpu.VMEM((model, q_cols), low),
            pltpu.VMEM((3, 4, local, hidden), low),
            pltpu.VMEM((3, row_size - 1, 4, local, hidden), low),
            pltpu.VMEM((row_size - 1, 4, local, all_cols), low),
            pltpu.VMEM((row_size - 1, 4, local, q_cols), low),
            pltpu.VMEM((3, local, all_cols), low),
            pltpu.VMEM((3, local, q_cols), low),
            pltpu.VMEM((3, local, all_cols), low),
            pltpu.VMEM((3, local, q_cols), low),
            pltpu.VMEM((4, rows, 2 * width), low),
            pltpu.VMEM((4, rows, 2 * width), low),
            pltpu.VMEM((4, rows, width), low),
            pltpu.VMEM((3, rows, width), low),
            pltpu.VMEM((rows, 2 * width), low),
            pltpu.VMEM((rows, width), low),
            pltpu.VMEM((rows, width), low),
            pltpu.VMEM((row_size, 8, local), wide),
            pltpu.VMEM((4 * row_size, 8, local), wide),
            dma((5,)),
            dma((2, 3)),
            dma((2, 3)),
            dma((3,)),
            dma((3,)),
            dma((3, row_size, 4)),
            dma((3, row_size, 4)),
            dma((3, 4)),
            dma((3, 4)),
            dma((3, 4)),
            dma((2, 4)),
            dma((2, 4)),
            dma((2, 4)),
            dma((4,)),
            dma((4,)),
            dma((4,)),
            dma((4,)),
            dma((row_size,)),
            dma((row_size,)),
            dma((row_size, 4)),
            dma((row_size, 4)),
            dma((4,)),
            dma((4,)),
            dma((row_size, 4)),
            dma((row_size, 4)),
            dma((4,)),
            dma((4,)),
            dma(()),
            dma(()),
            dma(()),
            dma(()),
            dma((row_size,)),
            dma((4, row_size)),
            dma((3,)),
            dma(()),
        ],
        compiler_params=pltpu.CompilerParams(
            collective_id=3, has_side_effects=True, vmem_limit_bytes=66_000_000
        ),
        cost_estimate=pl.CostEstimate(
            flops=14_000_000_000, bytes_accessed=40_000_000, transcendentals=2_000_000
        ),
    )(
        dhn,
        factor_two,
        h,
        dout,
        gains,
        tokens,
        factor_one,
        cos,
        sin,
        valid,
        q,
        lse,
        mix,
        xn,
        kv,
        aw,
        wo,
        out_part,
        *blocks,
    )


def per_device(
    tokens,
    w_query,
    key_matrix,
    value_matrix,
    w_output,
    w_gate,
    w_up,
    w_down,
    gain_attn,
    gain_ffn,
    lengths,
    cotangent,
):
    low = jnp.bfloat16
    wide = jnp.float32
    row_count = tokens.shape[0]
    me_row = lax.axis_index("row")
    query_pos = me_row * row_count + jnp.arange(row_count, dtype=jnp.int32)
    valid = (query_pos < lengths[0]).astype(wide)[:, None]
    cosine_table, sine_table = rope_tables(query_pos.astype(wide))

    gains = jnp.zeros((8, gain_attn.shape[0]), wide)
    gains = gains.at[0].set(gain_attn.astype(wide)).at[1].set(gain_ffn.astype(wide))
    q_cols, k_cols = w_query.shape[1], key_matrix.shape[1]
    grad_out = (cotangent.astype(wide) * valid).astype(low)
    (
        normed,
        factor_one,
        query_rows,
        kv_all,
        log_total,
        mixed_heads,
        residual,
        attn_weight,
        out_weight,
        gains,
        gate_weight,
        up_weight,
        down_weight,
        grad_out_full,
    ) = attn_fwd_call(
        tokens,
        grad_out,
        gains,
        cosine_table,
        sine_table,
        valid,
        w_query,
        key_matrix,
        value_matrix,
        w_output.T,
        w_gate,
        w_up,
        w_down.T,
    )
    residual_low = residual.astype(low)
    grad_normed_two, factor_two, out_part, grad_gate_part, grad_up_part, grad_down_part = ffn_call(
        residual_low, gains[1:2], grad_out_full, gate_weight, up_weight, down_weight
    )
    (
        layer_out,
        grad_tokens,
        gain_grads,
        grad_attn,
        grad_output,
        grad_gate,
        grad_up,
        grad_down,
    ) = attn_bwd_call(
        grad_normed_two,
        factor_two,
        residual,
        grad_out,
        gains,
        tokens,
        factor_one,
        cosine_table,
        sine_table,
        valid,
        query_rows,
        log_total,
        mixed_heads,
        normed,
        kv_all,
        attn_weight,
        out_weight,
        out_part,
        grad_gate_part,
        grad_up_part,
        grad_down_part,
    )
    return (
        layer_out,
        grad_tokens,
        gain_grads[0],
        gain_grads[1],
        grad_attn[:, :q_cols],
        grad_attn[:, q_cols : q_cols + k_cols],
        grad_attn[:, q_cols + k_cols :],
        grad_output.T,
        grad_gate.astype(wide),
        grad_up.astype(wide),
        grad_down.T.astype(wide),
    )


def solution(mesh):
    in_specs = (
        P(("dp", "row"), "col"),
        P(("dp", "row"), "col"),
        P(("dp", "row"), "col"),
        P(("dp", "row"), "col"),
        P("col", ("dp", "row")),
        P(("dp", "row"), "col"),
        P(("dp", "row"), "col"),
        P("col", ("dp", "row")),
        P(("dp", "row")),
        P(("dp", "row")),
        P("dp"),
        P(("dp", "row"), "col"),
    )
    out_specs = (
        P(("dp", "row"), "col"),
        P(("dp", "row"), "col"),
        P(("dp", "row")),
        P(("dp", "row")),
        P(("dp", "row"), "col"),
        P(("dp", "row"), "col"),
        P(("dp", "row"), "col"),
        P("col", ("dp", "row")),
        P(("dp", "row"), "col"),
        P(("dp", "row"), "col"),
        P("col", ("dp", "row")),
    )
    return jax.shard_map(
        per_device, mesh=mesh, in_specs=in_specs, out_specs=out_specs, check_vma=False
    )
```

```python
import math

import jax
import jax.numpy as jnp
from jax import lax
from jax.experimental import pallas as pl
from jax.experimental.pallas import tpu as pltpu
from jax.sharding import PartitionSpec as P

HEAD_SIZE = 256
EPSILON = 1e-06
ROPE_BASE = 1000042.0


def rope_tables(positions):
    half = HEAD_SIZE // 2
    freq = ROPE_BASE ** (-jnp.arange(half, dtype=jnp.float32) * 2.0 / HEAD_SIZE)
    angle = positions[:, None] * freq[None, :]
    return (jnp.cos(angle), jnp.sin(angle))


def contract_rows(left, right):
    return lax.dot_general(
        left, right, (((0,), (0,)), ((), ())), preferred_element_type=jnp.float32
    )


def times_transposed(left, right):
    return lax.dot_general(
        left, right, (((1,), (1,)), ((), ())), preferred_element_type=jnp.float32
    )


def dot_nn(left, right):
    return lax.dot_general(left, right, (((1,), (0,)), ((), ())), preferred_element_type=jnp.float32)


def tiles(count, size, body):
    def step(i, unused):
        body(pl.ds(pl.multiple_of(i * size, size), size))
        return unused

    lax.fori_loop(0, count // size, step, 0)


def remote(src, dst, send_sem, recv_sem, target):
    return pltpu.make_async_remote_copy(
        src_ref=src,
        dst_ref=dst,
        send_sem=send_sem,
        recv_sem=recv_sem,
        device_id=target,
        device_id_type=pl.DeviceIdType.MESH,
    )


def greet(targets):
    barrier = pltpu.get_barrier_semaphore()
    for target in targets:
        pl.semaphore_signal(
            barrier, inc=1, device_id=target, device_id_type=pl.DeviceIdType.MESH
        )
    pl.semaphore_wait(barrier, len(targets))


def ffn_kernel(
    h_ref,
    gain_ref,
    do_hbm,
    wg_hbm,
    wu_hbm,
    wd_hbm,
    dhn_ref,
    factor_ref,
    out_hbm,
    dwg_hbm,
    dwu_hbm,
    dwd_hbm,
    full,
    do,
    wg,
    wu,
    wd,
    hid,
    dg,
    du,
    gate,
    up,
    dhid,
    part,
    outp,
    core_in,
    x_out,
    x_in,
    z_out,
    z_in,
    stage,
    load_sem,
    z_send,
    f_send,
    z_recv,
    x_send,
    x_recv,
    c_send,
    c_recv,
    p_send,
    p_recv,
    rx_send,
    rx_recv,
    rz_send,
    rz_recv,
    o_sem,
    s_sem,
):
    rows, width = h_ref.shape
    model = width * 4
    hidden = wg.shape[1]
    low, wide = jnp.bfloat16, jnp.float32
    z, col = lax.axis_index("dp"), lax.axis_index("col")
    core, far = {"col": col ^ 1}, {"col": col ^ 2}
    mid = jnp.logical_and(z > 0, z < 3)

    def chunk(s):
        return jnp.where(jnp.logical_and(mid, s >= 2), 5 - s, s)

    def cols(p):
        return pl.ds(p * width, width)

    greet([{"dp": z ^ 1}, {"dp": z ^ 2}, {"dp": z ^ 3}, core, far])

    def z_own(target, index):
        slot = z ^ target
        return remote(
            h_ref, full.at[slot, :, cols(0)], z_send.at[index], z_recv.at[slot], {"dp": target}
        )

    @pl.when(z < 3)
    def _():
        z_own(z + 1, 0).start()

    @pl.when(z > 0)
    def _():
        z_own(z - 1, 1).start()

    def x_copy(j, src):
        return remote(src, full.at[j, :, cols(2)], x_send.at[j], x_recv.at[j], far)

    def c_copy(j, src, which):
        return remote(
            src, full.at[j, :, cols(1 + 2 * which)], c_send.at[which, j], c_recv.at[which, j], core
        )

    x_copy(0, h_ref).start()
    c_copy(0, h_ref, 0).start()
    loads = [
        pltpu.make_async_copy(wg_hbm, wg, load_sem.at[0]),
        pltpu.make_async_copy(wu_hbm, wu, load_sem.at[1]),
        pltpu.make_async_copy(wd_hbm, wd, load_sem.at[2]),
    ]
    for load in loads:
        load.start()

    def do_load(j):
        return pltpu.make_async_copy(do_hbm.at[j], do.at[j], load_sem.at[3 + j])

    for j in range(4):
        do_load(j).start()

    def copy_own(r):
        full[0, r, 0:width] = h_ref[r, :]

    tiles(rows, 64, copy_own)

    def forward(j, target):
        return remote(
            full.at[j, :, cols(0)],
            full.at[(z ^ j) ^ target, :, cols(0)],
            f_send.at[j],
            z_recv.at[(z ^ j) ^ target],
            {"dp": target},
        )

    def goes_up(j):
        return jnp.logical_and((z ^ j) < z, z < 3)

    def goes_down(j):
        return jnp.logical_and((z ^ j) > z, z > 0)

    def arrive(j):
        block = full.at[j, :, cols(0)]
        remote(block, block, f_send.at[j], z_recv.at[j], core).wait_recv()

        @pl.when(goes_up(j))
        def _():
            forward(j, z + 1).start()

        @pl.when(goes_down(j))
        def _():
            forward(j, z - 1).start()

        x_copy(j, block).start()
        c_copy(j, block, 0).start()

    def settle(j):
        block = full.at[j, :, cols(0)]
        x_copy(j, block).wait_recv()
        c_copy(j, full.at[j, :, cols(2)], 1).start()
        x_copy(j, block).wait_send()
        c_copy(j, block, 0).wait_send()

        @pl.when(jnp.logical_and(j > 0, jnp.logical_or(goes_up(j), goes_down(j))))
        def _():
            forward(j, z ^ j).wait_send()

        c_copy(j, block, 0).wait_recv()
        c_copy(j, block, 1).wait()

    def part_copy(s, slot):
        return remote(
            part.at[slot, :, pl.ds(2 * width, 2 * width)],
            core_in.at[s],
            p_send.at[s],
            p_recv.at[s],
            core,
        )

    def rx_copy(s):
        return remote(x_out.at[s], x_in.at[s], rx_send.at[s], rx_recv.at[s], far)

    def rz_copy(s, j):
        return remote(z_out.at[s], z_in.at[j], rz_send.at[s], rz_recv.at[j], {"dp": z ^ j})

    def reduce_core(s):
        slot = lax.rem(s, 2)
        part_copy(s, slot).wait()

        def add(r):
            x_out[s, r, :] = (
                part[slot, r, width : 2 * width].astype(wide)
                + core_in[s, r, width : 2 * width].astype(wide)
            ).astype(low)
            z_out[s, r, :] = (
                part[slot, r, 0:width].astype(wide) + core_in[s, r, 0:width].astype(wide)
            ).astype(low)

        tiles(rows, 64, add)
        rx_copy(s).start()

    def reduce_far(s):
        rx_copy(s).wait()

        def add(r):
            z_out[s, r, :] = (z_out[s, r, :].astype(wide) + x_in[s, r, :].astype(wide)).astype(low)

        tiles(rows, 64, add)

        @pl.when(s > 0)
        def _():
            rz_copy(s, chunk(s)).start()

    def out_copy(s):
        return pltpu.make_async_copy(
            outp.at[lax.rem(s, 2)], out_hbm.at[chunk(s)], o_sem.at[lax.rem(s, 2)]
        )

    def step(s, unused):
        j = chunk(s)
        base = s * rows

        @pl.when(jnp.logical_and(s < 3, jnp.logical_not(jnp.logical_and(s == 1, mid))))
        def _():
            arrive(chunk(s + 1))

        @pl.when(jnp.logical_and(s == 0, mid))
        def _():
            arrive(chunk(2))

        settle(j)

        def norm(r):
            x = full[j, r, :].astype(wide)
            factor = lax.rsqrt(jnp.sum(x * x, axis=1, keepdims=True) * (1.0 / model) + EPSILON)
            full[j, r, :] = (x * factor * gain_ref[...]).astype(low)

            @pl.when(s == 0)
            def _():
                factor_ref[r, :] = jnp.broadcast_to(factor, (factor.shape[0], 128))

        tiles(rows, 32, norm)

        @pl.when(s == 0)
        def _():
            for load in loads:
                load.wait()

        gate[...] = dot_nn(full[j], wg[...])
        up[...] = dot_nn(full[j], wu[...])

        @pl.when(s > 0)
        def _():
            reduce_core(s - 1)

        do_load(j).wait()
        dhid[...] = dot_nn(do[j], wd[...])

        def act(r):
            g = gate[r, :]
            u = up[r, :]
            d = dhid[r, :]
            sig = jax.nn.sigmoid(g)
            silu = g * sig
            at = pl.ds(pl.multiple_of(base + r.start, 64), 64)
            hid[at, :] = (silu * u).astype(low)
            dg[at, :] = (d * u * sig * (1.0 + g * (1.0 - sig))).astype(low)
            du[at, :] = (d * silu).astype(low)

        tiles(rows, 64, act)
        slot = lax.rem(s, 2)
        mine = pl.ds(pl.multiple_of(base, rows), rows)

        def dhn(q, p):
            w_rows = slice(p * width, (p + 1) * width)
            part[slot, :, q * width : (q + 1) * width] = (
                times_transposed(dg[mine, :], wg[w_rows, :])
                + times_transposed(du[mine, :], wu[w_rows, :])
            ).astype(low)

        dhn(2, 1)
        dhn(3, 3)
        dhn(0, 0)
        part_copy(s, slot).start()
        dhn(1, 2)

        @pl.when(s > 0)
        def _():
            reduce_far(s - 1)

        @pl.when(s >= 2)
        def _():
            out_copy(s - 2).wait()

        for p in range(4):
            outp[slot, :, p * width : (p + 1) * width] = times_transposed(
                hid[mine, :], wd[p * width : (p + 1) * width, :]
            ).astype(low)
        out_copy(s).start()
        return unused

    lax.fori_loop(0, 4, step, 0)

    reduce_core(3)
    count = model // width

    def stage_copy(target, i, slot):
        at = pl.ds(pl.multiple_of(i * width, width), width)
        return pltpu.make_async_copy(stage.at[slot], target.at[at, :], s_sem.at[slot])

    def weight_grad(target, right, left_of, first):
        def tile(i, unused):
            slot = lax.rem(i, 2)

            @pl.when(jnp.logical_or(i >= 2, not first))
            def _():
                stage_copy(target, 0, slot).wait()

            total = left_of(0, i, right)
            for s in range(1, 4):
                total = total + left_of(s, i, right)
            stage[slot] = total.astype(low)
            stage_copy(target, i, slot).start()
            return unused

        lax.fori_loop(0, count, tile, 0)

    def from_full(s, i, right):
        at = pl.ds(pl.multiple_of(i * width, width), width)
        return contract_rows(full[chunk(s), :, at], right[s * rows : (s + 1) * rows, :])

    def from_do(s, i, right):
        at = pl.ds(pl.multiple_of(i * width, width), width)
        return contract_rows(do[chunk(s), :, at], right[s * rows : (s + 1) * rows, :])

    weight_grad(dwg_hbm, dg, from_full, True)
    reduce_far(3)
    weight_grad(dwu_hbm, du, from_full, False)
    weight_grad(dwd_hbm, hid, from_do, False)
    stage_copy(dwd_hbm, 0, 0).wait()
    stage_copy(dwd_hbm, 0, 1).wait()
    out_copy(2).wait()
    out_copy(3).wait()
    for s in range(1, 4):
        rz_copy(s, chunk(s)).wait()

    def final(r):
        total = z_out[0, r, :].astype(wide)
        for j in range(1, 4):
            total = total + z_in[j, r, :].astype(wide)
        dhn_ref[r, :] = total

    tiles(rows, 64, final)

    @pl.when(z < 3)
    def _():
        z_own(z + 1, 0).wait_send()

    @pl.when(z > 0)
    def _():
        z_own(z - 1, 1).wait_send()


def ffn_call(h_low, gain, grad_full, wg, wu, wd):
    rows, width = h_low.shape
    model, hidden = wg.shape
    low, wide = jnp.bfloat16, jnp.float32
    vmem = pl.BlockSpec(memory_space=pltpu.VMEM)
    hbm = pl.BlockSpec(memory_space=pl.ANY)
    dma = pltpu.SemaphoreType.DMA
    tokens = 4 * rows
    return pl.pallas_call(
        ffn_kernel,
        out_shape=(
            jax.ShapeDtypeStruct((rows, width), wide),
            jax.ShapeDtypeStruct((rows, 128), wide),
            jax.ShapeDtypeStruct((4, rows, model), low),
            jax.ShapeDtypeStruct((model, hidden), low),
            jax.ShapeDtypeStruct((model, hidden), low),
            jax.ShapeDtypeStruct((model, hidden), low),
        ),
        in_specs=[vmem, vmem, hbm, hbm, hbm, hbm],
        out_specs=(vmem, vmem, hbm, hbm, hbm, hbm),
        scratch_shapes=[
            pltpu.VMEM((4, rows, model), low),
            pltpu.VMEM((4, rows, model), low),
            pltpu.VMEM((model, hidden), low),
            pltpu.VMEM((model, hidden), low),
            pltpu.VMEM((model, hidden), low),
            pltpu.VMEM((tokens, hidden), low),
            pltpu.VMEM((tokens, hidden), low),
            pltpu.VMEM((tokens, hidden), low),
            pltpu.VMEM((rows, hidden), wide),
            pltpu.VMEM((rows, hidden), wide),
            pltpu.VMEM((rows, hidden), wide),
            pltpu.VMEM((2, rows, model), low),
            pltpu.VMEM((2, rows, model), low),
            pltpu.VMEM((4, rows, 2 * width), low),
            pltpu.VMEM((4, rows, width), low),
            pltpu.VMEM((4, rows, width), low),
            pltpu.VMEM((4, rows, width), low),
            pltpu.VMEM((4, rows, width), low),
            pltpu.VMEM((2, width, hidden), low),
            dma((7,)),
            dma((2,)),
            dma((4,)),
            dma((4,)),
            dma((4,)),
            dma((4,)),
            dma((2, 4)),
            dma((2, 4)),
            dma((4,)),
            dma((4,)),
            dma((4,)),
            dma((4,)),
            dma((4,)),
            dma((4,)),
            dma((2,)),
            dma((2,)),
        ],
        compiler_params=pltpu.CompilerParams(
            collective_id=2, has_side_effects=True, vmem_limit_bytes=66_000_000
        ),
        cost_estimate=pl.CostEstimate(
            flops=18 * tokens * model * hidden,
            bytes_accessed=40_000_000,
            transcendentals=tokens * hidden,
        ),
    )(h_low, gain, grad_full, wg, wu, wd)


class Relay:
    def __init__(self, z, place, own_send, forward_send, recv):
        self.z, self.place = z, place
        self.own_send, self.forward_send, self.recv = own_send, forward_send, recv

    def own_copy(self, src, target, index):
        return remote(
            src,
            self.place(self.z, target),
            self.own_send.at[index],
            self.recv.at[self.z],
            {"dp": target},
        )

    def own(self, src, wait=False):
        @pl.when(self.z < 3)
        def _():
            copy = self.own_copy(src, self.z + 1, 0)
            copy.wait_send() if wait else copy.start()

        @pl.when(self.z > 0)
        def _():
            copy = self.own_copy(src, self.z - 1, 1)
            copy.wait_send() if wait else copy.start()

    def forward_copy(self, o, target):
        return remote(
            self.place(o, self.z),
            self.place(o, target),
            self.forward_send.at[o],
            self.recv.at[o],
            {"dp": target},
        )

    def forward(self, o, wait=False):
        @pl.when(jnp.logical_and(o < self.z, self.z < 3))
        def _():
            copy = self.forward_copy(o, self.z + 1)
            copy.wait_send() if wait else copy.start()

        @pl.when(jnp.logical_and(o > self.z, self.z > 0))
        def _():
            copy = self.forward_copy(o, self.z - 1)
            copy.wait_send() if wait else copy.start()

    def arrive(self, o):
        self.forward_copy(o, self.z ^ 1).wait_recv()
        self.forward(o)


def attn_fwd_kernel(
    tok_ref,
    cot_ref,
    gains_ref,
    cos_ref,
    sin_ref,
    valid_ref,
    wq_hbm,
    wk_hbm,
    wv_hbm,
    wo_hbm,
    wg_hbm,
    wu_hbm,
    wd_hbm,
    xn_ref,
    factor_ref,
    q_ref,
    kv_ref,
    lse_ref,
    mix_ref,
    h_ref,
    aw_ref,
    wo_ref,
    gain_ref,
    fg_hbm,
    fu_hbm,
    fd_hbm,
    do_hbm,
    full,
    qkv,
    gain_in,
    own_piece,
    part,
    core_in,
    x_out,
    x_in,
    load_sem,
    piece_sem,
    do_sem,
    g_send,
    g_recv,
    x_send,
    x_recv,
    t_send,
    t_recv,
    a_own,
    a_fwd,
    a_recv,
    ay_send,
    ay_recv,
    o_own,
    o_fwd,
    o_recv,
    oy_send,
    oy_recv,
    f_send,
    f_recv,
    fy_send,
    fy_recv,
    d_own,
    d_fwd,
    d_recv,
    dx_send,
    dx_recv,
    dc_send,
    dc_recv,
    kv_send,
    kv_recv,
    p_send,
    p_recv,
    r_send,
    r_recv,
):
    rows, width = tok_ref.shape
    model = 4 * width
    low, wide = jnp.bfloat16, jnp.float32
    row_size = lax.axis_size("row")
    local = wq_hbm.shape[0]
    q_cols, k_cols = wq_hbm.shape[1], wk_hbm.shape[1]
    hidden = fg_hbm.shape[1]
    half = HEAD_SIZE // 2
    z, y, col = (lax.axis_index(name) for name in ("dp", "row", "col"))
    core, far = {"col": col ^ 1}, {"col": col ^ 2}
    mid = jnp.logical_and(z > 0, z < 3)
    others = range(1, row_size)

    def chunk(s):
        return jnp.where(mid, 5 - s, s) if s >= 2 else s

    def cols(p):
        return pl.ds(p * width, width)

    def slot(o, r):
        return pl.ds(pl.multiple_of(((o ^ col) * row_size + r) * local, local), local)

    greet(
        [{"dp": z ^ j, "row": y ^ k} for j in range(4) for k in range(row_size) if j + k > 0]
        + [core, far]
    )

    loads = [
        pltpu.make_async_copy(src, aw_ref.at[slot(z, y), pl.ds(at, src.shape[1])], load_sem.at[i])
        for i, (src, at) in enumerate(
            ((wq_hbm, 0), (wk_hbm, q_cols), (wv_hbm, q_cols + k_cols))
        )
    ]
    load_out = pltpu.make_async_copy(wo_hbm, wo_ref.at[slot(z, y)], load_sem.at[3])
    for load in loads:
        load.start()
    load_out.start()

    def t_copy(which):
        src = full.at[:, cols(2)] if which == 2 else tok_ref
        target = far if which == 1 else core
        dst = full.at[:, cols((1, 2, 3)[which])]
        return remote(src, dst, t_send.at[which], t_recv.at[which], target)

    t_copy(1).start()
    t_copy(0).start()

    def g_copy(j, k):
        at = (z ^ col) * row_size + y
        return remote(
            gains_ref,
            gain_in.at[at],
            g_send.at[j, k],
            g_recv.at[j, k],
            {"dp": z ^ j, "row": y ^ k},
        )

    pairs = [(j, k) for j in range(4) for k in range(row_size) if j + k > 0]
    for j, k in pairs:
        g_copy(j, k).start()
    gain_in[(z ^ col) * row_size + y] = gains_ref[...]

    attn = Relay(z, lambda o, t: aw_ref.at[slot(o, y)], a_own, a_fwd, a_recv)
    outw = Relay(z, lambda o, t: wo_ref.at[slot(o, y)], o_own, o_fwd, o_recv)
    douts = Relay(z, lambda o, t: do_hbm.at[o ^ t, :, cols(0)], d_own, d_fwd, d_recv)

    def row_copy(ref, o, k, send, recv):
        block = ref.at[slot(o, y)]
        return remote(block, block, send.at[k, o], recv.at[k, o], {"row": y ^ k})

    def row_wait(ref, o, k, send, recv):
        block = ref.at[slot(o, y ^ k)]
        remote(block, block, send.at[k, o], recv.at[k, o], {"row": y ^ k}).wait_recv()

    for load in loads:
        load.wait()
    attn.own(aw_ref.at[slot(z, y)])
    for k in others:
        row_copy(aw_ref, z, k, ay_send, ay_recv).start()

    weights = ((wg_hbm, fg_hbm), (wu_hbm, fu_hbm), (wd_hbm, fd_hbm))

    def quarter(j):
        return pl.ds(pl.multiple_of((z ^ j) * hidden, hidden), hidden)

    pieces = [
        pltpu.make_async_copy(weights[a][0].at[:, quarter(0)], own_piece.at[a], piece_sem.at[a])
        for a in range(3)
    ]
    for piece in pieces:
        piece.start()

    full[:, 0:width] = tok_ref[...]
    t_copy(1).wait_recv()
    t_copy(2).start()
    attn.arrive(z ^ 1)
    for k in others:
        row_copy(aw_ref, z ^ 1, k, ay_send, ay_recv).start()
    load_out.wait()

    def attn_arrive(j):
        attn.arrive(z ^ j)
        for k in others:
            row_copy(aw_ref, z ^ j, k, ay_send, ay_recv).start()

    @pl.when(mid)
    def _():
        attn_arrive(3)

    outw.own(wo_ref.at[slot(z, y)])

    for j, k in pairs:
        g_copy(j, k).wait_recv()
    for i in range(4 * row_size):
        gain_ref[:, i * local : (i + 1) * local] = gain_in[i]
    t_copy(0).wait_recv()
    t_copy(2).wait_recv()

    def norm(r):
        x = full[r, :].astype(wide)
        factor = lax.rsqrt(jnp.sum(x * x, axis=1, keepdims=True) * (1.0 / model) + EPSILON)
        xn_ref[r, :] = (x * factor * gain_ref[0:1, :]).astype(low)
        factor_ref[r, :] = jnp.broadcast_to(factor, (factor.shape[0], 128))

    tiles(rows, 32, norm)

    @pl.when(jnp.logical_not(mid))
    def _():
        attn_arrive(2)

    attn_arrive_last = jnp.where(mid, 2, 3)
    attn.arrive(z ^ attn_arrive_last)
    for k in others:
        row_copy(aw_ref, z ^ attn_arrive_last, k, ay_send, ay_recv).start()
    for s in range(1, 4):
        outw.arrive(z ^ chunk(s))

    def f_copy(a, j):
        src, dst = weights[a]
        return remote(
            src.at[:, quarter(j)],
            dst.at[slot(z, y)],
            f_send.at[a, j],
            f_recv.at[a, j],
            {"dp": z ^ j},
        )

    for a in range(3):
        for j in (3, 2, 1):
            f_copy(a, j).start()

    def fy_copy(a, j, k):
        src = own_piece.at[a] if j == 0 else weights[a][1].at[slot(z ^ j, y)]
        return remote(
            src,
            weights[a][1].at[slot(z ^ j, y)],
            fy_send.at[a, k, j],
            fy_recv.at[a, k, j],
            {"row": y ^ k},
        )

    for o in range(4):
        for k in others:
            row_wait(aw_ref, o, k, ay_send, ay_recv)
    for n in range(0, q_cols + 2 * k_cols, 512):
        qkv[:, n : n + 512] = dot_nn(xn_ref[...], aw_ref[:, n : n + 512])

    def rope(r, at):
        c, s = cos_ref[r, :], sin_ref[r, :]
        first, second = qkv[r, at : at + half], qkv[r, at + half : at + 2 * half]
        return first * c - second * s, second * c + first * s

    def keys(r):
        first, second = rope(r, q_cols)
        kv_ref[y, r, 0:half] = first.astype(low)
        kv_ref[y, r, half : 2 * half] = second.astype(low)
        kv_ref[y, r, k_cols : 2 * k_cols] = qkv[r, q_cols + k_cols : q_cols + 2 * k_cols].astype(low)

    tiles(rows, 64, keys)
    heads = q_cols // HEAD_SIZE

    def queries(r):
        for h in range(heads):
            first, second = rope(r, h * HEAD_SIZE)
            q_ref[h, r, 0:half] = first.astype(low)
            q_ref[h, r, half : 2 * half] = second.astype(low)

    tiles(rows, 64, queries)

    def kv_copy(k, source):
        block = kv_ref.at[source]
        return remote(block, block, kv_send.at[k], kv_recv.at[k], {"row": y ^ k})

    for k in others:

        @pl.when((y ^ k) > y)
        def _():
            kv_copy(k, y).start()

    for o in range(4):
        for k in others:
            row_copy(wo_ref, o, k, oy_send, oy_recv).start()

    douts.own(cot_ref)

    def dx_copy(j):
        src = cot_ref if j == 0 else do_hbm.at[j, :, cols(0)]
        return remote(src, do_hbm.at[j, :, cols(2)], dx_send.at[j], dx_recv.at[j], far)

    def dc_copy(j, which):
        if which:
            src = do_hbm.at[j, :, cols(2)]
        else:
            src = cot_ref if j == 0 else do_hbm.at[j, :, cols(0)]
        return remote(
            src, do_hbm.at[j, :, cols(1 + 2 * which)], dc_send.at[which, j], dc_recv.at[which, j], core
        )

    dx_copy(0).start()
    dc_copy(0, 0).start()
    do_own = pltpu.make_async_copy(cot_ref, do_hbm.at[0, :, cols(0)], do_sem)
    do_own.start()
    for piece in pieces:
        piece.wait()
    stores = [
        pltpu.make_async_copy(own_piece.at[a], weights[a][1].at[slot(z, y)], piece_sem.at[a])
        for a in range(3)
    ]
    for a in range(3):
        stores[a].start()
        for k in others:
            fy_copy(a, 0, k).start()
    for k in others:

        @pl.when((y ^ k) < y)
        def _():
            kv_copy(k, y ^ k).wait_recv()

    q_tile = 256
    score_scale = 1.0 / math.sqrt(HEAD_SIZE)

    def attend_tile(i, unused):
        at = pl.ds(pl.multiple_of(i * q_tile, q_tile), q_tile)
        query_pos = y * rows + i * q_tile + lax.broadcasted_iota(jnp.int32, (q_tile, rows), 0)
        for h in range(heads):
            query = q_ref[h, at, :]

            def block(b, carry):
                top, total, accum = carry
                scores = times_transposed(query, kv_ref[b, :, 0:k_cols]) * score_scale
                key_pos = b * rows + lax.broadcasted_iota(jnp.int32, (q_tile, rows), 1)
                scores = jnp.where(key_pos <= query_pos, scores, -1e30)
                new_top = jnp.maximum(top, jnp.max(scores, axis=1, keepdims=True))
                probs = jnp.exp(scores - new_top)
                keep = jnp.exp(top - new_top)
                total = total * keep + jnp.sum(probs, axis=1, keepdims=True)
                accum = accum * keep + dot_nn(probs.astype(low), kv_ref[b, :, k_cols : 2 * k_cols])
                return new_top, total, accum

            top, total, accum = lax.fori_loop(
                0,
                y + 1,
                block,
                (
                    jnp.full((q_tile, 1), -1e30, wide),
                    jnp.zeros((q_tile, 1), wide),
                    jnp.zeros((q_tile, HEAD_SIZE), wide),
                ),
            )
            lse_ref[h, at, :] = jnp.broadcast_to(top + jnp.log(total), (q_tile, 128))
            mix_ref[at, h * HEAD_SIZE : (h + 1) * HEAD_SIZE] = (
                accum / total * valid_ref[at, :]
            ).astype(low)
        return unused

    lax.fori_loop(0, rows // q_tile, attend_tile, 0)

    for o in range(4):
        for k in others:
            row_wait(wo_ref, o, k, oy_send, oy_recv)
    part_copy = remote(part.at[:, pl.ds(2 * width, 2 * width)], core_in, p_send, p_recv, core)
    for at, p in ((2, 1), (3, 3), (0, 0)):
        part[:, at * width : (at + 1) * width] = times_transposed(
            mix_ref[...], wo_ref[p * width : (p + 1) * width, :]
        ).astype(low)
    part_copy.start()
    part[:, width : 2 * width] = times_transposed(
        mix_ref[...], wo_ref[2 * width : 3 * width, :]
    ).astype(low)
    part_copy.wait()

    def add_core(r):
        x_out[r, :] = (
            part[r, width : 2 * width].astype(wide) + core_in[r, width : 2 * width].astype(wide)
        ).astype(low)
        h_ref[r, :] = (
            tok_ref[r, :].astype(wide)
            + part[r, 0:width].astype(wide)
            + core_in[r, 0:width].astype(wide)
        )

    tiles(rows, 64, add_core)
    r_copy = remote(x_out, x_in, r_send, r_recv, far)
    r_copy.start()

    def f_arrive(a, j):
        f_copy(a, j).wait_recv()
        for k in others:
            fy_copy(a, j, k).start()

    for j in (1, 2, 3):
        f_arrive(0, j)
    r_copy.wait()

    def add_far(r):
        h_ref[r, :] = h_ref[r, :] + x_in[r, :].astype(wide)

    tiles(rows, 64, add_far)
    for a in (1, 2):
        for j in (1, 2, 3):
            f_arrive(a, j)

    def d_arrive(j):
        douts.arrive(z ^ j)
        dx_copy(j).start()
        dc_copy(j, 0).start()

    def d_settle(j):
        dx_copy(j).wait_recv()
        dc_copy(j, 1).start()

    d_settle(0)
    for s in range(1, 4):
        for j in sorted({s, 5 - s} if s >= 2 else {s}):
            if s < 2:
                d_arrive(j)
            else:

                @pl.when(chunk(s) == j)
                def _():
                    d_arrive(j)

    for j in (1, 2, 3):
        d_settle(j)

    for a in range(3):
        stores[a].wait()
        for j in range(4):
            for k in others:
                fy_copy(a, j, k).wait_send()
                block = weights[a][1].at[slot(z ^ j, y ^ k)]
                remote(
                    block, block, fy_send.at[a, k, j], fy_recv.at[a, k, j], {"row": y ^ k}
                ).wait_recv()
            if j:
                f_copy(a, j).wait_send()
    do_own.wait()
    for j in range(4):
        dx_copy(j).wait_send()
        dc_copy(j, 0).wait()
        dc_copy(j, 1).wait()
    for relay, src in ((attn, aw_ref.at[slot(z, y)]), (outw, wo_ref.at[slot(z, y)]), (douts, cot_ref)):
        relay.own(src, wait=True)
        for j in (1, 2, 3):
            relay.forward(z ^ j, wait=True)
    for o in range(4):
        for k in others:
            row_copy(aw_ref, o, k, ay_send, ay_recv).wait_send()
            row_copy(wo_ref, o, k, oy_send, oy_recv).wait_send()
    for k in others:

        @pl.when((y ^ k) > y)
        def _():
            kv_copy(k, y).wait_send()

    for j, k in pairs:
        g_copy(j, k).wait_send()
    for which in range(3):
        t_copy(which).wait_send()


def attn_fwd_call(tokens, cot, gains, cos, sin, valid, wq, wk, wv, wo, wg, wu, wd):
    rows, width = tokens.shape
    model = 4 * width
    low, wide = jnp.bfloat16, jnp.float32
    row_size = lax.axis_size("row")
    local, q_cols = wq.shape
    k_cols = wk.shape[1]
    hidden = wg.shape[1] // 4
    heads = q_cols // HEAD_SIZE
    vmem = pl.BlockSpec(memory_space=pltpu.VMEM)
    hbm = pl.BlockSpec(memory_space=pl.ANY)
    dma = pltpu.SemaphoreType.DMA
    relay = [dma((2,)), dma((4,)), dma((4,))]
    over_row = [dma((row_size, 4)), dma((row_size, 4))]
    shape = jax.ShapeDtypeStruct
    return pl.pallas_call(
        attn_fwd_kernel,
        out_shape=(
            shape((rows, model), low),
            shape((rows, 128), wide),
            shape((heads, rows, HEAD_SIZE), low),
            shape((row_size, rows, 2 * k_cols), low),
            shape((heads, rows, 128), wide),
            shape((rows, q_cols), low),
            shape((rows, width), wide),
            shape((model, q_cols + 2 * k_cols), low),
            shape((model, q_cols), low),
            shape((8, model), wide),
            shape((model, hidden), low),
            shape((model, hidden), low),
            shape((model, hidden), low),
            shape((4, rows, model), low),
        ),
        in_specs=[vmem] * 6 + [hbm] * 7,
        out_specs=(vmem,) * 10 + (hbm,) * 4,
        scratch_shapes=[
            pltpu.VMEM((rows, model), low),
            pltpu.VMEM((rows, q_cols + 2 * k_cols), wide),
            pltpu.VMEM((4 * row_size, 8, local), wide),
            pltpu.VMEM((3, local, hidden), low),
            pltpu.VMEM((rows, model), low),
            pltpu.VMEM((rows, 2 * width), low),
            pltpu.VMEM((rows, width), low),
            pltpu.VMEM((rows, width), low),
            dma((4,)),
            dma((3,)),
            dma(()),
            dma((4, row_size)),
            dma((4, row_size)),
            dma((1,)),
            dma((1,)),
            dma((3,)),
            dma((3,)),
            *relay,
            *over_row,
            *relay,
            *over_row,
            dma((3, 4)),
            dma((3, 4)),
            dma((3, row_size, 4)),
            dma((3, row_size, 4)),
            *relay,
            dma((4,)),
            dma((4,)),
            dma((2, 4)),
            dma((2, 4)),
            dma((row_size,)),
            dma((row_size,)),
            dma(()),
            dma(()),
            dma(()),
            dma(()),
        ],
        compiler_params=pltpu.CompilerParams(
            collective_id=1, has_side_effects=True, vmem_limit_bytes=60_000_000
        ),
        cost_estimate=pl.CostEstimate(
            flops=10_000_000_000, bytes_accessed=40_000_000, transcendentals=2_000_000
        ),
    )(tokens, cot, gains, cos, sin, valid, wq, wk, wv, wo, wg, wu, wd)


class Reduce:
    def __init__(self, z, mid, block, inbox, send, recv):
        self.z, self.mid, self.block, self.inbox = z, mid, block, inbox
        self.send, self.recv = send, recv

    def copy(self, j):
        owner = self.z ^ j
        above = owner > self.z
        target = jnp.where(above, self.z + 1, self.z - 1)
        slot = jnp.where(target == owner, jnp.where(above, 3, 4), (target ^ owner) - 1)
        return remote(
            self.block(j), self.inbox.at[slot], self.send.at[j], self.recv.at[slot], {"dp": target}
        )

    def arrived(self, slot):
        block = self.inbox.at[slot]
        remote(block, block, self.send.at[0], self.recv.at[slot], {"dp": self.z ^ 1}).wait_recv()

    def first(self, j):
        @pl.when(jnp.logical_not(self.mid))
        def _():
            self.copy(j).start()

    def relay(self, j, add):
        @pl.when(self.mid)
        def _():
            self.arrived(j - 1)
            add(j)
            self.copy(j).start()

    def finish(self, add):
        @pl.when(self.z > 0)
        def _():
            self.arrived(3)
            add(3)

        @pl.when(self.z < 3)
        def _():
            self.arrived(4)
            add(4)

    def drain(self):
        for j in (1, 2, 3):
            self.copy(j).wait_send()


def lane_sums(value):
    total = value[:, 0:128]
    for at in range(128, value.shape[1], 128):
        total = total + value[:, at : at + 128]
    return total


def attn_bwd_kernel(
    dhn_ref,
    factor_two_ref,
    h_ref,
    dout_ref,
    gain_ref,
    tok_ref,
    factor_one_ref,
    cos_ref,
    sin_ref,
    valid_ref,
    q_ref,
    lse_ref,
    mix_ref,
    xn_hbm,
    kv_hbm,
    aw_hbm,
    wo_hbm,
    out_hbm,
    dwg_hbm,
    dwu_hbm,
    dwd_hbm,
    layer_ref,
    dtok_ref,
    gains_ref,
    dattn_ref,
    dwo_ref,
    gg_ref,
    gu_ref,
    gd_ref,
    full,
    xn,
    kv,
    aw,
    wo,
    lanes,
    lanes_in,
    do,
    delta,
    dq,
    dkv,
    dkv_out,
    dkv_in,
    graw,
    dw_attn,
    dw_out,
    own_f,
    row_f,
    row_a,
    row_o,
    z_a,
    z_o,
    in_a,
    in_o,
    out_own,
    core_in,
    x_in,
    z_in,
    pcore_in,
    px_out,
    px_in,
    gvec,
    g_in,
    load_sem,
    l_send,
    l_recv,
    t_send,
    t_recv,
    fy_send,
    fy_recv,
    fz_send,
    fz_recv,
    own_sem,
    oc_send,
    oc_recv,
    oo_sem,
    ox_send,
    ox_recv,
    oz_send,
    oz_recv,
    kv_send,
    kv_recv,
    ay_send,
    ay_recv,
    az_send,
    az_recv,
    wy_send,
    wy_recv,
    wz_send,
    wz_recv,
    p_send,
    p_recv,
    r_send,
    r_recv,
    g_send,
    g_recv,
    gc_send,
    gc_recv,
):
    rows, width = tok_ref.shape
    model = 4 * width
    low, wide = jnp.bfloat16, jnp.float32
    row_size = lax.axis_size("row")
    local = model // (4 * row_size)
    heads = q_ref.shape[0]
    q_cols = heads * HEAD_SIZE
    all_cols = graw.shape[1]
    k_cols = (all_cols - q_cols) // 2
    hidden = own_f.shape[3]
    half = HEAD_SIZE // 2
    score_scale = 1.0 / math.sqrt(HEAD_SIZE)
    z, y, col = (lax.axis_index(name) for name in ("dp", "row", "col"))
    core, far = {"col": col ^ 1}, {"col": col ^ 2}
    others = range(1, row_size)
    mid = jnp.logical_and(z > 0, z < 3)
    third = jnp.where(mid, 2, 3)
    second = jnp.where(mid, 3, 2)
    by_distance = (third, second, 1, 0)
    partials = (dwg_hbm, dwu_hbm, dwd_hbm)
    results = (gg_ref, gu_ref, gd_ref)

    def cols(p):
        return pl.ds(p * width, width)

    greet(
        [{"dp": z ^ j, "row": y ^ k} for j in range(4) for k in range(row_size) if j + k > 0]
        + [{"col": col ^ m} for m in (1, 2, 3)]
    )

    def fy_copy(a, j, k):
        at = z ^ j ^ col
        return remote(
            partials[a].at[at, y ^ k],
            row_f.at[a, k - 1, j],
            fy_send.at[a, k, j],
            fy_recv.at[a, k, j],
            {"row": y ^ k},
        )

    far_first = (3, 2, 1, 0)
    for a in (0, 1):
        for j in far_first:
            for k in others:
                fy_copy(a, j, k).start()

    def own_load(a, j):
        return pltpu.make_async_copy(
            partials[a].at[z ^ j ^ col, y], own_f.at[a, j], own_sem.at[a, j]
        )

    def oc_copy(j, which):
        return remote(
            out_hbm.at[j, :, cols(1 + 2 * which)],
            core_in.at[j, :, cols(which)],
            oc_send.at[which, j],
            oc_recv.at[which, j],
            core,
        )

    def oo_copy(j, which):
        return pltpu.make_async_copy(
            out_hbm.at[j, :, cols(2 * which)], out_own.at[j, :, cols(which)], oo_sem.at[which, j]
        )

    loads = [
        pltpu.make_async_copy(src, dst, load_sem.at[i])
        for i, (src, dst) in enumerate(((wo_hbm, wo), (xn_hbm, xn), (aw_hbm, aw)))
    ]

    gain_two = gain_ref[1:2, 0:width]
    gain_one = gain_ref[0:1, 0:width]

    def residual(r):
        return h_ref[r, :].astype(low).astype(wide)

    def inner_two(r):
        lanes[0, r, :] = lane_sums(gain_two * dhn_ref[r, :] * residual(r)).astype(low)

    tiles(rows, 64, inner_two)
    for j in by_distance:
        for which in (0, 1):
            oc_copy(j, which).start()
            oo_copy(j, which).start()

    def l_copy(n, m):
        return remote(
            lanes.at[n], lanes_in.at[n, m - 1], l_send.at[n, m - 1], l_recv.at[n, m - 1], {"col": col ^ m}
        )

    for m in (2, 3, 1):
        l_copy(0, m).start()
    for load in loads:
        load.start()
    for a in range(3):
        for j in far_first:
            own_load(a, j).start()

    def inner(n, r):
        total = lanes[n, r, :].astype(wide)
        for m in range(3):
            total = total + lanes_in[n, m, r, :].astype(wide)
        return jnp.sum(total, axis=1, keepdims=True) * (1.0 / model)

    def gain_two_sum(i, total):
        r = pl.ds(pl.multiple_of(i * 64, 64), 64)
        return total + jnp.sum(
            dhn_ref[r, :] * residual(r) * factor_two_ref[r, 0:1], axis=0, keepdims=True
        )

    gain_two_grad = lax.fori_loop(0, rows // 64, gain_two_sum, jnp.zeros((1, width), wide))
    for m in (1, 2, 3):
        l_copy(0, m).wait_recv()

    def grad_residual(r):
        factor = factor_two_ref[r, 0:1]
        grad = (
            dout_ref[r, :].astype(wide)
            + factor * gain_two * dhn_ref[r, :]
            - residual(r) * factor * factor * factor * inner(0, r)
        ).astype(low)
        full[r, 0:width] = grad
        dtok_ref[r, :] = grad

    tiles(rows, 64, grad_residual)

    def t_copy(which):
        src = full.at[:, cols(2)] if which == 2 else full.at[:, cols(0)]
        dst = full.at[:, cols((1, 2, 3)[which])]
        return remote(
            src, dst, t_send.at[which], t_recv.at[which], far if which == 1 else core
        )

    def ox_copy(j):
        return remote(out_own.at[j, :, cols(1)], x_in.at[j], ox_send.at[j], ox_recv.at[j], far)

    def out_core(j):
        for which in (0, 1):
            oo_copy(j, which).wait()
            oc_copy(j, which).wait_recv()

        def add(r):
            out_own[j, r, width : 2 * width] = (
                out_own[j, r, width : 2 * width].astype(wide)
                + core_in[j, r, width : 2 * width].astype(wide)
            ).astype(low)
            out_own[j, r, 0:width] = (
                out_own[j, r, 0:width].astype(wide) + core_in[j, r, 0:width].astype(wide)
            ).astype(low)

        tiles(rows, 64, add)

    out_core(third)
    t_copy(1).start()
    t_copy(0).start()
    ox_copy(third).start()

    outs = Reduce(z, mid, lambda j: out_own.at[j, :, cols(0)], z_in, oz_send, oz_recv)

    def out_add(j):
        def add(r):
            out_own[j, r, 0:width] = (
                out_own[j, r, 0:width].astype(wide) + z_in[j - 1, r, :].astype(wide)
            ).astype(low)

        tiles(rows, 64, add)

    def out_far(j):
        ox_copy(j).wait_recv()

        def add(r):
            out_own[j, r, 0:width] = (
                out_own[j, r, 0:width].astype(wide) + x_in[j, r, :].astype(wide)
            ).astype(low)

        tiles(rows, 64, add)

    def fz_copy(a, j):
        at = pl.ds(pl.multiple_of(z * hidden, hidden), hidden)
        return remote(
            own_f.at[a, j], results[a].at[:, at], fz_send.at[a, j], fz_recv.at[a, j], {"dp": z ^ j}
        )

    def f_own(a):
        at = pl.ds(pl.multiple_of(z * hidden, hidden), hidden)
        return pltpu.make_async_copy(own_f.at[a, 0], results[a].at[:, at], own_sem.at[a, 0])

    def f_row(a, j):
        own_load(a, j).wait()
        for k in others:
            fy_copy(a, j, k).wait_recv()
        total = own_f[a, j].astype(wide)
        for k in others:
            total = total + row_f[a, k - 1, j].astype(wide)
        own_f[a, j] = total.astype(low)

    out_core(second)
    f_row(0, 3)
    ox_copy(second).start()
    out_core(1)
    fz_copy(0, 3).start()
    ox_copy(1).start()
    t_copy(1).wait_recv()
    t_copy(2).start()
    out_core(0)
    t_copy(0).wait_recv()
    f_row(0, 2)
    ox_copy(0).start()
    loads[0].wait()
    t_copy(2).wait_recv()

    do[...] = (dot_nn(full[...], wo[...]) * valid_ref[...]).astype(low)
    fz_copy(0, 2).start()
    for p in range(4):
        at = slice(p * width, (p + 1) * width)
        dw_out[at, :] = contract_rows(full[:, at], mix_ref[...]).astype(low)

    def deltas(r):
        for h in range(heads):
            at = slice(h * HEAD_SIZE, (h + 1) * HEAD_SIZE)
            total = jnp.sum(do[r, at].astype(wide) * mix_ref[r, at].astype(wide), axis=1, keepdims=True)
            delta[h, r, :] = jnp.broadcast_to(total, (total.shape[0], 128))

    tiles(rows, 64, deltas)
    dq[...] = jnp.zeros_like(dq)
    q_tile = 256

    def attend_block(b, slot):
        dkv[...] = jnp.zeros_like(dkv)

        def tile(i, unused):
            at = pl.ds(pl.multiple_of(i * q_tile, q_tile), q_tile)
            query_pos = y * rows + i * q_tile + lax.broadcasted_iota(jnp.int32, (q_tile, rows), 0)
            key_pos = b * rows + lax.broadcasted_iota(jnp.int32, (q_tile, rows), 1)
            for h in range(heads):
                head = slice(h * HEAD_SIZE, (h + 1) * HEAD_SIZE)
                query, grad = q_ref[h, at, :], do[at, head]
                keys, values = kv[slot, :, 0:k_cols], kv[slot, :, k_cols : 2 * k_cols]
                scores = times_transposed(query, keys) * score_scale
                probs = jnp.where(
                    key_pos <= query_pos, jnp.exp(scores - lse_ref[h, at, 0:1]), 0.0
                )
                grad_probs = times_transposed(grad, values)
                grad_scores = (probs * (grad_probs - delta[h, at, 0:1]) * score_scale).astype(low)
                dq[at, head] += dot_nn(grad_scores, keys)
                dkv[:, 0:k_cols] += contract_rows(grad_scores, query)
                dkv[:, k_cols : 2 * k_cols] += contract_rows(probs.astype(low), grad)
            return unused

        lax.fori_loop(0, rows // q_tile, tile, 0)

    def kv_copy(k):
        return remote(
            dkv_out, dkv_in.at[k - 1], kv_send.at[k], kv_recv.at[k], {"row": y ^ k}
        )

    blocks = [*others, 0]

    def when_block(k, body):
        if k:
            pl.when((y ^ k) < y)(body)
        else:
            body()

    def kv_load(i):
        return pltpu.make_async_copy(
            kv_hbm.at[y ^ blocks[i]], kv.at[i % 2], load_sem.at[3 + i % 2]
        )

    when_block(blocks[0], lambda: kv_load(0).start())
    for i, k in enumerate(others):
        when_block(k, lambda i=i: kv_load(i).wait())
        when_block(blocks[i + 1], lambda i=i: kv_load(i + 1).start())
        when_block(k, lambda i=i, k=k: attend_block(y ^ k, i % 2))
        if i:
            when_block(k - 1, lambda k=k: kv_copy(k - 1).wait_send())

        def keep(r):
            dkv_out[r, :] = dkv[r, :].astype(low)

        when_block(k, lambda: tiles(rows, 64, keep))
        if i == 0:
            f_row(0, 1)
            f_row(0, 0)
        when_block(k, lambda k=k: kv_copy(k).start())

    fz_copy(0, 1).start()
    f_own(0).start()
    out_far(third)
    f_row(1, 3)
    outs.first(third)
    fz_copy(1, 3).start()

    def wy_copy(j, k):
        at = pl.ds(pl.multiple_of(((z ^ j ^ col) * row_size + (y ^ k)) * local, local), local)
        return remote(
            dw_out.at[at], row_o.at[k - 1, j], wy_send.at[k, j], wy_recv.at[k, j], {"row": y ^ k}
        )

    for j in by_distance:
        for k in others:
            wy_copy(j, k).start()
    for j in far_first:
        for k in others:
            fy_copy(2, j, k).start()
    kv_load(len(others)).wait()
    out_far(second)
    outs.first(second)
    outs.relay(third, out_add)
    attend_block(y, len(others) % 2)

    def back(r, first, second, at):
        c, s = cos_ref[r, :], sin_ref[r, :]
        graw[r, at : at + half] = (first * c + second * s).astype(low)
        graw[r, at + half : at + 2 * half] = (second * c - first * s).astype(low)

    def queries(r):
        for h in range(heads):
            at = h * HEAD_SIZE
            back(r, dq[r, at : at + half], dq[r, at + half : at + 2 * half], at)

    tiles(rows, 64, queries)
    for k in others:

        @pl.when((y ^ k) > y)
        def _():
            kv_copy(k).wait_recv()

            def add(r):
                dkv[r, :] = dkv[r, :] + dkv_in[k - 1, r, :].astype(wide)

            tiles(rows, 64, add)

    def keys_back(r):
        back(r, dkv[r, 0:half], dkv[r, half : 2 * half], q_cols)
        graw[r, q_cols + k_cols : all_cols] = dkv[r, k_cols : 2 * k_cols].astype(low)

    tiles(rows, 64, keys_back)
    loads[1].wait()
    loads[2].wait()
    f_row(1, 2)

    def ay_copy(j, k):
        at = pl.ds(pl.multiple_of(((z ^ j ^ col) * row_size + (y ^ k)) * local, local), local)
        return remote(
            dw_attn.at[at], row_a.at[k - 1, j], ay_send.at[k, j], ay_recv.at[k, j], {"row": y ^ k}
        )

    for p in range(4):
        at = slice(p * width, (p + 1) * width)
        for n in range(0, all_cols, 512):
            dw_attn[at, n : n + 512] = contract_rows(xn[:, at], graw[:, n : n + 512]).astype(low)
    fz_copy(1, 2).start()
    for which in range(3):
        t_copy(which).wait_send()
    part = full
    part_copy = remote(part.at[:, pl.ds(2 * width, 2 * width)], pcore_in, p_send, p_recv, core)
    for q, p in ((2, 1), (3, 3)):
        part[:, q * width : (q + 1) * width] = times_transposed(
            graw[...], aw[p * width : (p + 1) * width, :]
        ).astype(low)
    for j in by_distance:
        for k in others:
            ay_copy(j, k).start()
    for q, p in ((0, 0), (1, 2)):
        part[:, q * width : (q + 1) * width] = times_transposed(
            graw[...], aw[p * width : (p + 1) * width, :]
        ).astype(low)
    part_copy.start()
    f_row(1, 1)
    f_row(1, 0)
    part_copy.wait()
    fz_copy(1, 1).start()
    f_own(1).start()

    def add_core(r):
        px_out[r, :] = (
            part[r, width : 2 * width].astype(wide) + pcore_in[r, width : 2 * width].astype(wide)
        ).astype(low)

    tiles(rows, 64, add_core)
    out_far(1)
    r_copy = remote(px_out, px_in, r_send, r_recv, far)
    r_copy.start()
    outs.first(1)
    outs.relay(second, out_add)

    outw = Reduce(z, mid, lambda j: z_o.at[j - 1], in_o, wz_send, wz_recv)

    def o_add(j):
        def add(r):
            z_o[j - 1, r, :] = (
                z_o[j - 1, r, :].astype(wide) + in_o[j - 1, r, :].astype(wide)
            ).astype(low)

        tiles(local, 32, add)

    def o_row(j):
        for k in others:
            wy_copy(j, k).wait_recv()
        at = pl.ds(pl.multiple_of(((z ^ j ^ col) * row_size + y) * local, local), local)
        total = dw_out[at, :].astype(wide)
        for k in others:
            total = total + row_o[k - 1, j].astype(wide)
        if isinstance(j, int) and j == 0:
            dwo_ref[...] = total
        else:
            z_o[j - 1] = total.astype(low)

    o_row(third)
    out_far(0)
    outw.first(third)
    outs.relay(1, out_add)
    o_row(second)
    o_row(1)
    outw.first(second)
    o_row(0)
    outw.first(1)
    r_copy.wait()

    def dxn(r):
        return (
            part[r, 0:width].astype(wide) + pcore_in[r, 0:width].astype(wide) + px_in[r, :].astype(wide)
        )

    def inner_one(i, total):
        r = pl.ds(pl.multiple_of(i * 64, 64), 64)
        grad, tokens = dxn(r), tok_ref[r, :].astype(wide)
        lanes[1, r, :] = lane_sums(gain_one * grad * tokens).astype(low)
        return total + jnp.sum(grad * tokens * factor_one_ref[r, 0:1], axis=0, keepdims=True)

    gain_one_grad = lax.fori_loop(0, rows // 64, inner_one, jnp.zeros((1, width), wide))
    for i in range(row_size):
        at = slice(i * local, (i + 1) * local)
        gvec[i, 0:1, :] = gain_one_grad[:, at]
        gvec[i, 1:2, :] = gain_two_grad[:, at]
        gvec[i, 2:8, :] = jnp.zeros((6, local), wide)
    f_row(2, 3)
    for m in (2, 3, 1):
        l_copy(1, m).start()
    mine = z == col

    def g_copy(k):
        return remote(
            gvec.at[y ^ k],
            g_in.at[z * row_size + y],
            g_send.at[k],
            g_recv.at[z, k],
            {"dp": col, "row": y ^ k},
        )

    for k in range(row_size):
        if k:
            g_copy(k).start()
        else:

            @pl.when(jnp.logical_not(mine))
            def _():
                g_copy(0).start()

            @pl.when(mine)
            def _():
                g_in[z * row_size + y] = gvec[y]

    fz_copy(2, 3).start()
    outw.relay(third, o_add)
    f_row(2, 2)
    f_row(2, 1)
    fz_copy(2, 2).start()
    outw.relay(second, o_add)
    f_row(2, 0)
    fz_copy(2, 1).start()
    f_own(2).start()
    outw.relay(1, o_add)
    for m in (1, 2, 3):
        l_copy(1, m).wait_recv()

    def grad_tokens(r):
        factor = factor_one_ref[r, 0:1]
        dtok_ref[r, :] = (
            dtok_ref[r, :].astype(wide)
            + factor * gain_one * dxn(r)
            - tok_ref[r, :].astype(wide) * factor * factor * factor * inner(1, r)
        ).astype(low)

    tiles(rows, 64, grad_tokens)

    attn = Reduce(z, mid, lambda j: z_a.at[j - 1], in_a, az_send, az_recv)

    def a_add(j):
        def add(r):
            z_a[j - 1, r, :] = (
                z_a[j - 1, r, :].astype(wide) + in_a[j - 1, r, :].astype(wide)
            ).astype(low)

        tiles(local, 32, add)

    def a_row(j):
        for k in others:
            ay_copy(j, k).wait_recv()
        at = pl.ds(pl.multiple_of(((z ^ j ^ col) * row_size + y) * local, local), local)
        total = dw_attn[at, :].astype(wide)
        for k in others:
            total = total + row_a[k - 1, j].astype(wide)
        if isinstance(j, int) and j == 0:
            dattn_ref[...] = total
        else:
            z_a[j - 1] = total.astype(low)

    a_row(third)
    a_row(second)
    attn.first(third)
    a_row(1)
    attn.first(second)
    a_row(0)
    attn.first(1)
    attn.relay(third, a_add)
    attn.relay(second, a_add)
    attn.relay(1, a_add)

    def gc_copy(m):
        return remote(
            gains_ref, gains_ref, gc_send.at[m - 1], gc_recv, {"col": col ^ m}
        )

    @pl.when(mine)
    def _():
        for j in range(4):
            for k in range(row_size):
                if j + k:
                    block = g_in.at[(z ^ j) * row_size + (y ^ k)]
                    remote(
                        block, block, g_send.at[k], g_recv.at[z ^ j, k], {"dp": z ^ j, "row": y ^ k}
                    ).wait_recv()
        total = g_in[0]
        for i in range(1, 4 * row_size):
            total = total + g_in[i]
        gains_ref[...] = total

    @pl.when(mine)
    def _():
        for m in (1, 2, 3):
            gc_copy(m).start()

    for slot in (3, 4):

        @pl.when((z > 0) if slot == 3 else (z < 3))
        def _():
            outs.arrived(slot)

        @pl.when((z == 0) if slot == 3 else (z == 3))
        def _():
            z_in[slot] = jnp.zeros((rows, width), low)

    def layer_out(r):
        total = h_ref[r, :] + out_own[0, r, 0:width].astype(wide)
        for slot in (3, 4):
            total = total + z_in[slot, r, :].astype(wide)
        layer_ref[r, :] = total.astype(low)

    tiles(rows, 64, layer_out)

    def o_last(slot):
        dwo_ref[...] = dwo_ref[...] + in_o[slot].astype(wide)

    outw.finish(o_last)
    for a in range(3):
        f_own(a).wait()
        for j in (1, 2, 3):
            at = pl.ds(pl.multiple_of((z ^ j) * hidden, hidden), hidden)
            block = results[a].at[:, at]
            remote(block, block, fz_send.at[a, j], fz_recv.at[a, j], {"dp": z ^ j}).wait_recv()

    def a_last(slot):
        dattn_ref[...] = dattn_ref[...] + in_a[slot].astype(wide)

    attn.finish(a_last)

    @pl.when(jnp.logical_not(mine))
    def _():
        gc_copy(1).wait_recv()

    @pl.when(mine)
    def _():
        for m in (1, 2, 3):
            gc_copy(m).wait_send()

    for k in range(row_size):
        if k:
            g_copy(k).wait_send()
        else:

            @pl.when(jnp.logical_not(mine))
            def _():
                g_copy(0).wait_send()

    for n in (0, 1):
        for m in (1, 2, 3):
            l_copy(n, m).wait_send()
    for summed in (outs, outw, attn):
        summed.drain()
    for j in range(4):
        ox_copy(j).wait_send()
        for which in (0, 1):
            oc_copy(j, which).wait_send()
        if j:
            for a in range(3):
                fz_copy(a, j).wait_send()
        for k in others:
            wy_copy(j, k).wait_send()
            ay_copy(j, k).wait_send()
            for a in range(3):
                fy_copy(a, j, k).wait_send()
    when_block(row_size - 1, lambda: kv_copy(row_size - 1).wait_send())


def attn_bwd_call(
    dhn,
    factor_two,
    h,
    dout,
    gains,
    tokens,
    factor_one,
    cos,
    sin,
    valid,
    q,
    lse,
    mix,
    xn,
    kv,
    aw,
    wo,
    out_part,
    dwg,
    dwu,
    dwd,
):
    rows, width = tokens.shape
    model, hidden = dwg.shape
    low, wide = jnp.bfloat16, jnp.float32
    row_size = lax.axis_size("row")
    local = model // (4 * row_size)
    all_cols, q_cols = aw.shape[1], wo.shape[1]
    heads = q_cols // HEAD_SIZE
    kv_cols = kv.shape[2]
    vmem = pl.BlockSpec(memory_space=pltpu.VMEM)
    hbm = pl.BlockSpec(memory_space=pl.ANY)
    dma = pltpu.SemaphoreType.DMA
    shape = jax.ShapeDtypeStruct
    blocks = [part.reshape(4, row_size, local, hidden) for part in (dwg, dwu, dwd)]
    return pl.pallas_call(
        attn_bwd_kernel,
        out_shape=(
            shape((rows, width), low),
            shape((rows, width), low),
            shape((8, local), wide),
            shape((local, all_cols), wide),
            shape((local, q_cols), wide),
            shape((local, 4 * hidden), low),
            shape((local, 4 * hidden), low),
            shape((local, 4 * hidden), low),
        ),
        in_specs=[vmem] * 13 + [hbm] * 8,
        out_specs=(vmem,) * 5 + (hbm,) * 3,
        scratch_shapes=[
            pltpu.VMEM((rows, model), low),
            pltpu.VMEM((rows, model), low),
            pltpu.VMEM((2, rows, kv_cols), low),
            pltpu.VMEM((model, all_cols), low),
            pltpu.VMEM((model, q_cols), low),
            pltpu.VMEM((2, rows, 128), low),
            pltpu.VMEM((2, 3, rows, 128), low),
            pltpu.VMEM((rows, q_cols), low),
            pltpu.VMEM((heads, rows, 128), wide),
            pltpu.VMEM((rows, q_cols), wide),
            pltpu.VMEM((rows, kv_cols), wide),
            pltpu.VMEM((rows, kv_cols), low),
            pltpu.VMEM((row_size - 1, rows, kv_cols), low),
            pltpu.VMEM((rows, all_cols), low),
            pltpu.VMEM((model, all_cols), low),
            pltpu.VMEM((model, q_cols), low),
            pltpu.VMEM((3, 4, local, hidden), low),
            pltpu.VMEM((3, row_size - 1, 4, local, hidden), low),
            pltpu.VMEM((row_size - 1, 4, local, all_cols), low),
            pltpu.VMEM((row_size - 1, 4, local, q_cols), low),
            pltpu.VMEM((3, local, all_cols), low),
            pltpu.VMEM((3, local, q_cols), low),
            pltpu.VMEM((5, local, all_cols), low),
            pltpu.VMEM((5, local, q_cols), low),
            pltpu.VMEM((4, rows, 2 * width), low),
            pltpu.VMEM((4, rows, 2 * width), low),
            pltpu.VMEM((4, rows, width), low),
            pltpu.VMEM((5, rows, width), low),
            pltpu.VMEM((rows, 2 * width), low),
            pltpu.VMEM((rows, width), low),
            pltpu.VMEM((rows, width), low),
            pltpu.VMEM((row_size, 8, local), wide),
            pltpu.VMEM((4 * row_size, 8, local), wide),
            dma((5,)),
            dma((2, 3)),
            dma((2, 3)),
            dma((3,)),
            dma((3,)),
            dma((3, row_size, 4)),
            dma((3, row_size, 4)),
            dma((3, 4)),
            dma((3, 4)),
            dma((3, 4)),
            dma((2, 4)),
            dma((2, 4)),
            dma((2, 4)),
            dma((4,)),
            dma((4,)),
            dma((4,)),
            dma((5,)),
            dma((row_size,)),
            dma((row_size,)),
            dma((row_size, 4)),
            dma((row_size, 4)),
            dma((4,)),
            dma((5,)),
            dma((row_size, 4)),
            dma((row_size, 4)),
            dma((4,)),
            dma((5,)),
            dma(()),
            dma(()),
            dma(()),
            dma(()),
            dma((row_size,)),
            dma((4, row_size)),
            dma((3,)),
            dma(()),
        ],
        compiler_params=pltpu.CompilerParams(
            collective_id=3, has_side_effects=True, vmem_limit_bytes=66_000_000
        ),
        cost_estimate=pl.CostEstimate(
            flops=14_000_000_000, bytes_accessed=40_000_000, transcendentals=2_000_000
        ),
    )(
        dhn,
        factor_two,
        h,
        dout,
        gains,
        tokens,
        factor_one,
        cos,
        sin,
        valid,
        q,
        lse,
        mix,
        xn,
        kv,
        aw,
        wo,
        out_part,
        *blocks,
    )


def per_device(
    tokens,
    w_query,
    key_matrix,
    value_matrix,
    w_output,
    w_gate,
    w_up,
    w_down,
    gain_attn,
    gain_ffn,
    lengths,
    cotangent,
):
    low = jnp.bfloat16
    wide = jnp.float32
    row_count = tokens.shape[0]
    me_row = lax.axis_index("row")
    query_pos = me_row * row_count + jnp.arange(row_count, dtype=jnp.int32)
    valid = (query_pos < lengths[0]).astype(wide)[:, None]
    cosine_table, sine_table = rope_tables(query_pos.astype(wide))

    gains = jnp.zeros((8, gain_attn.shape[0]), wide)
    gains = gains.at[0].set(gain_attn.astype(wide)).at[1].set(gain_ffn.astype(wide))
    q_cols, k_cols = w_query.shape[1], key_matrix.shape[1]
    grad_out = (cotangent.astype(wide) * valid).astype(low)
    (
        normed,
        factor_one,
        query_rows,
        kv_all,
        log_total,
        mixed_heads,
        residual,
        attn_weight,
        out_weight,
        gains,
        gate_weight,
        up_weight,
        down_weight,
        grad_out_full,
    ) = attn_fwd_call(
        tokens,
        grad_out,
        gains,
        cosine_table,
        sine_table,
        valid,
        w_query,
        key_matrix,
        value_matrix,
        w_output.T,
        w_gate,
        w_up,
        w_down.T,
    )
    residual_low = residual.astype(low)
    grad_normed_two, factor_two, out_part, grad_gate_part, grad_up_part, grad_down_part = ffn_call(
        residual_low, gains[1:2], grad_out_full, gate_weight, up_weight, down_weight
    )
    (
        layer_out,
        grad_tokens,
        gain_grads,
        grad_attn,
        grad_output,
        grad_gate,
        grad_up,
        grad_down,
    ) = attn_bwd_call(
        grad_normed_two,
        factor_two,
        residual,
        grad_out,
        gains,
        tokens,
        factor_one,
        cosine_table,
        sine_table,
        valid,
        query_rows,
        log_total,
        mixed_heads,
        normed,
        kv_all,
        attn_weight,
        out_weight,
        out_part,
        grad_gate_part,
        grad_up_part,
        grad_down_part,
    )
    return (
        layer_out,
        grad_tokens,
        gain_grads[0],
        gain_grads[1],
        grad_attn[:, :q_cols],
        grad_attn[:, q_cols : q_cols + k_cols],
        grad_attn[:, q_cols + k_cols :],
        grad_output.T,
        grad_gate.astype(wide),
        grad_up.astype(wide),
        grad_down.T.astype(wide),
    )


def solution(mesh):
    in_specs = (
        P(("dp", "row"), "col"),
        P(("dp", "row"), "col"),
        P(("dp", "row"), "col"),
        P(("dp", "row"), "col"),
        P("col", ("dp", "row")),
        P(("dp", "row"), "col"),
        P(("dp", "row"), "col"),
        P("col", ("dp", "row")),
        P(("dp", "row")),
        P(("dp", "row")),
        P("dp"),
        P(("dp", "row"), "col"),
    )
    out_specs = (
        P(("dp", "row"), "col"),
        P(("dp", "row"), "col"),
        P(("dp", "row")),
        P(("dp", "row")),
        P(("dp", "row"), "col"),
        P(("dp", "row"), "col"),
        P(("dp", "row"), "col"),
        P("col", ("dp", "row")),
        P(("dp", "row"), "col"),
        P(("dp", "row"), "col"),
        P("col", ("dp", "row")),
    )
    return jax.shard_map(
        per_device, mesh=mesh, in_specs=in_specs, out_specs=out_specs, check_vma=False
    )
```

```python
import math

import jax
import jax.numpy as jnp
from jax import lax
from jax.experimental import pallas as pl
from jax.experimental.pallas import tpu as pltpu
from jax.sharding import PartitionSpec as P

HEAD_SIZE = 256
EPSILON = 1e-06
ROPE_BASE = 1000042.0


def rope_tables(positions):
    half = HEAD_SIZE // 2
    freq = ROPE_BASE ** (-jnp.arange(half, dtype=jnp.float32) * 2.0 / HEAD_SIZE)
    angle = positions[:, None] * freq[None, :]
    return (jnp.cos(angle), jnp.sin(angle))


def contract_rows(left, right):
    return lax.dot_general(
        left, right, (((0,), (0,)), ((), ())), preferred_element_type=jnp.float32
    )


def times_transposed(left, right):
    return lax.dot_general(
        left, right, (((1,), (1,)), ((), ())), preferred_element_type=jnp.float32
    )


def dot_nn(left, right):
    return lax.dot_general(left, right, (((1,), (0,)), ((), ())), preferred_element_type=jnp.float32)


def tiles(count, size, body):
    def step(i, unused):
        body(pl.ds(pl.multiple_of(i * size, size), size))
        return unused

    lax.fori_loop(0, count // size, step, 0)


def remote(src, dst, send_sem, recv_sem, target):
    return pltpu.make_async_remote_copy(
        src_ref=src,
        dst_ref=dst,
        send_sem=send_sem,
        recv_sem=recv_sem,
        device_id=target,
        device_id_type=pl.DeviceIdType.MESH,
    )


def greet(targets):
    barrier = pltpu.get_barrier_semaphore()
    for target in targets:
        pl.semaphore_signal(
            barrier, inc=1, device_id=target, device_id_type=pl.DeviceIdType.MESH
        )
    pl.semaphore_wait(barrier, len(targets))


def ffn_kernel(
    h_ref,
    gain_ref,
    do_hbm,
    wg_hbm,
    wu_hbm,
    wd_hbm,
    dhn_ref,
    factor_ref,
    out_hbm,
    dwg_hbm,
    dwu_hbm,
    dwd_hbm,
    full,
    do,
    wg,
    wu,
    wd,
    hid,
    dg,
    du,
    gate,
    up,
    dhid,
    part,
    outp,
    core_in,
    x_out,
    x_in,
    z_out,
    z_in,
    stage,
    load_sem,
    z_send,
    f_send,
    z_recv,
    x_send,
    x_recv,
    c_send,
    c_recv,
    p_send,
    p_recv,
    rx_send,
    rx_recv,
    rz_send,
    rz_recv,
    o_sem,
    s_sem,
):
    rows, width = h_ref.shape
    model = width * 4
    hidden = wg.shape[1]
    low, wide = jnp.bfloat16, jnp.float32
    z, col = lax.axis_index("dp"), lax.axis_index("col")
    core, far = {"col": col ^ 1}, {"col": col ^ 2}
    mid = jnp.logical_and(z > 0, z < 3)

    def chunk(s):
        return jnp.where(jnp.logical_and(mid, s >= 2), 5 - s, s)

    def cols(p):
        return pl.ds(p * width, width)

    greet([{"dp": z ^ 1}, {"dp": z ^ 2}, {"dp": z ^ 3}, core, far])

    def z_own(target, index):
        slot = z ^ target
        return remote(
            h_ref, full.at[slot, :, cols(0)], z_send.at[index], z_recv.at[slot], {"dp": target}
        )

    @pl.when(z < 3)
    def _():
        z_own(z + 1, 0).start()

    @pl.when(z > 0)
    def _():
        z_own(z - 1, 1).start()

    def x_copy(j, src):
        return remote(src, full.at[j, :, cols(2)], x_send.at[j], x_recv.at[j], far)

    def c_copy(j, src, which):
        return remote(
            src, full.at[j, :, cols(1 + 2 * which)], c_send.at[which, j], c_recv.at[which, j], core
        )

    x_copy(0, h_ref).start()
    c_copy(0, h_ref, 0).start()
    loads = [
        pltpu.make_async_copy(wg_hbm, wg, load_sem.at[0]),
        pltpu.make_async_copy(wu_hbm, wu, load_sem.at[1]),
        pltpu.make_async_copy(wd_hbm, wd, load_sem.at[2]),
    ]
    for load in loads:
        load.start()

    def do_load(j):
        return pltpu.make_async_copy(do_hbm.at[j], do.at[j], load_sem.at[3 + j])

    for j in range(4):
        do_load(j).start()

    def copy_own(r):
        full[0, r, 0:width] = h_ref[r, :]

    tiles(rows, 64, copy_own)

    def forward(j, target):
        return remote(
            full.at[j, :, cols(0)],
            full.at[(z ^ j) ^ target, :, cols(0)],
            f_send.at[j],
            z_recv.at[(z ^ j) ^ target],
            {"dp": target},
        )

    def goes_up(j):
        return jnp.logical_and((z ^ j) < z, z < 3)

    def goes_down(j):
        return jnp.logical_and((z ^ j) > z, z > 0)

    def arrive(j):
        block = full.at[j, :, cols(0)]
        remote(block, block, f_send.at[j], z_recv.at[j], core).wait_recv()

        @pl.when(goes_up(j))
        def _():
            forward(j, z + 1).start()

        @pl.when(goes_down(j))
        def _():
            forward(j, z - 1).start()

        x_copy(j, block).start()
        c_copy(j, block, 0).start()

    def settle(j):
        block = full.at[j, :, cols(0)]
        x_copy(j, block).wait_recv()
        c_copy(j, full.at[j, :, cols(2)], 1).start()
        x_copy(j, block).wait_send()
        c_copy(j, block, 0).wait_send()

        @pl.when(jnp.logical_and(j > 0, jnp.logical_or(goes_up(j), goes_down(j))))
        def _():
            forward(j, z ^ j).wait_send()

        c_copy(j, block, 0).wait_recv()
        c_copy(j, block, 1).wait()

    def part_copy(s, slot):
        return remote(
            part.at[slot, :, pl.ds(2 * width, 2 * width)],
            core_in.at[s],
            p_send.at[s],
            p_recv.at[s],
            core,
        )

    def rx_copy(s):
        return remote(x_out.at[s], x_in.at[s], rx_send.at[s], rx_recv.at[s], far)

    def rz_copy(s, j):
        return remote(z_out.at[s], z_in.at[j], rz_send.at[s], rz_recv.at[j], {"dp": z ^ j})

    def reduce_core(s):
        slot = lax.rem(s, 2)
        part_copy(s, slot).wait()

        def add(r):
            x_out[s, r, :] = (
                part[slot, r, width : 2 * width].astype(wide)
                + core_in[s, r, width : 2 * width].astype(wide)
            ).astype(low)
            z_out[s, r, :] = (
                part[slot, r, 0:width].astype(wide) + core_in[s, r, 0:width].astype(wide)
            ).astype(low)

        tiles(rows, 64, add)
        rx_copy(s).start()

    def reduce_far(s):
        rx_copy(s).wait()

        def add(r):
            z_out[s, r, :] = (z_out[s, r, :].astype(wide) + x_in[s, r, :].astype(wide)).astype(low)

        tiles(rows, 64, add)

        @pl.when(s > 0)
        def _():
            rz_copy(s, chunk(s)).start()

    def out_copy(s):
        return pltpu.make_async_copy(
            outp.at[lax.rem(s, 2)], out_hbm.at[chunk(s)], o_sem.at[lax.rem(s, 2)]
        )

    def step(s, unused):
        j = chunk(s)
        base = s * rows

        @pl.when(jnp.logical_and(s < 3, jnp.logical_not(jnp.logical_and(s == 1, mid))))
        def _():
            arrive(chunk(s + 1))

        @pl.when(jnp.logical_and(s == 0, mid))
        def _():
            arrive(chunk(2))

        settle(j)

        def norm(r):
            x = full[j, r, :].astype(wide)
            factor = lax.rsqrt(jnp.sum(x * x, axis=1, keepdims=True) * (1.0 / model) + EPSILON)
            full[j, r, :] = (x * factor * gain_ref[1:2, :]).astype(low)

            @pl.when(s == 0)
            def _():
                factor_ref[r, :] = jnp.broadcast_to(factor, (factor.shape[0], 128))

        tiles(rows, 32, norm)

        @pl.when(s == 0)
        def _():
            for load in loads:
                load.wait()

        gate[...] = dot_nn(full[j], wg[...])
        up[...] = dot_nn(full[j], wu[...])

        @pl.when(s > 0)
        def _():
            reduce_core(s - 1)

        do_load(j).wait()
        dhid[...] = dot_nn(do[j], wd[...])

        def act(r):
            g = gate[r, :]
            u = up[r, :]
            d = dhid[r, :]
            sig = jax.nn.sigmoid(g)
            silu = g * sig
            at = pl.ds(pl.multiple_of(base + r.start, 64), 64)
            hid[at, :] = (silu * u).astype(low)
            dg[at, :] = (d * u * sig * (1.0 + g * (1.0 - sig))).astype(low)
            du[at, :] = (d * silu).astype(low)

        tiles(rows, 64, act)
        slot = lax.rem(s, 2)
        mine = pl.ds(pl.multiple_of(base, rows), rows)

        def dhn(q, p):
            w_rows = slice(p * width, (p + 1) * width)
            part[slot, :, q * width : (q + 1) * width] = (
                times_transposed(dg[mine, :], wg[w_rows, :])
                + times_transposed(du[mine, :], wu[w_rows, :])
            ).astype(low)

        dhn(2, 1)
        dhn(3, 3)
        dhn(0, 0)
        part_copy(s, slot).start()
        dhn(1, 2)

        @pl.when(s > 0)
        def _():
            reduce_far(s - 1)

        @pl.when(s >= 2)
        def _():
            out_copy(s - 2).wait()

        for p in range(4):
            outp[slot, :, p * width : (p + 1) * width] = times_transposed(
                hid[mine, :], wd[p * width : (p + 1) * width, :]
            ).astype(low)
        out_copy(s).start()
        return unused

    lax.fori_loop(0, 4, step, 0)

    reduce_core(3)
    count = model // width

    def stage_copy(target, i, slot):
        at = pl.ds(pl.multiple_of(i * width, width), width)
        return pltpu.make_async_copy(stage.at[slot], target.at[at, :], s_sem.at[slot])

    def weight_grad(target, right, left_of, first):
        def tile(i, unused):
            slot = lax.rem(i, 2)

            @pl.when(jnp.logical_or(i >= 2, not first))
            def _():
                stage_copy(target, 0, slot).wait()

            total = left_of(0, i, right)
            for s in range(1, 4):
                total = total + left_of(s, i, right)
            stage[slot] = total.astype(low)
            stage_copy(target, i, slot).start()
            return unused

        lax.fori_loop(0, count, tile, 0)

    def from_full(s, i, right):
        at = pl.ds(pl.multiple_of(i * width, width), width)
        return contract_rows(full[chunk(s), :, at], right[s * rows : (s + 1) * rows, :])

    def from_do(s, i, right):
        at = pl.ds(pl.multiple_of(i * width, width), width)
        return contract_rows(do[chunk(s), :, at], right[s * rows : (s + 1) * rows, :])

    weight_grad(dwg_hbm, dg, from_full, True)
    reduce_far(3)
    weight_grad(dwu_hbm, du, from_full, False)
    weight_grad(dwd_hbm, hid, from_do, False)
    stage_copy(dwd_hbm, 0, 0).wait()
    stage_copy(dwd_hbm, 0, 1).wait()
    out_copy(2).wait()
    out_copy(3).wait()
    for s in range(1, 4):
        rz_copy(s, chunk(s)).wait()

    def final(r):
        total = z_out[0, r, :].astype(wide)
        for j in range(1, 4):
            total = total + z_in[j, r, :].astype(wide)
        dhn_ref[r, :] = total

    tiles(rows, 64, final)

    @pl.when(z < 3)
    def _():
        z_own(z + 1, 0).wait_send()

    @pl.when(z > 0)
    def _():
        z_own(z - 1, 1).wait_send()


def ffn_call(h_low, gain, grad_full, wg, wu, wd):
    rows, width = h_low.shape
    model, hidden = wg.shape
    low, wide = jnp.bfloat16, jnp.float32
    vmem = pl.BlockSpec(memory_space=pltpu.VMEM)
    hbm = pl.BlockSpec(memory_space=pl.ANY)
    dma = pltpu.SemaphoreType.DMA
    tokens = 4 * rows
    return pl.pallas_call(
        ffn_kernel,
        out_shape=(
            jax.ShapeDtypeStruct((rows, width), wide),
            jax.ShapeDtypeStruct((rows, 128), wide),
            jax.ShapeDtypeStruct((4, rows, model), low),
            jax.ShapeDtypeStruct((model, hidden), low),
            jax.ShapeDtypeStruct((model, hidden), low),
            jax.ShapeDtypeStruct((model, hidden), low),
        ),
        in_specs=[vmem, vmem, hbm, hbm, hbm, hbm],
        out_specs=(vmem, vmem, hbm, hbm, hbm, hbm),
        scratch_shapes=[
            pltpu.VMEM((4, rows, model), low),
            pltpu.VMEM((4, rows, model), low),
            pltpu.VMEM((model, hidden), low),
            pltpu.VMEM((model, hidden), low),
            pltpu.VMEM((model, hidden), low),
            pltpu.VMEM((tokens, hidden), low),
            pltpu.VMEM((tokens, hidden), low),
            pltpu.VMEM((tokens, hidden), low),
            pltpu.VMEM((rows, hidden), wide),
            pltpu.VMEM((rows, hidden), wide),
            pltpu.VMEM((rows, hidden), wide),
            pltpu.VMEM((2, rows, model), low),
            pltpu.VMEM((2, rows, model), low),
            pltpu.VMEM((4, rows, 2 * width), low),
            pltpu.VMEM((4, rows, width), low),
            pltpu.VMEM((4, rows, width), low),
            pltpu.VMEM((4, rows, width), low),
            pltpu.VMEM((4, rows, width), low),
            pltpu.VMEM((2, width, hidden), low),
            dma((7,)),
            dma((2,)),
            dma((4,)),
            dma((4,)),
            dma((4,)),
            dma((4,)),
            dma((2, 4)),
            dma((2, 4)),
            dma((4,)),
            dma((4,)),
            dma((4,)),
            dma((4,)),
            dma((4,)),
            dma((4,)),
            dma((2,)),
            dma((2,)),
        ],
        compiler_params=pltpu.CompilerParams(
            collective_id=2, has_side_effects=True, vmem_limit_bytes=66_000_000
        ),
        cost_estimate=pl.CostEstimate(
            flops=18 * tokens * model * hidden,
            bytes_accessed=40_000_000,
            transcendentals=tokens * hidden,
        ),
    )(h_low, gain, grad_full, wg, wu, wd)


class Relay:
    def __init__(self, z, place, own_send, forward_send, recv):
        self.z, self.place = z, place
        self.own_send, self.forward_send, self.recv = own_send, forward_send, recv

    def own_copy(self, src, target, index):
        return remote(
            src,
            self.place(self.z, target),
            self.own_send.at[index],
            self.recv.at[self.z],
            {"dp": target},
        )

    def own(self, src, wait=False):
        @pl.when(self.z < 3)
        def _():
            copy = self.own_copy(src, self.z + 1, 0)
            copy.wait_send() if wait else copy.start()

        @pl.when(self.z > 0)
        def _():
            copy = self.own_copy(src, self.z - 1, 1)
            copy.wait_send() if wait else copy.start()

    def forward_copy(self, o, target):
        return remote(
            self.place(o, self.z),
            self.place(o, target),
            self.forward_send.at[o],
            self.recv.at[o],
            {"dp": target},
        )

    def forward(self, o, wait=False):
        @pl.when(jnp.logical_and(o < self.z, self.z < 3))
        def _():
            copy = self.forward_copy(o, self.z + 1)
            copy.wait_send() if wait else copy.start()

        @pl.when(jnp.logical_and(o > self.z, self.z > 0))
        def _():
            copy = self.forward_copy(o, self.z - 1)
            copy.wait_send() if wait else copy.start()

    def arrive(self, o):
        self.forward_copy(o, self.z ^ 1).wait_recv()
        self.forward(o)


def attn_fwd_kernel(
    tok_ref,
    cot_in_ref,
    gains_ref,
    cos_ref,
    sin_ref,
    valid_ref,
    wq_hbm,
    wk_hbm,
    wv_hbm,
    wo_hbm,
    wg_hbm,
    wu_hbm,
    wd_hbm,
    factor_ref,
    q_ref,
    kv_ref,
    lse_ref,
    mix_ref,
    h_ref,
    hlow_ref,
    gain_ref,
    xn_hbm,
    aw_hbm,
    woo_hbm,
    fg_hbm,
    fu_hbm,
    fd_hbm,
    do_hbm,
    xn_ref,
    aw_ref,
    wo_ref,
    cot_ref,
    out_sem,
    full,
    qkv,
    gain_in,
    own_piece,
    part,
    core_in,
    x_out,
    x_in,
    load_sem,
    piece_sem,
    do_sem,
    g_send,
    g_recv,
    x_send,
    x_recv,
    t_send,
    t_recv,
    a_own,
    a_fwd,
    a_recv,
    ay_send,
    ay_recv,
    o_own,
    o_fwd,
    o_recv,
    oy_send,
    oy_recv,
    f_send,
    f_recv,
    fy_send,
    fy_recv,
    d_own,
    d_fwd,
    d_recv,
    dx_send,
    dx_recv,
    dc_send,
    dc_recv,
    kv_send,
    kv_recv,
    p_send,
    p_recv,
    r_send,
    r_recv,
):
    rows, width = tok_ref.shape
    model = 4 * width
    low, wide = jnp.bfloat16, jnp.float32
    row_size = lax.axis_size("row")
    local = wq_hbm.shape[0]
    q_cols, k_cols = wq_hbm.shape[1], wk_hbm.shape[1]
    hidden = fg_hbm.shape[1]
    half = HEAD_SIZE // 2
    z, y, col = (lax.axis_index(name) for name in ("dp", "row", "col"))
    core, far = {"col": col ^ 1}, {"col": col ^ 2}
    mid = jnp.logical_and(z > 0, z < 3)
    others = range(1, row_size)

    def chunk(s):
        return jnp.where(mid, 5 - s, s) if s >= 2 else s

    def cols(p):
        return pl.ds(p * width, width)

    def slot(o, r):
        return pl.ds(pl.multiple_of(((o ^ col) * row_size + r) * local, local), local)

    greet(
        [{"dp": z ^ j, "row": y ^ k} for j in range(4) for k in range(row_size) if j + k > 0]
        + [core, far]
    )

    loads = [
        pltpu.make_async_copy(src, aw_ref.at[slot(z, y), pl.ds(at, src.shape[1])], load_sem.at[i])
        for i, (src, at) in enumerate(
            ((wq_hbm, 0), (wk_hbm, q_cols), (wv_hbm, q_cols + k_cols))
        )
    ]
    load_out = pltpu.make_async_copy(wo_hbm, wo_ref.at[slot(z, y)], load_sem.at[3])
    for load in loads:
        load.start()
    load_out.start()

    def t_copy(which):
        src = full.at[:, cols(2)] if which == 2 else tok_ref
        target = far if which == 1 else core
        dst = full.at[:, cols((1, 2, 3)[which])]
        return remote(src, dst, t_send.at[which], t_recv.at[which], target)

    t_copy(1).start()
    t_copy(0).start()

    def g_copy(j, k):
        at = (z ^ col) * row_size + y
        return remote(
            gains_ref,
            gain_in.at[at],
            g_send.at[j, k],
            g_recv.at[j, k],
            {"dp": z ^ j, "row": y ^ k},
        )

    pairs = [(j, k) for j in range(4) for k in range(row_size) if j + k > 0]
    for j, k in pairs:
        g_copy(j, k).start()
    gain_in[(z ^ col) * row_size + y] = gains_ref[...]

    attn = Relay(z, lambda o, t: aw_ref.at[slot(o, y)], a_own, a_fwd, a_recv)
    outw = Relay(z, lambda o, t: wo_ref.at[slot(o, y)], o_own, o_fwd, o_recv)
    douts = Relay(z, lambda o, t: do_hbm.at[o ^ t, :, cols(0)], d_own, d_fwd, d_recv)

    def row_copy(ref, o, k, send, recv):
        block = ref.at[slot(o, y)]
        return remote(block, block, send.at[k, o], recv.at[k, o], {"row": y ^ k})

    def row_wait(ref, o, k, send, recv):
        block = ref.at[slot(o, y ^ k)]
        remote(block, block, send.at[k, o], recv.at[k, o], {"row": y ^ k}).wait_recv()

    for load in loads:
        load.wait()
    attn.own(aw_ref.at[slot(z, y)])
    for k in others:
        row_copy(aw_ref, z, k, ay_send, ay_recv).start()

    weights = ((wg_hbm, fg_hbm), (wu_hbm, fu_hbm), (wd_hbm, fd_hbm))

    def quarter(j):
        return pl.ds(pl.multiple_of((z ^ j) * hidden, hidden), hidden)

    pieces = [
        pltpu.make_async_copy(weights[a][0].at[:, quarter(0)], own_piece.at[a], piece_sem.at[a])
        for a in range(3)
    ]
    for piece in pieces:
        piece.start()

    full[:, 0:width] = tok_ref[...]
    cot_ref[...] = (cot_in_ref[...].astype(wide) * valid_ref[...]).astype(low)
    t_copy(1).wait_recv()
    t_copy(2).start()
    attn.arrive(z ^ 1)
    for k in others:
        row_copy(aw_ref, z ^ 1, k, ay_send, ay_recv).start()
    load_out.wait()

    def attn_arrive(j):
        attn.arrive(z ^ j)
        for k in others:
            row_copy(aw_ref, z ^ j, k, ay_send, ay_recv).start()

    @pl.when(mid)
    def _():
        attn_arrive(3)

    outw.own(wo_ref.at[slot(z, y)])

    for j, k in pairs:
        g_copy(j, k).wait_recv()
    for i in range(4 * row_size):
        gain_ref[:, i * local : (i + 1) * local] = gain_in[i]
    t_copy(0).wait_recv()
    t_copy(2).wait_recv()

    def norm(r):
        x = full[r, :].astype(wide)
        factor = lax.rsqrt(jnp.sum(x * x, axis=1, keepdims=True) * (1.0 / model) + EPSILON)
        xn_ref[r, :] = (x * factor * gain_ref[0:1, :]).astype(low)
        factor_ref[r, :] = jnp.broadcast_to(factor, (factor.shape[0], 128))

    tiles(rows, 32, norm)

    @pl.when(jnp.logical_not(mid))
    def _():
        attn_arrive(2)

    attn_arrive_last = jnp.where(mid, 2, 3)
    attn.arrive(z ^ attn_arrive_last)
    for k in others:
        row_copy(aw_ref, z ^ attn_arrive_last, k, ay_send, ay_recv).start()
    for s in range(1, 4):
        outw.arrive(z ^ chunk(s))

    def f_copy(a, j):
        src, dst = weights[a]
        return remote(
            src.at[:, quarter(j)],
            dst.at[slot(z, y)],
            f_send.at[a, j],
            f_recv.at[a, j],
            {"dp": z ^ j},
        )

    for a in range(3):
        for j in (3, 2, 1):
            f_copy(a, j).start()

    def fy_copy(a, j, k):
        src = own_piece.at[a] if j == 0 else weights[a][1].at[slot(z ^ j, y)]
        return remote(
            src,
            weights[a][1].at[slot(z ^ j, y)],
            fy_send.at[a, k, j],
            fy_recv.at[a, k, j],
            {"row": y ^ k},
        )

    for o in range(4):
        for k in others:
            row_wait(aw_ref, o, k, ay_send, ay_recv)
    outs = [
        pltpu.make_async_copy(src, dst, out_sem.at[i])
        for i, (src, dst) in enumerate(((xn_ref, xn_hbm), (aw_ref, aw_hbm), (wo_ref, woo_hbm)))
    ]
    outs[0].start()
    outs[1].start()
    for n in range(0, q_cols + 2 * k_cols, 512):
        qkv[:, n : n + 512] = dot_nn(xn_ref[...], aw_ref[:, n : n + 512])

    def rope(r, at):
        c, s = cos_ref[r, :], sin_ref[r, :]
        first, second = qkv[r, at : at + half], qkv[r, at + half : at + 2 * half]
        return first * c - second * s, second * c + first * s

    def keys(r):
        first, second = rope(r, q_cols)
        kv_ref[y, r, 0:half] = first.astype(low)
        kv_ref[y, r, half : 2 * half] = second.astype(low)
        kv_ref[y, r, k_cols : 2 * k_cols] = qkv[r, q_cols + k_cols : q_cols + 2 * k_cols].astype(low)

    tiles(rows, 64, keys)
    heads = q_cols // HEAD_SIZE

    def queries(r):
        for h in range(heads):
            first, second = rope(r, h * HEAD_SIZE)
            q_ref[h, r, 0:half] = first.astype(low)
            q_ref[h, r, half : 2 * half] = second.astype(low)

    tiles(rows, 64, queries)

    def kv_copy(k, source):
        block = kv_ref.at[source]
        return remote(block, block, kv_send.at[k], kv_recv.at[k], {"row": y ^ k})

    for k in others:

        @pl.when((y ^ k) > y)
        def _():
            kv_copy(k, y).start()

    for o in range(4):
        for k in others:
            row_copy(wo_ref, o, k, oy_send, oy_recv).start()

    douts.own(cot_ref)

    def dx_copy(j):
        src = cot_ref if j == 0 else do_hbm.at[j, :, cols(0)]
        return remote(src, do_hbm.at[j, :, cols(2)], dx_send.at[j], dx_recv.at[j], far)

    def dc_copy(j, which):
        if which:
            src = do_hbm.at[j, :, cols(2)]
        else:
            src = cot_ref if j == 0 else do_hbm.at[j, :, cols(0)]
        return remote(
            src, do_hbm.at[j, :, cols(1 + 2 * which)], dc_send.at[which, j], dc_recv.at[which, j], core
        )

    dx_copy(0).start()
    dc_copy(0, 0).start()
    do_own = pltpu.make_async_copy(cot_ref, do_hbm.at[0, :, cols(0)], do_sem)
    do_own.start()
    for piece in pieces:
        piece.wait()
    stores = [
        pltpu.make_async_copy(own_piece.at[a], weights[a][1].at[slot(z, y)], piece_sem.at[a])
        for a in range(3)
    ]
    for a in range(3):
        stores[a].start()
        for k in others:
            fy_copy(a, 0, k).start()
    for k in others:

        @pl.when((y ^ k) < y)
        def _():
            kv_copy(k, y ^ k).wait_recv()

    q_tile = 256
    score_scale = 1.0 / math.sqrt(HEAD_SIZE)

    def attend_tile(i, unused):
        at = pl.ds(pl.multiple_of(i * q_tile, q_tile), q_tile)
        query_pos = y * rows + i * q_tile + lax.broadcasted_iota(jnp.int32, (q_tile, rows), 0)
        for h in range(heads):
            query = q_ref[h, at, :]

            def block(b, carry):
                top, total, accum = carry
                scores = times_transposed(query, kv_ref[b, :, 0:k_cols]) * score_scale
                key_pos = b * rows + lax.broadcasted_iota(jnp.int32, (q_tile, rows), 1)
                scores = jnp.where(key_pos <= query_pos, scores, -1e30)
                new_top = jnp.maximum(top, jnp.max(scores, axis=1, keepdims=True))
                probs = jnp.exp(scores - new_top)
                keep = jnp.exp(top - new_top)
                total = total * keep + jnp.sum(probs, axis=1, keepdims=True)
                accum = accum * keep + dot_nn(probs.astype(low), kv_ref[b, :, k_cols : 2 * k_cols])
                return new_top, total, accum

            top, total, accum = lax.fori_loop(
                0,
                y + 1,
                block,
                (
                    jnp.full((q_tile, 1), -1e30, wide),
                    jnp.zeros((q_tile, 1), wide),
                    jnp.zeros((q_tile, HEAD_SIZE), wide),
                ),
            )
            lse_ref[h, at, :] = jnp.broadcast_to(top + jnp.log(total), (q_tile, 128))
            mix_ref[at, h * HEAD_SIZE : (h + 1) * HEAD_SIZE] = (
                accum / total * valid_ref[at, :]
            ).astype(low)
        return unused

    lax.fori_loop(0, rows // q_tile, attend_tile, 0)

    for o in range(4):
        for k in others:
            row_wait(wo_ref, o, k, oy_send, oy_recv)
    outs[2].start()
    part_copy = remote(part.at[:, pl.ds(2 * width, 2 * width)], core_in, p_send, p_recv, core)
    for at, p in ((2, 1), (3, 3), (0, 0)):
        part[:, at * width : (at + 1) * width] = times_transposed(
            mix_ref[...], wo_ref[p * width : (p + 1) * width, :]
        ).astype(low)
    part_copy.start()
    part[:, width : 2 * width] = times_transposed(
        mix_ref[...], wo_ref[2 * width : 3 * width, :]
    ).astype(low)
    part_copy.wait()

    def add_core(r):
        x_out[r, :] = (
            part[r, width : 2 * width].astype(wide) + core_in[r, width : 2 * width].astype(wide)
        ).astype(low)
        h_ref[r, :] = (
            tok_ref[r, :].astype(wide)
            + part[r, 0:width].astype(wide)
            + core_in[r, 0:width].astype(wide)
        )

    tiles(rows, 64, add_core)
    r_copy = remote(x_out, x_in, r_send, r_recv, far)
    r_copy.start()

    def f_arrive(a, j):
        f_copy(a, j).wait_recv()
        for k in others:
            fy_copy(a, j, k).start()

    for j in (1, 2, 3):
        f_arrive(0, j)
    r_copy.wait()

    def add_far(r):
        total = h_ref[r, :] + x_in[r, :].astype(wide)
        h_ref[r, :] = total
        hlow_ref[r, :] = total.astype(low)

    tiles(rows, 64, add_far)
    for a in (1, 2):
        for j in (1, 2, 3):
            f_arrive(a, j)

    def d_arrive(j):
        douts.arrive(z ^ j)
        dx_copy(j).start()
        dc_copy(j, 0).start()

    def d_settle(j):
        dx_copy(j).wait_recv()
        dc_copy(j, 1).start()

    d_settle(0)
    for s in range(1, 4):
        for j in sorted({s, 5 - s} if s >= 2 else {s}):
            if s < 2:
                d_arrive(j)
            else:

                @pl.when(chunk(s) == j)
                def _():
                    d_arrive(j)

    for j in (1, 2, 3):
        d_settle(j)

    for a in range(3):
        stores[a].wait()
        for j in range(4):
            for k in others:
                fy_copy(a, j, k).wait_send()
                block = weights[a][1].at[slot(z ^ j, y ^ k)]
                remote(
                    block, block, fy_send.at[a, k, j], fy_recv.at[a, k, j], {"row": y ^ k}
                ).wait_recv()
            if j:
                f_copy(a, j).wait_send()
    do_own.wait()
    for out in outs:
        out.wait()
    for j in range(4):
        dx_copy(j).wait_send()
        dc_copy(j, 0).wait()
        dc_copy(j, 1).wait()
    for relay, src in ((attn, aw_ref.at[slot(z, y)]), (outw, wo_ref.at[slot(z, y)]), (douts, cot_ref)):
        relay.own(src, wait=True)
        for j in (1, 2, 3):
            relay.forward(z ^ j, wait=True)
    for o in range(4):
        for k in others:
            row_copy(aw_ref, o, k, ay_send, ay_recv).wait_send()
            row_copy(wo_ref, o, k, oy_send, oy_recv).wait_send()
    for k in others:

        @pl.when((y ^ k) > y)
        def _():
            kv_copy(k, y).wait_send()

    for j, k in pairs:
        g_copy(j, k).wait_send()
    for which in range(3):
        t_copy(which).wait_send()


def attn_fwd_call(tokens, cot, gains, cos, sin, valid, wq, wk, wv, wo, wg, wu, wd):
    rows, width = tokens.shape
    model = 4 * width
    low, wide = jnp.bfloat16, jnp.float32
    row_size = lax.axis_size("row")
    local, q_cols = wq.shape
    k_cols = wk.shape[1]
    hidden = wg.shape[1] // 4
    heads = q_cols // HEAD_SIZE
    vmem = pl.BlockSpec(memory_space=pltpu.VMEM)
    hbm = pl.BlockSpec(memory_space=pl.ANY)
    dma = pltpu.SemaphoreType.DMA
    relay = [dma((2,)), dma((4,)), dma((4,))]
    over_row = [dma((row_size, 4)), dma((row_size, 4))]
    shape = jax.ShapeDtypeStruct
    return pl.pallas_call(
        attn_fwd_kernel,
        out_shape=(
            shape((rows, 128), wide),
            shape((heads, rows, HEAD_SIZE), low),
            shape((row_size, rows, 2 * k_cols), low),
            shape((heads, rows, 128), wide),
            shape((rows, q_cols), low),
            shape((rows, width), wide),
            shape((rows, width), low),
            shape((8, model), wide),
            shape((rows, model), low),
            shape((model, q_cols + 2 * k_cols), low),
            shape((model, q_cols), low),
            shape((model, hidden), low),
            shape((model, hidden), low),
            shape((model, hidden), low),
            shape((4, rows, model), low),
        ),
        in_specs=[vmem] * 6 + [hbm] * 7,
        out_specs=(vmem,) * 8 + (hbm,) * 7,
        scratch_shapes=[
            pltpu.VMEM((rows, model), low),
            pltpu.VMEM((model, q_cols + 2 * k_cols), low),
            pltpu.VMEM((model, q_cols), low),
            pltpu.VMEM((rows, width), low),
            dma((3,)),
            pltpu.VMEM((rows, model), low),
            pltpu.VMEM((rows, q_cols + 2 * k_cols), wide),
            pltpu.VMEM((4 * row_size, 8, local), wide),
            pltpu.VMEM((3, local, hidden), low),
            pltpu.VMEM((rows, model), low),
            pltpu.VMEM((rows, 2 * width), low),
            pltpu.VMEM((rows, width), low),
            pltpu.VMEM((rows, width), low),
            dma((4,)),
            dma((3,)),
            dma(()),
            dma((4, row_size)),
            dma((4, row_size)),
            dma((1,)),
            dma((1,)),
            dma((3,)),
            dma((3,)),
            *relay,
            *over_row,
            *relay,
            *over_row,
            dma((3, 4)),
            dma((3, 4)),
            dma((3, row_size, 4)),
            dma((3, row_size, 4)),
            *relay,
            dma((4,)),
            dma((4,)),
            dma((2, 4)),
            dma((2, 4)),
            dma((row_size,)),
            dma((row_size,)),
            dma(()),
            dma(()),
            dma(()),
            dma(()),
        ],
        compiler_params=pltpu.CompilerParams(
            collective_id=1, has_side_effects=True, vmem_limit_bytes=60_000_000
        ),
        cost_estimate=pl.CostEstimate(
            flops=10_000_000_000, bytes_accessed=40_000_000, transcendentals=2_000_000
        ),
    )(tokens, cot, gains, cos, sin, valid, wq, wk, wv, wo, wg, wu, wd)


class Reduce:
    def __init__(self, z, mid, block, inbox, send, recv):
        self.z, self.mid, self.block, self.inbox = z, mid, block, inbox
        self.send, self.recv = send, recv

    def copy(self, j):
        owner = self.z ^ j
        above = owner > self.z
        target = jnp.where(above, self.z + 1, self.z - 1)
        slot = jnp.where(target == owner, jnp.where(above, 3, 4), (target ^ owner) - 1)
        return remote(
            self.block(j), self.inbox.at[slot], self.send.at[j], self.recv.at[slot], {"dp": target}
        )

    def arrived(self, slot):
        block = self.inbox.at[slot]
        remote(block, block, self.send.at[0], self.recv.at[slot], {"dp": self.z ^ 1}).wait_recv()

    def first(self, j):
        @pl.when(jnp.logical_not(self.mid))
        def _():
            self.copy(j).start()

    def relay(self, j, add):
        @pl.when(self.mid)
        def _():
            self.arrived(j - 1)
            add(j)
            self.copy(j).start()

    def finish(self, add):
        @pl.when(self.z > 0)
        def _():
            self.arrived(3)
            add(3)

        @pl.when(self.z < 3)
        def _():
            self.arrived(4)
            add(4)

    def drain(self):
        for j in (1, 2, 3):
            self.copy(j).wait_send()


def lane_sums(value):
    total = value[:, 0:128]
    for at in range(128, value.shape[1], 128):
        total = total + value[:, at : at + 128]
    return total


def attn_bwd_kernel(
    dhn_ref,
    factor_two_ref,
    h_ref,
    dout_ref,
    gain_ref,
    tok_ref,
    factor_one_ref,
    cos_ref,
    sin_ref,
    valid_ref,
    q_ref,
    lse_ref,
    mix_ref,
    xn_hbm,
    kv_hbm,
    aw_hbm,
    wo_hbm,
    out_hbm,
    dwg_hbm,
    dwu_hbm,
    dwd_hbm,
    layer_ref,
    dtok_ref,
    gains_ref,
    dattn_ref,
    dwo_ref,
    gg_ref,
    gu_ref,
    gd_ref,
    full,
    xn,
    kv,
    aw,
    wo,
    lanes,
    lanes_in,
    do,
    delta,
    dq,
    dkv,
    dkv_out,
    dkv_in,
    graw,
    dw_attn,
    dw_out,
    own_f,
    row_f,
    row_a,
    row_o,
    z_a,
    z_o,
    in_a,
    in_o,
    out_own,
    core_in,
    x_in,
    z_in,
    pcore_in,
    px_out,
    px_in,
    gvec,
    g_in,
    load_sem,
    l_send,
    l_recv,
    t_send,
    t_recv,
    fy_send,
    fy_recv,
    fz_send,
    fz_recv,
    own_sem,
    oc_send,
    oc_recv,
    oo_sem,
    ox_send,
    ox_recv,
    oz_send,
    oz_recv,
    kv_send,
    kv_recv,
    ay_send,
    ay_recv,
    az_send,
    az_recv,
    wy_send,
    wy_recv,
    wz_send,
    wz_recv,
    p_send,
    p_recv,
    r_send,
    r_recv,
    g_send,
    g_recv,
    gc_send,
    gc_recv,
):
    rows, width = tok_ref.shape
    model = 4 * width
    low, wide = jnp.bfloat16, jnp.float32
    row_size = lax.axis_size("row")
    local = model // (4 * row_size)
    heads = q_ref.shape[0]
    q_cols = heads * HEAD_SIZE
    all_cols = graw.shape[1]
    k_cols = (all_cols - q_cols) // 2
    hidden = own_f.shape[3]
    half = HEAD_SIZE // 2
    score_scale = 1.0 / math.sqrt(HEAD_SIZE)
    z, y, col = (lax.axis_index(name) for name in ("dp", "row", "col"))
    core, far = {"col": col ^ 1}, {"col": col ^ 2}
    others = range(1, row_size)
    mid = jnp.logical_and(z > 0, z < 3)
    third = jnp.where(mid, 2, 3)
    second = jnp.where(mid, 3, 2)
    by_distance = (third, second, 1, 0)
    partials = (dwg_hbm, dwu_hbm, dwd_hbm)
    results = (gg_ref, gu_ref, gd_ref)

    def cols(p):
        return pl.ds(p * width, width)

    greet(
        [{"dp": z ^ j, "row": y ^ k} for j in range(4) for k in range(row_size) if j + k > 0]
        + [{"col": col ^ m} for m in (1, 2, 3)]
    )

    def fy_copy(a, j, k):
        at = z ^ j ^ col
        return remote(
            partials[a].at[at, y ^ k],
            row_f.at[a, k - 1, j],
            fy_send.at[a, k, j],
            fy_recv.at[a, k, j],
            {"row": y ^ k},
        )

    far_first = (3, 2, 1, 0)
    for a in (0, 1):
        for j in far_first:
            for k in others:
                fy_copy(a, j, k).start()

    def own_load(a, j):
        return pltpu.make_async_copy(
            partials[a].at[z ^ j ^ col, y], own_f.at[a, j], own_sem.at[a, j]
        )

    def oc_copy(j, which):
        return remote(
            out_hbm.at[j, :, cols(1 + 2 * which)],
            core_in.at[j, :, cols(which)],
            oc_send.at[which, j],
            oc_recv.at[which, j],
            core,
        )

    def oo_copy(j, which):
        return pltpu.make_async_copy(
            out_hbm.at[j, :, cols(2 * which)], out_own.at[j, :, cols(which)], oo_sem.at[which, j]
        )

    loads = [
        pltpu.make_async_copy(src, dst, load_sem.at[i])
        for i, (src, dst) in enumerate(((wo_hbm, wo), (xn_hbm, xn), (aw_hbm, aw)))
    ]

    gain_two = gain_ref[1:2, 0:width]
    gain_one = gain_ref[0:1, 0:width]

    def residual(r):
        return h_ref[r, :].astype(low).astype(wide)

    def inner_two(r):
        lanes[0, r, :] = lane_sums(gain_two * dhn_ref[r, :] * residual(r)).astype(low)

    tiles(rows, 64, inner_two)
    for j in by_distance:
        for which in (0, 1):
            oc_copy(j, which).start()
            oo_copy(j, which).start()

    def l_copy(n, m):
        return remote(
            lanes.at[n], lanes_in.at[n, m - 1], l_send.at[n, m - 1], l_recv.at[n, m - 1], {"col": col ^ m}
        )

    for m in (2, 3, 1):
        l_copy(0, m).start()
    for load in loads:
        load.start()
    for a in range(3):
        for j in far_first:
            own_load(a, j).start()

    def inner(n, r):
        total = lanes[n, r, :].astype(wide)
        for m in range(3):
            total = total + lanes_in[n, m, r, :].astype(wide)
        return jnp.sum(total, axis=1, keepdims=True) * (1.0 / model)

    def gain_two_sum(i, total):
        r = pl.ds(pl.multiple_of(i * 64, 64), 64)
        return total + jnp.sum(
            dhn_ref[r, :] * residual(r) * factor_two_ref[r, 0:1], axis=0, keepdims=True
        )

    gain_two_grad = lax.fori_loop(0, rows // 64, gain_two_sum, jnp.zeros((1, width), wide))
    for m in (1, 2, 3):
        l_copy(0, m).wait_recv()

    def grad_residual(r):
        factor = factor_two_ref[r, 0:1]
        grad = (
            dout_ref[r, :].astype(wide) * valid_ref[r, :]
            + factor * gain_two * dhn_ref[r, :]
            - residual(r) * factor * factor * factor * inner(0, r)
        ).astype(low)
        full[r, 0:width] = grad
        dtok_ref[r, :] = grad

    tiles(rows, 64, grad_residual)

    def t_copy(which):
        src = full.at[:, cols(2)] if which == 2 else full.at[:, cols(0)]
        dst = full.at[:, cols((1, 2, 3)[which])]
        return remote(
            src, dst, t_send.at[which], t_recv.at[which], far if which == 1 else core
        )

    def ox_copy(j):
        return remote(out_own.at[j, :, cols(1)], x_in.at[j], ox_send.at[j], ox_recv.at[j], far)

    def out_core(j):
        for which in (0, 1):
            oo_copy(j, which).wait()
            oc_copy(j, which).wait_recv()

        def add(r):
            out_own[j, r, width : 2 * width] = (
                out_own[j, r, width : 2 * width].astype(wide)
                + core_in[j, r, width : 2 * width].astype(wide)
            ).astype(low)
            out_own[j, r, 0:width] = (
                out_own[j, r, 0:width].astype(wide) + core_in[j, r, 0:width].astype(wide)
            ).astype(low)

        tiles(rows, 64, add)

    out_core(third)
    t_copy(1).start()
    t_copy(0).start()
    ox_copy(third).start()

    outs = Reduce(z, mid, lambda j: out_own.at[j, :, cols(0)], z_in, oz_send, oz_recv)

    def out_add(j):
        def add(r):
            out_own[j, r, 0:width] = (
                out_own[j, r, 0:width].astype(wide) + z_in[j - 1, r, :].astype(wide)
            ).astype(low)

        tiles(rows, 64, add)

    def out_far(j):
        ox_copy(j).wait_recv()

        def add(r):
            out_own[j, r, 0:width] = (
                out_own[j, r, 0:width].astype(wide) + x_in[j, r, :].astype(wide)
            ).astype(low)

        tiles(rows, 64, add)

    def fz_copy(a, j):
        at = pl.ds(pl.multiple_of(z * hidden, hidden), hidden)
        return remote(
            own_f.at[a, j], results[a].at[:, at], fz_send.at[a, j], fz_recv.at[a, j], {"dp": z ^ j}
        )

    def f_own(a):
        at = pl.ds(pl.multiple_of(z * hidden, hidden), hidden)
        return pltpu.make_async_copy(own_f.at[a, 0], results[a].at[:, at], own_sem.at[a, 0])

    def f_row(a, j):
        own_load(a, j).wait()
        for k in others:
            fy_copy(a, j, k).wait_recv()
        total = own_f[a, j].astype(wide)
        for k in others:
            total = total + row_f[a, k - 1, j].astype(wide)
        own_f[a, j] = total.astype(low)

    out_core(second)
    f_row(0, 3)
    ox_copy(second).start()
    out_core(1)
    fz_copy(0, 3).start()
    ox_copy(1).start()
    t_copy(1).wait_recv()
    t_copy(2).start()
    out_core(0)
    t_copy(0).wait_recv()
    f_row(0, 2)
    ox_copy(0).start()
    loads[0].wait()
    t_copy(2).wait_recv()

    do[...] = (dot_nn(full[...], wo[...]) * valid_ref[...]).astype(low)
    fz_copy(0, 2).start()
    for p in range(4):
        at = slice(p * width, (p + 1) * width)
        dw_out[at, :] = contract_rows(full[:, at], mix_ref[...]).astype(low)

    def deltas(r):
        for h in range(heads):
            at = slice(h * HEAD_SIZE, (h + 1) * HEAD_SIZE)
            total = jnp.sum(do[r, at].astype(wide) * mix_ref[r, at].astype(wide), axis=1, keepdims=True)
            delta[h, r, :] = jnp.broadcast_to(total, (total.shape[0], 128))

    tiles(rows, 64, deltas)
    dq[...] = jnp.zeros_like(dq)
    q_tile = 256

    def attend_block(b, slot):
        dkv[...] = jnp.zeros_like(dkv)

        def tile(i, unused):
            at = pl.ds(pl.multiple_of(i * q_tile, q_tile), q_tile)
            query_pos = y * rows + i * q_tile + lax.broadcasted_iota(jnp.int32, (q_tile, rows), 0)
            key_pos = b * rows + lax.broadcasted_iota(jnp.int32, (q_tile, rows), 1)
            for h in range(heads):
                head = slice(h * HEAD_SIZE, (h + 1) * HEAD_SIZE)
                query, grad = q_ref[h, at, :], do[at, head]
                keys, values = kv[slot, :, 0:k_cols], kv[slot, :, k_cols : 2 * k_cols]
                scores = times_transposed(query, keys) * score_scale
                probs = jnp.where(
                    key_pos <= query_pos, jnp.exp(scores - lse_ref[h, at, 0:1]), 0.0
                )
                grad_probs = times_transposed(grad, values)
                grad_scores = (probs * (grad_probs - delta[h, at, 0:1]) * score_scale).astype(low)
                dq[at, head] += dot_nn(grad_scores, keys)
                dkv[:, 0:k_cols] += contract_rows(grad_scores, query)
                dkv[:, k_cols : 2 * k_cols] += contract_rows(probs.astype(low), grad)
            return unused

        lax.fori_loop(0, rows // q_tile, tile, 0)

    def kv_copy(k):
        return remote(
            dkv_out, dkv_in.at[k - 1], kv_send.at[k], kv_recv.at[k], {"row": y ^ k}
        )

    blocks = [*others, 0]

    def when_block(k, body):
        if k:
            pl.when((y ^ k) < y)(body)
        else:
            body()

    def kv_load(i):
        return pltpu.make_async_copy(
            kv_hbm.at[y ^ blocks[i]], kv.at[i % 2], load_sem.at[3 + i % 2]
        )

    when_block(blocks[0], lambda: kv_load(0).start())
    for i, k in enumerate(others):
        when_block(k, lambda i=i: kv_load(i).wait())
        when_block(blocks[i + 1], lambda i=i: kv_load(i + 1).start())
        when_block(k, lambda i=i, k=k: attend_block(y ^ k, i % 2))
        if i:
            when_block(k - 1, lambda k=k: kv_copy(k - 1).wait_send())

        def keep(r):
            dkv_out[r, :] = dkv[r, :].astype(low)

        when_block(k, lambda: tiles(rows, 64, keep))
        if i == 0:
            f_row(0, 1)
            f_row(0, 0)
        when_block(k, lambda k=k: kv_copy(k).start())

    fz_copy(0, 1).start()
    f_own(0).start()
    out_far(third)
    f_row(1, 3)
    outs.first(third)
    fz_copy(1, 3).start()

    def wy_copy(j, k):
        at = pl.ds(pl.multiple_of(((z ^ j ^ col) * row_size + (y ^ k)) * local, local), local)
        return remote(
            dw_out.at[at], row_o.at[k - 1, j], wy_send.at[k, j], wy_recv.at[k, j], {"row": y ^ k}
        )

    for j in by_distance:
        for k in others:
            wy_copy(j, k).start()
    for j in far_first:
        for k in others:
            fy_copy(2, j, k).start()
    kv_load(len(others)).wait()
    out_far(second)
    outs.first(second)
    outs.relay(third, out_add)
    attend_block(y, len(others) % 2)

    def back(r, first, second, at):
        c, s = cos_ref[r, :], sin_ref[r, :]
        graw[r, at : at + half] = (first * c + second * s).astype(low)
        graw[r, at + half : at + 2 * half] = (second * c - first * s).astype(low)

    def queries(r):
        for h in range(heads):
            at = h * HEAD_SIZE
            back(r, dq[r, at : at + half], dq[r, at + half : at + 2 * half], at)

    tiles(rows, 64, queries)
    for k in others:

        @pl.when((y ^ k) > y)
        def _():
            kv_copy(k).wait_recv()

            def add(r):
                dkv[r, :] = dkv[r, :] + dkv_in[k - 1, r, :].astype(wide)

            tiles(rows, 64, add)

    def keys_back(r):
        back(r, dkv[r, 0:half], dkv[r, half : 2 * half], q_cols)
        graw[r, q_cols + k_cols : all_cols] = dkv[r, k_cols : 2 * k_cols].astype(low)

    tiles(rows, 64, keys_back)
    loads[1].wait()
    loads[2].wait()
    f_row(1, 2)

    def ay_copy(j, k):
        at = pl.ds(pl.multiple_of(((z ^ j ^ col) * row_size + (y ^ k)) * local, local), local)
        return remote(
            dw_attn.at[at], row_a.at[k - 1, j], ay_send.at[k, j], ay_recv.at[k, j], {"row": y ^ k}
        )

    for p in range(4):
        at = slice(p * width, (p + 1) * width)
        for n in range(0, all_cols, 512):
            dw_attn[at, n : n + 512] = contract_rows(xn[:, at], graw[:, n : n + 512]).astype(low)
    fz_copy(1, 2).start()
    for which in range(3):
        t_copy(which).wait_send()
    part = full
    part_copy = remote(part.at[:, pl.ds(2 * width, 2 * width)], pcore_in, p_send, p_recv, core)
    for q, p in ((2, 1), (3, 3)):
        part[:, q * width : (q + 1) * width] = times_transposed(
            graw[...], aw[p * width : (p + 1) * width, :]
        ).astype(low)
    for j in by_distance:
        for k in others:
            ay_copy(j, k).start()
    for q, p in ((0, 0), (1, 2)):
        part[:, q * width : (q + 1) * width] = times_transposed(
            graw[...], aw[p * width : (p + 1) * width, :]
        ).astype(low)
    part_copy.start()
    f_row(1, 1)
    f_row(1, 0)
    part_copy.wait()
    fz_copy(1, 1).start()
    f_own(1).start()

    def add_core(r):
        px_out[r, :] = (
            part[r, width : 2 * width].astype(wide) + pcore_in[r, width : 2 * width].astype(wide)
        ).astype(low)

    tiles(rows, 64, add_core)
    out_far(1)
    r_copy = remote(px_out, px_in, r_send, r_recv, far)
    r_copy.start()
    outs.first(1)
    outs.relay(second, out_add)

    outw = Reduce(z, mid, lambda j: z_o.at[j - 1], in_o, wz_send, wz_recv)

    def o_add(j):
        def add(r):
            z_o[j - 1, r, :] = (
                z_o[j - 1, r, :].astype(wide) + in_o[j - 1, r, :].astype(wide)
            ).astype(low)

        tiles(local, 32, add)

    def o_row(j):
        for k in others:
            wy_copy(j, k).wait_recv()
        at = pl.ds(pl.multiple_of(((z ^ j ^ col) * row_size + y) * local, local), local)
        total = dw_out[at, :].astype(wide)
        for k in others:
            total = total + row_o[k - 1, j].astype(wide)
        if isinstance(j, int) and j == 0:
            dwo_ref[...] = total
        else:
            z_o[j - 1] = total.astype(low)

    o_row(third)
    out_far(0)
    outw.first(third)
    outs.relay(1, out_add)
    o_row(second)
    o_row(1)
    outw.first(second)
    o_row(0)
    outw.first(1)
    r_copy.wait()

    def dxn(r):
        return (
            part[r, 0:width].astype(wide) + pcore_in[r, 0:width].astype(wide) + px_in[r, :].astype(wide)
        )

    def inner_one(i, total):
        r = pl.ds(pl.multiple_of(i * 64, 64), 64)
        grad, tokens = dxn(r), tok_ref[r, :].astype(wide)
        lanes[1, r, :] = lane_sums(gain_one * grad * tokens).astype(low)
        return total + jnp.sum(grad * tokens * factor_one_ref[r, 0:1], axis=0, keepdims=True)

    gain_one_grad = lax.fori_loop(0, rows // 64, inner_one, jnp.zeros((1, width), wide))
    for i in range(row_size):
        at = slice(i * local, (i + 1) * local)
        gvec[i, 0:1, :] = gain_one_grad[:, at]
        gvec[i, 1:2, :] = gain_two_grad[:, at]
        gvec[i, 2:8, :] = jnp.zeros((6, local), wide)
    f_row(2, 3)
    for m in (2, 3, 1):
        l_copy(1, m).start()
    mine = z == col

    def g_copy(k):
        return remote(
            gvec.at[y ^ k],
            g_in.at[z * row_size + y],
            g_send.at[k],
            g_recv.at[z, k],
            {"dp": col, "row": y ^ k},
        )

    for k in range(row_size):
        if k:
            g_copy(k).start()
        else:

            @pl.when(jnp.logical_not(mine))
            def _():
                g_copy(0).start()

            @pl.when(mine)
            def _():
                g_in[z * row_size + y] = gvec[y]

    fz_copy(2, 3).start()
    outw.relay(third, o_add)
    f_row(2, 2)
    f_row(2, 1)
    fz_copy(2, 2).start()
    outw.relay(second, o_add)
    f_row(2, 0)
    fz_copy(2, 1).start()
    f_own(2).start()
    outw.relay(1, o_add)
    for m in (1, 2, 3):
        l_copy(1, m).wait_recv()

    def grad_tokens(r):
        factor = factor_one_ref[r, 0:1]
        dtok_ref[r, :] = (
            dtok_ref[r, :].astype(wide)
            + factor * gain_one * dxn(r)
            - tok_ref[r, :].astype(wide) * factor * factor * factor * inner(1, r)
        ).astype(low)

    tiles(rows, 64, grad_tokens)

    attn = Reduce(z, mid, lambda j: z_a.at[j - 1], in_a, az_send, az_recv)

    def a_add(j):
        def add(r):
            z_a[j - 1, r, :] = (
                z_a[j - 1, r, :].astype(wide) + in_a[j - 1, r, :].astype(wide)
            ).astype(low)

        tiles(local, 32, add)

    def a_row(j):
        for k in others:
            ay_copy(j, k).wait_recv()
        at = pl.ds(pl.multiple_of(((z ^ j ^ col) * row_size + y) * local, local), local)
        total = dw_attn[at, :].astype(wide)
        for k in others:
            total = total + row_a[k - 1, j].astype(wide)
        if isinstance(j, int) and j == 0:
            dattn_ref[...] = total
        else:
            z_a[j - 1] = total.astype(low)

    a_row(third)
    a_row(second)
    attn.first(third)
    a_row(1)
    attn.first(second)
    a_row(0)
    attn.first(1)
    attn.relay(third, a_add)
    attn.relay(second, a_add)
    attn.relay(1, a_add)

    def gc_copy(m):
        return remote(
            gains_ref, gains_ref, gc_send.at[m - 1], gc_recv, {"col": col ^ m}
        )

    @pl.when(mine)
    def _():
        for j in range(4):
            for k in range(row_size):
                if j + k:
                    block = g_in.at[(z ^ j) * row_size + (y ^ k)]
                    remote(
                        block, block, g_send.at[k], g_recv.at[z ^ j, k], {"dp": z ^ j, "row": y ^ k}
                    ).wait_recv()
        total = g_in[0]
        for i in range(1, 4 * row_size):
            total = total + g_in[i]
        gains_ref[...] = total

    @pl.when(mine)
    def _():
        for m in (1, 2, 3):
            gc_copy(m).start()

    for slot in (3, 4):

        @pl.when((z > 0) if slot == 3 else (z < 3))
        def _():
            outs.arrived(slot)

        @pl.when((z == 0) if slot == 3 else (z == 3))
        def _():
            z_in[slot] = jnp.zeros((rows, width), low)

    def layer_out(r):
        total = h_ref[r, :] + out_own[0, r, 0:width].astype(wide)
        for slot in (3, 4):
            total = total + z_in[slot, r, :].astype(wide)
        layer_ref[r, :] = total.astype(low)

    tiles(rows, 64, layer_out)

    def o_last(slot):
        dwo_ref[...] = dwo_ref[...] + in_o[slot].astype(wide)

    outw.finish(o_last)
    for a in range(3):
        f_own(a).wait()
        for j in (1, 2, 3):
            at = pl.ds(pl.multiple_of((z ^ j) * hidden, hidden), hidden)
            block = results[a].at[:, at]
            remote(block, block, fz_send.at[a, j], fz_recv.at[a, j], {"dp": z ^ j}).wait_recv()

    def a_last(slot):
        dattn_ref[...] = dattn_ref[...] + in_a[slot].astype(wide)

    attn.finish(a_last)

    @pl.when(jnp.logical_not(mine))
    def _():
        gc_copy(1).wait_recv()

    @pl.when(mine)
    def _():
        for m in (1, 2, 3):
            gc_copy(m).wait_send()

    for k in range(row_size):
        if k:
            g_copy(k).wait_send()
        else:

            @pl.when(jnp.logical_not(mine))
            def _():
                g_copy(0).wait_send()

    for n in (0, 1):
        for m in (1, 2, 3):
            l_copy(n, m).wait_send()
    for summed in (outs, outw, attn):
        summed.drain()
    for j in range(4):
        ox_copy(j).wait_send()
        for which in (0, 1):
            oc_copy(j, which).wait_send()
        if j:
            for a in range(3):
                fz_copy(a, j).wait_send()
        for k in others:
            wy_copy(j, k).wait_send()
            ay_copy(j, k).wait_send()
            for a in range(3):
                fy_copy(a, j, k).wait_send()
    when_block(row_size - 1, lambda: kv_copy(row_size - 1).wait_send())


def attn_bwd_call(
    dhn,
    factor_two,
    h,
    dout,
    gains,
    tokens,
    factor_one,
    cos,
    sin,
    valid,
    q,
    lse,
    mix,
    xn,
    kv,
    aw,
    wo,
    out_part,
    dwg,
    dwu,
    dwd,
):
    rows, width = tokens.shape
    model, hidden = dwg.shape
    low, wide = jnp.bfloat16, jnp.float32
    row_size = lax.axis_size("row")
    local = model // (4 * row_size)
    all_cols, q_cols = aw.shape[1], wo.shape[1]
    heads = q_cols // HEAD_SIZE
    kv_cols = kv.shape[2]
    vmem = pl.BlockSpec(memory_space=pltpu.VMEM)
    hbm = pl.BlockSpec(memory_space=pl.ANY)
    dma = pltpu.SemaphoreType.DMA
    shape = jax.ShapeDtypeStruct
    blocks = [part.reshape(4, row_size, local, hidden) for part in (dwg, dwu, dwd)]
    return pl.pallas_call(
        attn_bwd_kernel,
        out_shape=(
            shape((rows, width), low),
            shape((rows, width), low),
            shape((8, local), wide),
            shape((local, all_cols), wide),
            shape((local, q_cols), wide),
            shape((local, 4 * hidden), low),
            shape((local, 4 * hidden), low),
            shape((local, 4 * hidden), low),
        ),
        in_specs=[vmem] * 13 + [hbm] * 8,
        out_specs=(vmem,) * 5 + (hbm,) * 3,
        scratch_shapes=[
            pltpu.VMEM((rows, model), low),
            pltpu.VMEM((rows, model), low),
            pltpu.VMEM((2, rows, kv_cols), low),
            pltpu.VMEM((model, all_cols), low),
            pltpu.VMEM((model, q_cols), low),
            pltpu.VMEM((2, rows, 128), low),
            pltpu.VMEM((2, 3, rows, 128), low),
            pltpu.VMEM((rows, q_cols), low),
            pltpu.VMEM((heads, rows, 128), wide),
            pltpu.VMEM((rows, q_cols), wide),
            pltpu.VMEM((rows, kv_cols), wide),
            pltpu.VMEM((rows, kv_cols), low),
            pltpu.VMEM((row_size - 1, rows, kv_cols), low),
            pltpu.VMEM((rows, all_cols), low),
            pltpu.VMEM((model, all_cols), low),
            pltpu.VMEM((model, q_cols), low),
            pltpu.VMEM((3, 4, local, hidden), low),
            pltpu.VMEM((3, row_size - 1, 4, local, hidden), low),
            pltpu.VMEM((row_size - 1, 4, local, all_cols), low),
            pltpu.VMEM((row_size - 1, 4, local, q_cols), low),
            pltpu.VMEM((3, local, all_cols), low),
            pltpu.VMEM((3, local, q_cols), low),
            pltpu.VMEM((5, local, all_cols), low),
            pltpu.VMEM((5, local, q_cols), low),
            pltpu.VMEM((4, rows, 2 * width), low),
            pltpu.VMEM((4, rows, 2 * width), low),
            pltpu.VMEM((4, rows, width), low),
            pltpu.VMEM((5, rows, width), low),
            pltpu.VMEM((rows, 2 * width), low),
            pltpu.VMEM((rows, width), low),
            pltpu.VMEM((rows, width), low),
            pltpu.VMEM((row_size, 8, local), wide),
            pltpu.VMEM((4 * row_size, 8, local), wide),
            dma((5,)),
            dma((2, 3)),
            dma((2, 3)),
            dma((3,)),
            dma((3,)),
            dma((3, row_size, 4)),
            dma((3, row_size, 4)),
            dma((3, 4)),
            dma((3, 4)),
            dma((3, 4)),
            dma((2, 4)),
            dma((2, 4)),
            dma((2, 4)),
            dma((4,)),
            dma((4,)),
            dma((4,)),
            dma((5,)),
            dma((row_size,)),
            dma((row_size,)),
            dma((row_size, 4)),
            dma((row_size, 4)),
            dma((4,)),
            dma((5,)),
            dma((row_size, 4)),
            dma((row_size, 4)),
            dma((4,)),
            dma((5,)),
            dma(()),
            dma(()),
            dma(()),
            dma(()),
            dma((row_size,)),
            dma((4, row_size)),
            dma((3,)),
            dma(()),
        ],
        compiler_params=pltpu.CompilerParams(
            collective_id=3, has_side_effects=True, vmem_limit_bytes=66_000_000
        ),
        cost_estimate=pl.CostEstimate(
            flops=14_000_000_000, bytes_accessed=40_000_000, transcendentals=2_000_000
        ),
    )(
        dhn,
        factor_two,
        h,
        dout,
        gains,
        tokens,
        factor_one,
        cos,
        sin,
        valid,
        q,
        lse,
        mix,
        xn,
        kv,
        aw,
        wo,
        out_part,
        *blocks,
    )


def per_device(
    tokens,
    w_query,
    key_matrix,
    value_matrix,
    w_output,
    w_gate,
    w_up,
    w_down,
    gain_attn,
    gain_ffn,
    lengths,
    cotangent,
):
    low = jnp.bfloat16
    wide = jnp.float32
    row_count = tokens.shape[0]
    me_row = lax.axis_index("row")
    query_pos = me_row * row_count + jnp.arange(row_count, dtype=jnp.int32)
    valid = (query_pos < lengths[0]).astype(wide)[:, None]
    cosine_table, sine_table = rope_tables(query_pos.astype(wide))

    gains = jnp.zeros((8, gain_attn.shape[0]), wide)
    gains = gains.at[0].set(gain_attn.astype(wide)).at[1].set(gain_ffn.astype(wide))
    q_cols, k_cols = w_query.shape[1], key_matrix.shape[1]
    (
        factor_one,
        query_rows,
        kv_all,
        log_total,
        mixed_heads,
        residual,
        residual_low,
        gains,
        normed,
        attn_weight,
        out_weight,
        gate_weight,
        up_weight,
        down_weight,
        grad_out_full,
    ) = attn_fwd_call(
        tokens,
        cotangent,
        gains,
        cosine_table,
        sine_table,
        valid,
        w_query,
        key_matrix,
        value_matrix,
        w_output.T,
        w_gate,
        w_up,
        w_down.T,
    )
    grad_normed_two, factor_two, out_part, grad_gate_part, grad_up_part, grad_down_part = ffn_call(
        residual_low, gains, grad_out_full, gate_weight, up_weight, down_weight
    )
    (
        layer_out,
        grad_tokens,
        gain_grads,
        grad_attn,
        grad_output,
        grad_gate,
        grad_up,
        grad_down,
    ) = attn_bwd_call(
        grad_normed_two,
        factor_two,
        residual,
        cotangent,
        gains,
        tokens,
        factor_one,
        cosine_table,
        sine_table,
        valid,
        query_rows,
        log_total,
        mixed_heads,
        normed,
        kv_all,
        attn_weight,
        out_weight,
        out_part,
        grad_gate_part,
        grad_up_part,
        grad_down_part,
    )
    return (
        layer_out,
        grad_tokens,
        gain_grads[0],
        gain_grads[1],
        grad_attn[:, :q_cols],
        grad_attn[:, q_cols : q_cols + k_cols],
        grad_attn[:, q_cols + k_cols :],
        grad_output.T,
        grad_gate.astype(wide),
        grad_up.astype(wide),
        grad_down.T.astype(wide),
    )


def solution(mesh):
    in_specs = (
        P(("dp", "row"), "col"),
        P(("dp", "row"), "col"),
        P(("dp", "row"), "col"),
        P(("dp", "row"), "col"),
        P("col", ("dp", "row")),
        P(("dp", "row"), "col"),
        P(("dp", "row"), "col"),
        P("col", ("dp", "row")),
        P(("dp", "row")),
        P(("dp", "row")),
        P("dp"),
        P(("dp", "row"), "col"),
    )
    out_specs = (
        P(("dp", "row"), "col"),
        P(("dp", "row"), "col"),
        P(("dp", "row")),
        P(("dp", "row")),
        P(("dp", "row"), "col"),
        P(("dp", "row"), "col"),
        P(("dp", "row"), "col"),
        P("col", ("dp", "row")),
        P(("dp", "row"), "col"),
        P(("dp", "row"), "col"),
        P("col", ("dp", "row")),
    )
    return jax.shard_map(
        per_device, mesh=mesh, in_specs=in_specs, out_specs=out_specs, check_vma=False
    )
```
